32 devices in a mesh: dp: 16 (over z, y, core), tensor: 2 (over x).
Axes of the slice: x: 2, y: 2, z: 4, core: 2. Of those that a mesh axis runs over, the one named last changes fastest.
Arguments:
- tokens: float32 [2, 25600, 512], P(None, ('dp', 'tensor')), may hold values from -6 to 6
- key_mask: int32 [2, 128, 200], P(None, 'dp'), may hold values from 0 to 1, as said below
- expert_ids: int32 [2, 25600, 2], P(None, 'dp'), may hold values from 0 to 31, as said below
- slot_ids: int32 [2, 25600, 2], P(None, 'dp'), may hold values from -1 to 119, as said below
- norm1_gain: float32 [512], P(('dp', 'tensor')), may hold values from 0.25 to 1.75
- norm1_bias: float32 [512], P(('dp', 'tensor')), may hold values from -3 to 3
- qkv_weight: bfloat16 [512, 3, 512], P('dp', None, 'tensor'), may hold values from -0.25 to 0.25
- out_weight: bfloat16 [512, 512], P('tensor', 'dp'), may hold values from -1 to 1
- norm2_gain: float32 [512], P(('dp', 'tensor')), may hold values from 0.25 to 1.75
- norm2_bias: float32 [512], P(('dp', 'tensor')), may hold values from -3 to 3
- router_weight: float32 [512, 32], P(('dp', 'tensor')), may hold values from -0.25 to 0.25
- expert_in: bfloat16 [32, 512, 2048], P(None, 'dp', 'tensor'), may hold values from -0.25 to 0.25
- expert_out: bfloat16 [32, 2048, 512], P(None, 'tensor', 'dp'), may hold values from -3 to 3
- cotangent: float32 [2, 25600, 512], P(None, ('dp', 'tensor')), may hold values from -6 to 6
Outputs:
- block_out: float32 [2, 25600, 512], P(None, ('dp', 'tensor'))
- input_grad: float32 [2, 25600, 512], P(None, ('dp', 'tensor'))
- norm1_gain_grad: float32 [512], P(('dp', 'tensor'))
- norm1_bias_grad: float32 [512], P(('dp', 'tensor'))
- qkv_grad: float32 [512, 3, 512], P('dp', None, 'tensor')
- out_grad: float32 [512, 512], P('tensor', 'dp')
- norm2_gain_grad: float32 [512], P(('dp', 'tensor'))
- norm2_bias_grad: float32 [512], P(('dp', 'tensor'))
- router_grad: float32 [512, 32], P(('dp', 'tensor'))
- expert_in_grad: float32 [32, 512, 2048], P(None, 'dp', 'tensor')
- expert_out_grad: float32 [32, 2048, 512], P(None, 'tensor', 'dp')
The draws below stay inside these ranges and needn't reach their ends.
Inputs may be any that keep to these rules, and one draw needn't show every extreme that they name: `key_mask`: position 0 of every image is 1; positions 197 to 199 are 0. `expert_ids`: each row names two different experts. `slot_ids`: slots count within routing groups of 1600 consecutive rows of a micro-batch. -1 marks a dropped route; no two other routes of a group share expert and slot, and the slots used by one expert in a group are 0, 1, 2, ... without gaps.
All inputs are finite; a program needn't handle non-finite values.
Results may differ from the reference program's by a relative error of at most 0.035.
Values may be sent and summed in bfloat16 or wider, within the bound.
A program may use at most 264 MiB of HBM per device.

```python
import jax
import jax.numpy as jnp
from jax import lax

D = 512
HEADS = 8
HEAD = 64
FF = 2048
EXPERTS = 32
LEN = 200
MICRO = 2
IMGS = 8
VALID = 197
CAP = 120
ROWS = 25600
N_DP = 16


def draw_key_mask(key, part):
    shape_all = (MICRO, N_DP * IMGS, LEN)
    positions = lax.broadcasted_iota(jnp.int32, shape_all, 2)
    random_bits = jax.random.randint(key, shape_all, 0, 8)
    keeper = (positions < VALID) & ((random_bits != 0) | (positions == 0))
    return keeper.astype(jnp.int32)


def route_tables(key):
    base_key = jax.random.fold_in(key, 7)
    first_key, second_key, third_key, fourth_key = jax.random.split(base_key, 4)
    group_count = MICRO * N_DP
    group_rows = IMGS * LEN
    favored = jax.random.randint(first_key, (group_count, 1), 0, EXPERTS)
    chooser = jax.random.randint(second_key, (group_count, group_rows), 0, 4) == 0
    spread_pick = jax.random.randint(third_key, (group_count, group_rows), 0, EXPERTS)
    primary = jnp.where(chooser, favored, spread_pick)
    secondary = (primary + 1 + jax.random.randint(fourth_key, (group_count, group_rows), 0, EXPERTS - 1)) % EXPERTS
    ordered = jnp.concatenate([primary, secondary], axis=1)
    onehots = (ordered[:, :, None] == jnp.arange(EXPERTS, dtype=jnp.int32)).astype(jnp.int32)
    ranks = jnp.sum((jnp.cumsum(onehots, axis=1) - 1) * onehots, axis=-1)
    places = jnp.where(ranks < CAP, ranks, -1)
    expert_table = jnp.stack([primary, secondary], -1).reshape(MICRO, N_DP * group_rows, 2)
    place_table = jnp.stack([places[:, :group_rows], places[:, group_rows:]], -1).reshape(MICRO, N_DP * group_rows, 2)
    return (expert_table.astype(jnp.int32), place_table.astype(jnp.int32))


def draw_expert_ids(key, part):
    return route_tables(key)[0]


def draw_slot_ids(key, part):
    return route_tables(key)[1]


def spiked(values, key, source, target, blocks, factor):
    def block_of(axis_at):
        return (jnp.arange(values.shape[axis_at]) // (values.shape[axis_at] // blocks)).reshape((-1,) + (1,) * (values.ndim - 1 - axis_at))

    first = jax.random.permutation(key, blocks)[block_of(target)]
    far = (block_of(target) + blocks // 2) % blocks
    return jnp.where((block_of(source) == first) | (block_of(source) == far), factor * values, values)


def levels(key, extent, cuts, smallest, high):
    def one(axis_at, parts):
        draws = jax.random.uniform(jax.random.fold_in(jax.random.fold_in(key, 6), axis_at), (parts,), jnp.float32, smallest / len(cuts), high / len(cuts))
        return jnp.repeat(jnp.exp(draws), extent[axis_at] // parts).reshape((-1,) + (1,) * (len(extent) - axis_at - 1))

    factor_of = one(*cuts[0])
    for cut in cuts[1:]:
        factor_of = factor_of * one(*cut)
    return factor_of


def normal_values(key, dims, scale, most, shards=(), held_as=jnp.bfloat16):
    factor_of = levels(key, dims, shards, -0.22, 0.18) if shards else 1.0
    drawn = jax.random.normal(key, dims, jnp.float32) * scale * factor_of
    return jnp.minimum(jnp.maximum(drawn, -most), most).astype(held_as)


def heavy_noise(key, extent, deviation, limit, cuts, heavy, kind=jnp.bfloat16):
    entries = deviation * jax.random.normal(key, extent, jnp.float32)
    if cuts:
        entries = entries * levels(key, extent, cuts, -0.22, 0.18)
    return jnp.clip(spiked(entries, jax.random.fold_in(key, 3), *heavy), -limit, limit).astype(kind)


def setup_inputs(seed: int = 0) -> dict:
    arg_keys = jax.random.split(jax.random.key(seed), 15)
    tokens = normal_values(arg_keys[0], (MICRO, ROWS, D), 1.0, 6.0, ((1, 32),), jnp.float32)
    key_mask = draw_key_mask(jax.random.fold_in(arg_keys[14], 71), 0)
    expert_ids = draw_expert_ids(jax.random.fold_in(arg_keys[14], 71), 0)
    slot_ids = draw_slot_ids(jax.random.fold_in(arg_keys[14], 71), 0)
    norm1_gain = jnp.clip(1.0 + 0.15 * jax.random.normal(arg_keys[4], (D,), jnp.float32), 0.25, 1.75)
    norm1_bias = normal_values(arg_keys[5], (D,), 0.5, 3.0, ((0, 32),), jnp.float32)
    qkv_weight = normal_values(arg_keys[6], (D, 3, D), D ** -0.5, 0.25, ((0, 16), (2, 2)))
    out_weight = normal_values(arg_keys[7], (D, D), (D // 16) ** -0.5, 1.0, ((0, 2), (1, 16)))
    norm2_gain = jnp.clip(1.0 + 0.15 * jax.random.normal(arg_keys[8], (D,), jnp.float32), 0.25, 1.75)
    norm2_bias = normal_values(arg_keys[9], (D,), 0.5, 3.0, ((0, 32),), jnp.float32)
    router_weight = normal_values(arg_keys[10], (D, EXPERTS), D ** -0.5, 0.25, ((0, 32),), jnp.float32)
    expert_in = normal_values(arg_keys[11], (EXPERTS, D, FF), D ** -0.5, 0.25, ((1, 16), (2, 2)))
    expert_out = normal_values(arg_keys[12], (EXPERTS, FF, D), (max(FF // 512, 1)) ** -0.5, 3.0, ((1, 2), (2, 16)))
    cotangent = heavy_noise(arg_keys[13], (MICRO, ROWS, D), 1.0, 6.0, ((1, 32),), (1, 2, 32, 2.75), jnp.float32)
    return {"tokens": tokens, "key_mask": key_mask, "expert_ids": expert_ids, "slot_ids": slot_ids, "norm1_gain": norm1_gain, "norm1_bias": norm1_bias, "qkv_weight": qkv_weight, "out_weight": out_weight, "norm2_gain": norm2_gain, "norm2_bias": norm2_bias, "router_weight": router_weight, "expert_in": expert_in, "expert_out": expert_out, "cotangent": cotangent}


@jax.custom_vjp
def low(v):
    return lax.optimization_barrier(v.astype(jnp.bfloat16)).astype(jnp.float32)

@jax.custom_vjp
def low_back(v):
    return v

def low_keep(v):
    return (low(v), None)

def low_pass(kept, grad):
    return (grad,)

def back_keep(v):
    return (v, None)

def back_low(kept, grad):
    return (low(grad),)
low.defvjp(low_keep, low_pass)
low_back.defvjp(back_keep, back_low)

def norm_rows(values, gain, offset):
    center = lax.optimization_barrier(jnp.mean(values, -1, keepdims=True))
    shifted = values - center
    spread = lax.optimization_barrier(jnp.mean(shifted * shifted, -1, keepdims=True))
    return shifted * lax.rsqrt(spread + 1e-06) * gain + offset

def group_forward(weights, row_block, key_flags, experts, places):
    gain_one, bias_one, qkv_full, attn_full, gain_two, bias_two, router_full, first_layer, second_layer = weights
    highest = lax.Precision.HIGHEST
    group_rows = row_block.shape[0]
    slot_count = EXPERTS * CAP
    normed = low(norm_rows(row_block, gain_one, bias_one))

    def project(which):
        product = jnp.dot(normed, qkv_full[:, which, :], precision=highest)
        return low_back(low(product)).reshape(IMGS, LEN, HEADS, HEAD)
    query, keyed, valued = (project(0), project(1), project(2))
    scores = low_back(jnp.einsum('bqhd,bkhd->bhqk', query, keyed, precision=highest) * HEAD ** (-0.5))
    scores = jnp.where(key_flags[:, None, None, :] > 0, scores, -1e+30)
    probs = low(jax.nn.softmax(scores, axis=-1))
    mixed = jnp.einsum('bhqk,bkhd->bqhd', probs, valued, precision=highest)
    mixed = low_back(low(mixed)).reshape(group_rows, D)
    attention = low_back(jnp.dot(mixed, attn_full, precision=highest))
    middle = row_block + attention
    routed = low(norm_rows(middle, gain_two, bias_two))
    gates = jax.nn.softmax(jnp.dot(routed, router_full, precision=highest), axis=-1)
    retained = places >= 0
    chosen = jnp.take_along_axis(gates, experts, axis=1) * retained
    slot_index = jnp.where(retained, experts * CAP + places, slot_count)
    owner = jnp.full((slot_count + 1,), -1, jnp.int32)
    owner = owner.at[slot_index.reshape(-1)].set(jnp.arange(2 * group_rows, dtype=jnp.int32))[:slot_count]
    present = owner >= 0
    source = jnp.maximum(owner, 0)
    dispatched = jnp.where(present[:, None], routed[source // 2], 0.0).reshape(EXPERTS, CAP, D)
    slot_gate = jnp.where(present, chosen.reshape(-1)[source], 0.0)
    hidden_pre = low_back(jnp.einsum('ecd,edf->ecf', dispatched, first_layer, precision=highest))
    hidden = low(jax.nn.gelu(hidden_pre))
    expert_result = low_back(jnp.einsum('ecf,efd->ecd', hidden, second_layer, precision=highest))
    weighted = slot_gate[:, None] * expert_result.reshape(slot_count, D)
    padded = jnp.concatenate([weighted, jnp.zeros((1, D), weighted.dtype)], 0)
    combined = low_back(padded[slot_index[:, 0]] + padded[slot_index[:, 1]])
    return middle + combined

def reference(tokens, key_mask, expert_ids, slot_ids, norm1_gain, norm1_bias, qkv_weight, out_weight, norm2_gain, norm2_bias, router_weight, expert_in, expert_out, cotangent):
    weights = tuple((item.astype(jnp.float32) for item in (norm1_gain, norm1_bias, qkv_weight, out_weight, norm2_gain, norm2_bias, router_weight, expert_in, expert_out)))
    group_rows = IMGS * LEN
    group_count = MICRO * N_DP
    row_groups = tokens.reshape(group_count, group_rows, D)
    flag_groups = key_mask.reshape(group_count, IMGS, LEN)
    expert_groups = expert_ids.reshape(group_count, group_rows, 2)
    place_groups = slot_ids.reshape(group_count, group_rows, 2)
    cot_groups = cotangent.reshape(group_count, group_rows, D)

    def one_group(summed, batch):
        row_block, key_flags, experts, places, cot_block = batch

        def forward(params, inputs):
            return group_forward(params, inputs, key_flags, experts, places)
        result, pullback = jax.vjp(forward, weights, row_block)
        weight_grads, row_grads = pullback(cot_block)
        summed = jax.tree.map(lambda left, right: left + right, summed, weight_grads)
        return (summed, (result, row_grads))
    zeros = jax.tree.map(jnp.zeros_like, weights)
    summed, (results, row_grads) = lax.scan(one_group, zeros, (row_groups, flag_groups, expert_groups, place_groups, cot_groups))
    return (results.reshape(tokens.shape), row_grads.reshape(tokens.shape), summed[0], summed[1], summed[2], summed[3], summed[4], summed[5], summed[6], summed[7], summed[8])
```

```python
import functools

import jax
import jax.numpy as jnp
from jax import lax
from jax.experimental import pallas as pl
from jax.experimental.pallas import tpu as pltpu
from jax.sharding import Mesh, PartitionSpec as P

HEAD = 64
CAP = 120
EPSILON = 1e-06
LANES = 128
VMEM = 60 * 1024 * 1024
NN = (((1,), (0,)), ((), ()))
NT = (((1,), (1,)), ((), ()))
TN = (((0,), (0,)), ((), ()))
HIGH = lax.Precision.HIGHEST
GELU_C = 0.7978845608028654
GELU_A = 0.044715


def mm(a, b, dims=NN, precision=None):
    return lax.dot_general(a, b, dims, precision=precision, preferred_element_type=jnp.float32)


def three_parts(value):
    high = value.astype(jnp.bfloat16)
    rest = value - high.astype(jnp.float32)
    middle = rest.astype(jnp.bfloat16)
    last = (rest - middle.astype(jnp.float32)).astype(jnp.bfloat16)
    return high, middle, last


def standardize(values):
    center = jnp.mean(values, -1, keepdims=True)
    shifted = values - center
    spread = jnp.mean(shifted * shifted, -1, keepdims=True)
    inverse = lax.rsqrt(spread + EPSILON)
    return shifted * inverse, inverse


def norm_back(grad, unit, inverse):
    return inverse * (
        grad
        - jnp.mean(grad, -1, keepdims=True)
        - unit * jnp.mean(grad * unit, -1, keepdims=True)
    )


def even_lanes(shape):
    return lax.broadcasted_iota(jnp.int32, shape, 1) < HEAD


def forward_kernel(
    tok_ref, bias_ref, mats_ref, norms_ref, router_ref,
    middle_ref, routed_ref, proj_ref, mixed_ref, gates_ref,
):
    images, length, width = tok_ref.shape
    rows = images * length
    tok = tok_ref[...].reshape(rows, width)
    unit, _ = standardize(tok)
    normed = (unit * norms_ref[0:1] + norms_ref[1:2]).astype(jnp.bfloat16)
    for c in range(3):
        part = mm(normed, mats_ref[c]).reshape(images, length, width)
        for b in range(images):
            proj_ref[b, :, c * width:(c + 1) * width] = part[b].astype(jnp.bfloat16)
    even = even_lanes((length, LANES))
    scale = jnp.bfloat16(HEAD ** -0.5)
    zero = jnp.zeros((), jnp.bfloat16)
    attended = []
    for b in range(images):
        bias = bias_ref[b]
        pieces = []
        for pair in range(width // LANES):
            lanes = slice(pair * LANES, (pair + 1) * LANES)
            query = proj_ref[b, :, lanes] * scale
            keyed = proj_ref[b, :, width + pair * LANES:width + (pair + 1) * LANES]
            valued = proj_ref[b, :, 2 * width + pair * LANES:2 * width + (pair + 1) * LANES]
            halves = []
            for odd in range(2):
                chosen = jnp.where(even != bool(odd), query, zero)
                scores = mm(chosen, keyed, NT) + bias
                lifted = jnp.exp(scores - jnp.max(scores, -1, keepdims=True))
                probs = lifted * (1.0 / jnp.sum(lifted, -1, keepdims=True))
                halves.append(mm(probs.astype(jnp.bfloat16), valued))
            both = jnp.where(even, halves[0], halves[1])
            mixed_ref[b, :, lanes] = both.astype(jnp.bfloat16)
            pieces.append(both)
        attended.append(jnp.concatenate(pieces, 1))
    joined = jnp.concatenate(attended, 0).astype(jnp.bfloat16)
    middle = tok + mm(joined, mats_ref[3], NT)
    middle_ref[...] = middle.reshape(images, length, width)
    unit, _ = standardize(middle)
    routed = (unit * norms_ref[2:3] + norms_ref[3:4]).astype(jnp.bfloat16)
    wide = routed.astype(jnp.float32)
    routed_ref[...] = wide.reshape(images, length, width).astype(jnp.bfloat16)
    logits = mm(wide, router_ref[...], NN, HIGH)
    lane = lax.broadcasted_iota(jnp.int32, logits.shape, 1)
    logits = jnp.where(lane < 32, logits, -1e30)
    lifted = jnp.exp(logits - jnp.max(logits, -1, keepdims=True))
    gates = lifted / jnp.sum(lifted, -1, keepdims=True)
    gates_ref[...] = gates.reshape(images, length, LANES)


def attention_forward(tok, bias, mats, norms, router, per_step):
    images, length, width = tok.shape

    def rows(last):
        return pl.BlockSpec((per_step, length, last), lambda s: (s, 0, 0))

    def whole(a):
        return pl.BlockSpec(a.shape, lambda s: (0,) * a.ndim)

    shapes = [
        (width, jnp.float32), (width, jnp.bfloat16), (3 * width, jnp.bfloat16),
        (width, jnp.bfloat16), (LANES, jnp.float32),
    ]
    return pl.pallas_call(
        forward_kernel,
        grid=(images // per_step,),
        in_specs=[
            rows(width), pl.BlockSpec((per_step, 1, length), lambda s: (s, 0, 0)),
            whole(mats), whole(norms), whole(router),
        ],
        out_specs=[rows(n) for n, _ in shapes],
        out_shape=[jax.ShapeDtypeStruct((images, length, n), kind) for n, kind in shapes],
        compiler_params=pltpu.CompilerParams(vmem_limit_bytes=VMEM),
        cost_estimate=pl.CostEstimate(
            flops=images * length * width * width * 10, bytes_accessed=images * length * width * 16,
            transcendentals=images * length * length * 8),
        name="attention_forward",
    )(tok, bias, mats, norms, router)


def backward_kernel(
    tok_ref, middle_ref, cot_ref, grad_ref, gates_ref, proj_ref, mixed_ref,
    bias_ref, mats_ref, norms_ref, router_t_ref,
    input_ref, dmats_ref, dnorms_ref, drouter_ref,
    dproj_ref, dmats_acc,
):
    images, length, width = tok_ref.shape
    rows = images * length
    step = pl.program_id(0)

    @pl.when(step == 0)
    def _():
        dmats_acc[...] = jnp.zeros_like(dmats_acc)
        dnorms_ref[...] = jnp.zeros_like(dnorms_ref)
        drouter_ref[...] = jnp.zeros_like(drouter_ref)

    def flat(ref):
        return ref[...].reshape(rows, ref.shape[2])

    middle = flat(middle_ref)
    unit, inverse = standardize(middle)
    grad = flat(grad_ref)
    gates = flat(gates_ref)
    gate_cot = grad[:, width:]
    logit_grad = gates * (gate_cot - jnp.sum(gates * gate_cot, -1, keepdims=True))
    routed = (unit * norms_ref[2:3] + norms_ref[3:4]).astype(jnp.bfloat16)
    drouter_ref[...] += mm(routed.astype(jnp.float32), logit_grad, TN, HIGH)
    routed_grad = grad[:, :width] + mm(logit_grad, router_t_ref[...], NN, HIGH)
    dnorms_ref[2:3] += jnp.sum(routed_grad * unit, 0, keepdims=True)
    dnorms_ref[3:4] += jnp.sum(routed_grad, 0, keepdims=True)
    middle_grad = flat(cot_ref) + norm_back(routed_grad * norms_ref[2:3], unit, inverse)
    attn_cot = middle_grad.astype(jnp.bfloat16)
    joined = jnp.concatenate([mixed_ref[b].astype(jnp.float32) for b in range(images)], 0)
    dmats_acc[3] += mm(attn_cot, joined.astype(jnp.bfloat16), TN)
    mixed_grad = mm(attn_cot, mats_ref[3]).reshape(images, length, width)
    even = even_lanes((length, LANES))
    zero = jnp.zeros((), jnp.bfloat16)
    scale = jnp.bfloat16(HEAD ** -0.5)
    for b in range(images):
        bias = bias_ref[b]
        mixed_low = mixed_grad[b].astype(jnp.bfloat16)
        for pair in range(width // LANES):
            lanes = slice(pair * LANES, (pair + 1) * LANES)
            query = proj_ref[b, :, lanes] * scale
            keyed = proj_ref[b, :, width + pair * LANES:width + (pair + 1) * LANES]
            valued = proj_ref[b, :, 2 * width + pair * LANES:2 * width + (pair + 1) * LANES]
            out_cot = mixed_low[:, lanes]
            query_grad = keyed_grad = value_grad = None
            for odd in range(2):
                mask = even != bool(odd)
                query_half = jnp.where(mask, query, zero)
                keyed_half = jnp.where(mask, keyed, zero)
                cot_half = jnp.where(mask, out_cot, zero)
                scores = mm(query_half, keyed, NT) + bias
                lifted = jnp.exp(scores - jnp.max(scores, -1, keepdims=True))
                probs = lifted * (1.0 / jnp.sum(lifted, -1, keepdims=True))
                prob_grad = mm(cot_half, valued, NT)
                value_part = mm(probs.astype(jnp.bfloat16), cot_half, TN)
                inner = jnp.sum(probs * prob_grad, -1, keepdims=True)
                score_grad = (probs * (prob_grad - inner)).astype(jnp.bfloat16)
                query_part = mm(score_grad, keyed_half)
                keyed_part = mm(score_grad, query_half, TN)
                if odd:
                    query_grad, keyed_grad, value_grad = (
                        query_grad + query_part, keyed_grad + keyed_part, value_grad + value_part)
                else:
                    query_grad, keyed_grad, value_grad = query_part, keyed_part, value_part
            base = pair * LANES
            rows_here = slice(b * length, (b + 1) * length)
            dproj_ref[rows_here, base:base + LANES] = query_grad * (HEAD ** -0.5)
            dproj_ref[rows_here, width + base:width + base + LANES] = keyed_grad
            dproj_ref[rows_here, 2 * width + base:2 * width + base + LANES] = value_grad
    tok = flat(tok_ref)
    unit, inverse = standardize(tok)
    normed = (unit * norms_ref[0:1] + norms_ref[1:2]).astype(jnp.bfloat16)
    normed_grad = jnp.zeros((rows, width), jnp.float32)
    for c in range(3):
        part = dproj_ref[:, c * width:(c + 1) * width].astype(jnp.bfloat16)
        dmats_acc[c] += mm(normed, part, TN)
        normed_grad += mm(part, mats_ref[c], NT)
    dnorms_ref[0:1] += jnp.sum(normed_grad * unit, 0, keepdims=True)
    dnorms_ref[1:2] += jnp.sum(normed_grad, 0, keepdims=True)
    input_grad = middle_grad + norm_back(normed_grad * norms_ref[0:1], unit, inverse)
    input_ref[...] = input_grad.reshape(images, length, width)

    @pl.when(step == pl.num_programs(0) - 1)
    def _():
        dmats_ref[...] = dmats_acc[...].astype(jnp.bfloat16)


def attention_backward(tok, middle, cot, grad, gates, proj, mixed, bias, mats, norms, router_t, per_step):
    images, length, width = tok.shape

    def rows(last):
        return pl.BlockSpec((per_step, length, last), lambda s: (s, 0, 0))

    def whole(shape):
        return pl.BlockSpec(shape, lambda s: (0,) * len(shape))

    return pl.pallas_call(
        backward_kernel,
        grid=(images // per_step,),
        in_specs=[
            rows(width), rows(width), rows(width), rows(width + LANES), rows(LANES),
            rows(3 * width), rows(width), pl.BlockSpec((per_step, 1, length), lambda s: (s, 0, 0)),
            whole(mats.shape), whole(norms.shape), whole(router_t.shape),
        ],
        out_specs=[
            rows(width), whole(mats.shape), whole((4, width)), whole((width, LANES)),
        ],
        out_shape=[
            jax.ShapeDtypeStruct((images, length, width), jnp.float32),
            jax.ShapeDtypeStruct(mats.shape, jnp.bfloat16),
            jax.ShapeDtypeStruct((4, width), jnp.float32),
            jax.ShapeDtypeStruct((width, LANES), jnp.float32),
        ],
        scratch_shapes=[
            pltpu.VMEM((per_step * length, 3 * width), jnp.float32),
            pltpu.VMEM(mats.shape, jnp.float32),
        ],
        compiler_params=pltpu.CompilerParams(vmem_limit_bytes=VMEM),
        cost_estimate=pl.CostEstimate(
            flops=images * length * width * width * 30, bytes_accessed=images * length * width * 30,
            transcendentals=images * length * length * 8),
        name="attention_backward",
    )(tok, middle, cot, grad, gates, proj, mixed, bias, mats, norms, router_t)


def expert_kernel(
    expert_ref, slots_ref, cots_ref, weights_ref, router_ref,
    result_ref, back_ref, dweights_ref,
    rows_t, grads_t, grads, gate_scr, result_acc, back_acc, first_acc, second_acc,
):
    count, width = slots_ref.shape
    tile = weights_ref.shape[-1]
    chunk = rows_t.shape[2]
    step = pl.program_id(0)
    first = weights_ref[:, :, 0, 0].reshape(width, tile)
    second = weights_ref[:, :, 0, 1].reshape(width, tile)

    @pl.when(step == 0)
    def _():
        def prepare(r, carry):
            here = pl.ds(pl.multiple_of(r * chunk, 16), chunk)
            slots = slots_ref[here]
            logits = mm(slots, router_ref[0]) + mm(slots, router_ref[1]) + mm(slots, router_ref[2])
            lane = lax.broadcasted_iota(jnp.int32, logits.shape, 1)
            logits = jnp.where(lane < 32, logits, -1e30)
            lifted = jnp.exp(logits - jnp.max(logits, -1, keepdims=True))
            gates = lifted / jnp.sum(lifted, -1, keepdims=True)
            gate = jnp.sum(jnp.where(lane == expert_ref[0], gates, 0.0), -1, keepdims=True)
            gate_scr[here] = jnp.broadcast_to(gate, logits.shape)
            low = (cots_ref[here].astype(jnp.float32) * gate).astype(jnp.bfloat16)
            grads[here] = low
            rows_t[r] = slots.T
            grads_t[r] = low.T
            result_acc[here] = jnp.zeros((chunk, width), jnp.float32)
            back_acc[here] = jnp.zeros((chunk, width), jnp.float32)
            return carry

        lax.fori_loop(0, count // chunk, prepare, 0)

    first_acc[...] = jnp.zeros_like(first_acc)
    second_acc[...] = jnp.zeros_like(second_acc)

    def work(r, carry):
        here = pl.ds(pl.multiple_of(r * chunk, 16), chunk)
        pre = mm(slots_ref[here], first)
        square = pre * pre
        half = 0.5 + 0.5 * jnp.tanh(pre * (GELU_C + (GELU_C * GELU_A) * square))
        hidden = (pre * half).astype(jnp.bfloat16)
        slope = half + 2.0 * half * (1.0 - half) * pre * (GELU_C + (3.0 * GELU_C * GELU_A) * square)
        hidden_grad = mm(grads[here], second)
        pre_grad = (hidden_grad * slope).astype(jnp.bfloat16)
        result_acc[here] += mm(hidden, second, NT)
        back_acc[here] += mm(pre_grad, first, NT)
        first_acc[...] += mm(rows_t[r], pre_grad)
        second_acc[...] += mm(grads_t[r], hidden)
        return carry

    lax.fori_loop(0, count // chunk, work, 0)
    block = weights_ref.shape[:2] + weights_ref.shape[4:]
    dweights_ref[:, :, 0, 0] = first_acc[...].astype(jnp.bfloat16).reshape(block)
    dweights_ref[:, :, 0, 1] = second_acc[...].astype(jnp.bfloat16).reshape(block)

    @pl.when(step == pl.num_programs(0) - 1)
    def _():
        def finish(r, carry):
            here = pl.ds(pl.multiple_of(r * chunk, 16), chunk)
            result = result_acc[here]
            gate = gate_scr[here][:, 0:1]
            result_ref[here] = (result * gate).astype(jnp.bfloat16)
            gate_grad = jnp.sum(cots_ref[here].astype(jnp.float32) * result, -1, keepdims=True)
            lane = lax.broadcasted_iota(jnp.int32, (chunk, LANES), 1)
            back_ref[here, 0:width] = back_acc[here].astype(jnp.bfloat16)
            back_ref[here, width:width + LANES] = jnp.where(
                lane == expert_ref[0], gate_grad, 0.0).astype(jnp.bfloat16)
            return carry

        lax.fori_loop(0, count // chunk, finish, 0)


def run_expert(expert, slots, cots, weights, router):
    count, width = slots.shape
    planes, inner, parts, _, depth, extent = weights.shape
    tile = min(512, extent)
    per_part = extent // tile
    chunk = 480

    def whole(shape):
        return pl.BlockSpec(shape, lambda s, e: (0,) * len(shape))

    weight_spec = pl.BlockSpec(
        (planes, inner, 1, 2, depth, tile), lambda s, e: (0, 0, s // per_part, 0, 0, s % per_part))
    return pl.pallas_call(
        expert_kernel,
        grid_spec=pltpu.PrefetchScalarGridSpec(
            num_scalar_prefetch=1,
            grid=(parts * per_part,),
            in_specs=[whole(slots.shape), whole(cots.shape), weight_spec, whole(router.shape)],
            out_specs=[whole((count, width)), whole((count, width + LANES)), weight_spec],
            scratch_shapes=[
                pltpu.VMEM((count // chunk, width, chunk), jnp.bfloat16),
                pltpu.VMEM((count // chunk, width, chunk), jnp.bfloat16),
                pltpu.VMEM((count, width), jnp.bfloat16),
                pltpu.VMEM((count, LANES), jnp.float32),
                pltpu.VMEM((count, width), jnp.float32),
                pltpu.VMEM((count, width), jnp.float32),
                pltpu.VMEM((width, tile), jnp.float32),
                pltpu.VMEM((width, tile), jnp.float32),
            ],
        ),
        out_shape=[
            jax.ShapeDtypeStruct((count, width), jnp.bfloat16),
            jax.ShapeDtypeStruct((count, width + LANES), jnp.bfloat16),
            jax.ShapeDtypeStruct(weights.shape, jnp.bfloat16),
        ],
        compiler_params=pltpu.CompilerParams(vmem_limit_bytes=VMEM),
        cost_estimate=pl.CostEstimate(
            flops=12 * count * width * extent * parts,
            bytes_accessed=4 * 2 * width * extent * parts + count * width * 8,
            transcendentals=count * extent * parts),
        name="expert",
    )(expert, slots, cots, weights, router)


def per_device(planes, inner, parts, tokens, key_mask, expert_ids, slot_ids, norm1_gain, norm1_bias,
               qkv_weight, out_weight, norm2_gain, norm2_bias, router_weight, expert_in, expert_out,
               cotangent):
    micros, own_rows, width = tokens.shape
    length = key_mask.shape[2]
    group_rows = own_rows * parts
    images = own_rows // length
    total = micros * images
    experts = expert_in.shape[0]
    homes = inner * parts
    local = experts // homes
    depth, extent = expert_in.shape[1:]
    small = norm1_gain.shape[0]
    every = ("o", "i", "t")
    plane_at, inner_at, part_at = (lax.axis_index(name) for name in every)
    low = jnp.bfloat16

    loose = jnp.concatenate([
        jnp.stack([norm1_gain, norm1_bias, norm2_gain, norm2_bias], 1), router_weight], 1)
    loose_count = 3 * loose.size
    columns = qkv_weight.shape[2]
    loose_rows = -(-loose_count // (16 * columns)) * 16
    loose_low = jnp.concatenate([p.reshape(-1) for p in three_parts(loose)])
    loose_low = jnp.pad(loose_low, (0, loose_rows * columns - loose_count)).reshape(loose_rows, columns)
    packed = jnp.concatenate([
        qkv_weight.transpose(1, 0, 2).reshape(3 * depth, columns), out_weight.T, loose_low], 0)
    gathered = lax.all_gather(packed, ("o", "i"), axis=0)
    gathered = lax.all_gather(gathered, "t", axis=0)
    mats = gathered[:, :, :4 * depth].reshape(parts, planes * inner, 4, depth, columns)
    mats = mats.transpose(2, 1, 3, 0, 4).reshape(4, width, width)
    loose_all = gathered[:, :, 4 * depth:].reshape(parts, planes * inner, loose_rows * columns)
    loose_all = loose_all[:, :, :loose_count].astype(jnp.float32)
    loose_all = loose_all.reshape(parts, planes * inner, 3, small, 4 + experts)
    loose_all = (loose_all[:, :, 0] + loose_all[:, :, 1]) + loose_all[:, :, 2]
    loose_all = loose_all.transpose(1, 0, 2, 3).reshape(width, 4 + experts)
    norms = loose_all[:, :4].T
    router = jnp.pad(loose_all[:, 4:], ((0, 0), (0, LANES - experts)))
    router_three = jnp.stack(three_parts(router))

    weights = []
    first_in = expert_in.reshape(homes, local, depth, extent)
    second_in = expert_out.transpose(0, 2, 1).reshape(homes, local, depth, extent)
    for k in range(local):
        both = jnp.stack([first_in[:, k], second_in[:, k]], 1)
        mine = lax.all_to_all(both, ("i", "t"), 0, 0, tiled=True)
        if planes == 2:
            other = lax.ppermute(mine, "o", [(0, 1), (1, 0)])
            full = jnp.where(plane_at == 0, jnp.stack([mine, other]), jnp.stack([other, mine]))
        else:
            full = lax.all_gather(mine, "o", axis=0)
        weights.append(full.reshape(planes, inner, parts, 2, depth, extent))

    own_first = part_at * own_rows
    slot_index = jnp.where(slot_ids >= 0, expert_ids * CAP + slot_ids, -1)
    if parts == 2:
        slot_index = jnp.concatenate([
            lax.dynamic_slice_in_dim(slot_index, own_first, own_rows, 1),
            lax.dynamic_slice_in_dim(slot_index, own_rows - own_first, own_rows, 1)], 1)
    homes_i = lax.broadcasted_iota(jnp.int32, (inner, local, CAP), 0)
    locals_i = lax.broadcasted_iota(jnp.int32, (inner, local, CAP), 1)
    cap_i = lax.broadcasted_iota(jnp.int32, (inner, local, CAP), 2)
    places = ((homes_i * parts + part_at) * local + locals_i) * CAP + cap_i

    def table(m, positions, rows=slice(None)):
        index = slot_index[m, rows]
        flat = positions.reshape(1, -1)
        return ((index[:, 0:1] == flat) | (index[:, 1:2] == flat)).astype(low)

    def share(rows):
        if parts == 2:
            return jnp.concatenate([rows, lax.ppermute(rows, "t", [(0, 1), (1, 0)])], 1)
        return lax.all_gather(rows, "t", axis=1, tiled=True)

    def dispatch(shared):
        sent = []
        for m in range(micros):
            slots = mm(table(m, places), shared[m], TN).astype(low)
            slots = lax.all_to_all(slots.reshape(inner, local * CAP, width), "i", 0, 0, tiled=True)
            sent.append(slots.reshape(inner, local, CAP, width))
        return [
            jnp.concatenate([s[:, k].reshape(inner * CAP, width) for s in sent], 0) for k in range(local)]

    cot_slots = dispatch(share(cotangent.astype(low)))

    flags = lax.dynamic_slice_in_dim(key_mask, part_at * images, images, 1).reshape(total, 1, length)
    bias = jnp.where(flags > 0, 0.0, -1e30).astype(jnp.float32)
    tok = tokens.reshape(total, length, width)
    per_step = 2 if total % 2 == 0 else 1
    middle, routed, proj, mixed, gates = attention_forward(tok, bias, mats, norms, router, per_step)

    row_slots = dispatch(share(routed.reshape(micros, own_rows, width)))

    first_out, second_out, results, backs = [], [], [], []
    for k in range(local):
        expert = ((inner_at * parts + part_at) * local + k).astype(jnp.int32).reshape(1)
        result, back, dweights = run_expert(expert, row_slots[k], cot_slots[k], weights[k], router_three)
        results.append(result.reshape(micros, inner, CAP, width))
        backs.append(back.reshape(micros, inner, CAP, width + LANES))
        dweights = dweights.reshape(planes, homes, 2, depth, extent)
        if planes == 2:
            theirs = lax.dynamic_index_in_dim(dweights, 1 - plane_at, 0, keepdims=False)
            ours = lax.dynamic_index_in_dim(dweights, plane_at, 0, keepdims=False)
            summed = ours.astype(jnp.float32) + lax.ppermute(
                theirs, "o", [(0, 1), (1, 0)]).astype(jnp.float32)
            summed = summed.astype(low)
        else:
            summed = lax.psum_scatter(dweights, "o", scatter_dimension=0, tiled=True)[0]
        final = lax.all_to_all(summed, ("i", "t"), 0, 0, tiled=True)
        first_out.append(final[:, 0])
        second_out.append(final[:, 1])
    first_grad = jnp.stack(first_out, 1).reshape(experts, depth, extent).astype(jnp.float32)
    second_grad = jnp.stack(second_out, 1).reshape(experts, depth, extent).astype(jnp.float32)
    second_grad = second_grad.transpose(0, 2, 1)

    def collect(values):
        size = values[0].shape[-1]
        answers = []
        for m in range(micros):
            back = jnp.stack([v[m] for v in values], 1).reshape(inner, local * CAP, size)
            back = lax.all_to_all(back, "i", 0, 0, tiled=True).reshape(inner * local * CAP, size)
            if parts == 2:
                away = mm(table(m, places, slice(own_rows, None)), back).astype(low)
                here = mm(table(m, places, slice(0, own_rows)), back)
                answers.append(here + lax.ppermute(away, "t", [(0, 1), (1, 0)]).astype(jnp.float32))
            else:
                whole = mm(table(m, places), back).astype(low)
                answers.append(lax.psum_scatter(
                    whole, "t", scatter_dimension=0, tiled=True).astype(jnp.float32))
        return jnp.stack(answers)

    grad = collect(backs)
    combined = collect(results)
    block_out = middle.reshape(micros, own_rows, width) + combined

    input_grad, dmats, dnorms, drouter = attention_backward(
        tok, middle, cotangent.reshape(total, length, width), grad.reshape(total, length, width + LANES),
        gates, proj, mixed, bias, mats, norms, router.T, per_step)
    input_grad = input_grad.reshape(micros, own_rows, width)

    dmats = dmats.reshape(4, planes, inner, depth, parts, columns).transpose(2, 4, 1, 0, 3, 5)
    dmats = dmats.reshape(homes, planes, 4 * depth, columns)
    dloose = jnp.concatenate([dnorms.T, drouter[:, :experts]], 1)
    dloose = dloose.reshape(planes, inner, parts, small * (4 + experts)).transpose(1, 2, 0, 3)
    dloose = jnp.concatenate(three_parts(dloose), -1)
    dloose = jnp.pad(dloose, ((0, 0),) * 3 + ((0, loose_rows * columns - loose_count),))
    dloose = dloose.reshape(homes, planes, loose_rows, columns)
    payload = jnp.concatenate([dmats, dloose], 2)
    payload = lax.all_to_all(payload, ("i", "t"), 0, 0, tiled=True)
    payload = jnp.sum(payload.astype(jnp.float32), 0)
    if planes == 2:
        theirs = lax.dynamic_index_in_dim(payload, 1 - plane_at, 0, keepdims=False)
        ours = lax.dynamic_index_in_dim(payload, plane_at, 0, keepdims=False)
        reduced = ours + lax.ppermute(theirs, "o", [(0, 1), (1, 0)])
    else:
        reduced = lax.psum_scatter(payload, "o", scatter_dimension=0, tiled=True)[0]
    matrices = reduced[:4 * depth].reshape(4, depth, columns)
    qkv_grad = matrices[:3].transpose(1, 0, 2)
    out_grad = matrices[3].T
    tail = reduced[4 * depth:].reshape(-1)[:loose_count].reshape(3, small, 4 + experts)
    tail = (tail[0] + tail[1]) + tail[2]
    return (
        block_out, input_grad, tail[:, 0], tail[:, 1], qkv_grad, out_grad, tail[:, 2], tail[:, 3],
        tail[:, 4:], first_grad, second_grad,
    )


def solution(mesh):
    dp, parts = mesh.shape["dp"], mesh.shape["tensor"]
    inner = min(8, 32 // parts, dp)
    planes = dp // inner
    fine = Mesh(mesh.devices.reshape(planes, inner, parts), ("o", "i", "t"))
    dps = ("o", "i")
    every = ("o", "i", "t")
    rows = P(None, every, None)
    return jax.shard_map(
        functools.partial(per_device, planes, inner, parts),
        mesh=fine,
        in_specs=(
            rows, P(None, dps, None), P(None, dps, None), P(None, dps, None), P(every), P(every),
            P(dps, None, "t"), P("t", dps), P(every), P(every), P(every, None),
            P(None, dps, "t"), P(None, "t", dps), rows,
        ),
        out_specs=(
            rows, rows, P(every), P(every), P(dps, None, "t"), P("t", dps), P(every), P(every),
            P(every, None), P(None, dps, "t"), P(None, "t", dps),
        ),
        check_vma=False,
    )
```

```python
import functools

import jax
import jax.numpy as jnp
from jax import lax
from jax.experimental import pallas as pl
from jax.experimental.pallas import tpu as pltpu
from jax.sharding import Mesh, PartitionSpec as P

HEAD = 64
CAP = 120
EPSILON = 1e-06
LANES = 128
VMEM = 60 * 1024 * 1024
NN = (((1,), (0,)), ((), ()))
NT = (((1,), (1,)), ((), ()))
TN = (((0,), (0,)), ((), ()))
HIGH = lax.Precision.HIGHEST
GELU_C = 0.7978845608028654
GELU_A = 0.044715


def mm(a, b, dims=NN, precision=None):
    return lax.dot_general(a, b, dims, precision=precision, preferred_element_type=jnp.float32)


def three_parts(value):
    high = value.astype(jnp.bfloat16)
    rest = value - high.astype(jnp.float32)
    middle = rest.astype(jnp.bfloat16)
    last = (rest - middle.astype(jnp.float32)).astype(jnp.bfloat16)
    return high, middle, last


def standardize(values):
    center = jnp.mean(values, -1, keepdims=True)
    shifted = values - center
    spread = jnp.mean(shifted * shifted, -1, keepdims=True)
    inverse = lax.rsqrt(spread + EPSILON)
    return shifted * inverse, inverse


def norm_back(grad, unit, inverse):
    return inverse * (
        grad
        - jnp.mean(grad, -1, keepdims=True)
        - unit * jnp.mean(grad * unit, -1, keepdims=True)
    )


def even_lanes(shape):
    return lax.broadcasted_iota(jnp.int32, shape, 1) < HEAD


def router_gates(routed, parts):
    logits = mm(routed, parts, NT)
    logits = logits + pltpu.roll(logits, LANES - 32, 1) + pltpu.roll(logits, LANES - 64, 1)
    lane = lax.broadcasted_iota(jnp.int32, logits.shape, 1)
    logits = jnp.where(lane < 32, logits, -1e30)
    lifted = jnp.exp(logits - jnp.max(logits, -1, keepdims=True))
    return lifted / jnp.sum(lifted, -1, keepdims=True)


def forward_rows(first, images, tok_ref, bias_ref, mats_ref, norms_ref, parts_ref,
                 middle_ref, proj_ref, mixed_ref, gates_ref):
    _, length, width = tok_ref.shape
    pieces, _, _, columns = mats_ref.shape
    rows = images * length
    here = pl.ds(first, images)
    tok = tok_ref[here].reshape(rows, width)
    unit, _ = standardize(tok)
    normed = (unit * norms_ref[0:1] + norms_ref[1:2]).astype(jnp.bfloat16)
    for c in range(3):
        for p in range(pieces):
            part = mm(normed, mats_ref[p, c]).reshape(images, length, columns)
            base = c * width + p * columns
            for b in range(images):
                proj_ref[first + b, :, base:base + columns] = part[b].astype(jnp.bfloat16)
    even = even_lanes((length, LANES))
    scale = jnp.bfloat16(HEAD ** -0.5)
    zero = jnp.zeros((), jnp.bfloat16)
    attended = []
    for b in range(images):
        bias = bias_ref[first + b]
        parts = []
        for pair in range(width // LANES):
            lanes = slice(pair * LANES, (pair + 1) * LANES)
            query = proj_ref[first + b, :, lanes] * scale
            keyed = proj_ref[first + b, :, width + pair * LANES:width + (pair + 1) * LANES]
            valued = proj_ref[first + b, :, 2 * width + pair * LANES:2 * width + (pair + 1) * LANES]
            halves = []
            for odd in range(2):
                chosen = jnp.where(even != bool(odd), query, zero)
                scores = mm(chosen, keyed, NT) + bias
                lifted = jnp.exp(scores - jnp.max(scores, -1, keepdims=True))
                probs = lifted * (1.0 / jnp.sum(lifted, -1, keepdims=True))
                halves.append(mm(probs.astype(jnp.bfloat16), valued))
            both = jnp.where(even, halves[0], halves[1])
            mixed_ref[first + b, :, lanes] = both.astype(jnp.bfloat16)
            parts.append(both)
        attended.append(jnp.concatenate(parts, 1))
    joined = jnp.concatenate(attended, 0).astype(jnp.bfloat16)
    middle = tok
    for p in range(pieces):
        middle += mm(joined[:, p * columns:(p + 1) * columns], mats_ref[p, 3], NT)
    middle_ref[here] = middle.reshape(images, length, width)
    unit, _ = standardize(middle)
    routed = unit * norms_ref[2:3] + norms_ref[3:4]
    low = routed.astype(jnp.bfloat16)
    gates_ref[here] = router_gates(low, parts_ref[...]).reshape(images, length, LANES)
    return routed, low


def forward_kernel(
    tok_ref, bias_ref, mats_ref, norms_ref, parts_ref,
    middle_ref, routed_ref, proj_ref, mixed_ref, gates_ref,
):
    images, length, width = tok_ref.shape
    routed, _ = forward_rows(0, images, tok_ref, bias_ref, mats_ref, norms_ref, parts_ref,
                             middle_ref, proj_ref, mixed_ref, gates_ref)
    routed_ref[...] = routed.reshape(images, length, width).astype(jnp.bfloat16)


def attention_forward(tok, bias, mats, norms, router, per_step):
    images, length, width = tok.shape

    def rows(last):
        return pl.BlockSpec((per_step, length, last), lambda s: (s, 0, 0))

    def whole(a):
        return pl.BlockSpec(a.shape, lambda s: (0,) * a.ndim)

    shapes = [
        (width, jnp.float32), (width, jnp.bfloat16), (3 * width, jnp.bfloat16),
        (width, jnp.bfloat16), (LANES, jnp.float32),
    ]
    return pl.pallas_call(
        forward_kernel,
        grid=(images // per_step,),
        in_specs=[
            rows(width), pl.BlockSpec((per_step, 1, length), lambda s: (s, 0, 0)),
            whole(mats), whole(norms), whole(router),
        ],
        out_specs=[rows(n) for n, _ in shapes],
        out_shape=[jax.ShapeDtypeStruct((images, length, n), kind) for n, kind in shapes],
        compiler_params=pltpu.CompilerParams(vmem_limit_bytes=VMEM),
        cost_estimate=pl.CostEstimate(
            flops=images * length * width * width * 10, bytes_accessed=images * length * width * 16,
            transcendentals=images * length * length * 8),
        name="attention_forward",
    )(tok, bias, mats, norms, router)


def backward_kernel(
    tok_ref, middle_ref, cot_ref, grad_ref, gates_ref, proj_ref, mixed_ref,
    bias_ref, mats_ref, norms_ref, router_t_ref,
    input_ref, dmats_ref, dnorms_ref, drouter_ref,
    dproj_ref, dmats_acc,
):
    images, length, width = tok_ref.shape
    rows = images * length
    step = pl.program_id(0)

    @pl.when(step == 0)
    def _():
        dmats_acc[...] = jnp.zeros_like(dmats_acc)
        dnorms_ref[...] = jnp.zeros_like(dnorms_ref)
        drouter_ref[...] = jnp.zeros_like(drouter_ref)

    def flat(ref):
        return ref[...].reshape(rows, ref.shape[2])

    middle = flat(middle_ref)
    unit, inverse = standardize(middle)
    grad = flat(grad_ref)
    gates = flat(gates_ref)
    gate_cot = grad[:, width:]
    logit_grad = gates * (gate_cot - jnp.sum(gates * gate_cot, -1, keepdims=True))
    routed = (unit * norms_ref[2:3] + norms_ref[3:4]).astype(jnp.bfloat16)
    drouter_ref[...] += mm(routed.astype(jnp.float32), logit_grad, TN, HIGH)
    routed_grad = grad[:, :width] + mm(logit_grad, router_t_ref[...], NN, HIGH)
    dnorms_ref[2:3] += jnp.sum(routed_grad * unit, 0, keepdims=True)
    dnorms_ref[3:4] += jnp.sum(routed_grad, 0, keepdims=True)
    middle_grad = flat(cot_ref) + norm_back(routed_grad * norms_ref[2:3], unit, inverse)
    attn_cot = middle_grad.astype(jnp.bfloat16)
    joined = jnp.concatenate([mixed_ref[b].astype(jnp.float32) for b in range(images)], 0)
    joined = joined.astype(jnp.bfloat16)
    pieces, _, _, columns = mats_ref.shape
    spans = [slice(p * columns, (p + 1) * columns) for p in range(pieces)]
    for p in range(pieces):
        dmats_acc[p, 3] += mm(attn_cot, joined[:, spans[p]], TN)
    mixed_grad = jnp.concatenate([mm(attn_cot, mats_ref[p, 3]) for p in range(pieces)], 1)
    mixed_grad = mixed_grad.reshape(images, length, width)
    even = even_lanes((length, LANES))
    zero = jnp.zeros((), jnp.bfloat16)
    scale = jnp.bfloat16(HEAD ** -0.5)
    for b in range(images):
        bias = bias_ref[b]
        mixed_low = mixed_grad[b].astype(jnp.bfloat16)
        for pair in range(width // LANES):
            lanes = slice(pair * LANES, (pair + 1) * LANES)
            query = proj_ref[b, :, lanes] * scale
            keyed = proj_ref[b, :, width + pair * LANES:width + (pair + 1) * LANES]
            valued = proj_ref[b, :, 2 * width + pair * LANES:2 * width + (pair + 1) * LANES]
            out_cot = mixed_low[:, lanes]
            query_grad = keyed_grad = value_grad = None
            for odd in range(2):
                mask = even != bool(odd)
                query_half = jnp.where(mask, query, zero)
                keyed_half = jnp.where(mask, keyed, zero)
                cot_half = jnp.where(mask, out_cot, zero)
                scores = mm(query_half, keyed, NT) + bias
                lifted = jnp.exp(scores - jnp.max(scores, -1, keepdims=True))
                probs = lifted * (1.0 / jnp.sum(lifted, -1, keepdims=True))
                prob_grad = mm(cot_half, valued, NT)
                value_part = mm(probs.astype(jnp.bfloat16), cot_half, TN)
                inner = jnp.sum(probs * prob_grad, -1, keepdims=True)
                score_grad = (probs * (prob_grad - inner)).astype(jnp.bfloat16)
                query_part = mm(score_grad, keyed_half)
                keyed_part = mm(score_grad, query_half, TN)
                if odd:
                    query_grad, keyed_grad, value_grad = (
                        query_grad + query_part, keyed_grad + keyed_part, value_grad + value_part)
                else:
                    query_grad, keyed_grad, value_grad = query_part, keyed_part, value_part
            base = pair * LANES
            rows_here = slice(b * length, (b + 1) * length)
            dproj_ref[rows_here, base:base + LANES] = query_grad * (HEAD ** -0.5)
            dproj_ref[rows_here, width + base:width + base + LANES] = keyed_grad
            dproj_ref[rows_here, 2 * width + base:2 * width + base + LANES] = value_grad
    tok = flat(tok_ref)
    unit, inverse = standardize(tok)
    normed = (unit * norms_ref[0:1] + norms_ref[1:2]).astype(jnp.bfloat16)
    normed_grad = jnp.zeros((rows, width), jnp.float32)
    for c in range(3):
        part = dproj_ref[:, c * width:(c + 1) * width].astype(jnp.bfloat16)
        for p in range(pieces):
            dmats_acc[p, c] += mm(normed, part[:, spans[p]], TN)
            normed_grad += mm(part[:, spans[p]], mats_ref[p, c], NT)
    dnorms_ref[0:1] += jnp.sum(normed_grad * unit, 0, keepdims=True)
    dnorms_ref[1:2] += jnp.sum(normed_grad, 0, keepdims=True)
    input_grad = middle_grad + norm_back(normed_grad * norms_ref[0:1], unit, inverse)
    input_ref[...] = input_grad.reshape(images, length, width)

    @pl.when(step == pl.num_programs(0) - 1)
    def _():
        dmats_ref[...] = dmats_acc[...].astype(jnp.bfloat16)


def attention_backward(tok, middle, cot, grad, gates, proj, mixed, bias, mats, norms, router_t, per_step):
    images, length, width = tok.shape

    def rows(last):
        return pl.BlockSpec((per_step, length, last), lambda s: (s, 0, 0))

    def whole(shape):
        return pl.BlockSpec(shape, lambda s: (0,) * len(shape))

    return pl.pallas_call(
        backward_kernel,
        grid=(images // per_step,),
        in_specs=[
            rows(width), rows(width), rows(width), rows(width + LANES), rows(LANES),
            rows(3 * width), rows(width), pl.BlockSpec((per_step, 1, length), lambda s: (s, 0, 0)),
            whole(mats.shape), whole(norms.shape), whole(router_t.shape),
        ],
        out_specs=[
            rows(width), whole(mats.shape), whole((4, width)), whole((width, LANES)),
        ],
        out_shape=[
            jax.ShapeDtypeStruct((images, length, width), jnp.float32),
            jax.ShapeDtypeStruct(mats.shape, jnp.bfloat16),
            jax.ShapeDtypeStruct((4, width), jnp.float32),
            jax.ShapeDtypeStruct((width, LANES), jnp.float32),
        ],
        scratch_shapes=[
            pltpu.VMEM((per_step * length, 3 * width), jnp.float32),
            pltpu.VMEM(mats.shape, jnp.float32),
        ],
        compiler_params=pltpu.CompilerParams(vmem_limit_bytes=VMEM),
        cost_estimate=pl.CostEstimate(
            flops=images * length * width * width * 30, bytes_accessed=images * length * width * 30,
            transcendentals=images * length * length * 8),
        name="attention_backward",
    )(tok, middle, cot, grad, gates, proj, mixed, bias, mats, norms, router_t)


def expert_kernel(
    expert_ref, slots_ref, cots_ref, weights_ref, router_ref,
    result_ref, back_ref, dweights_ref,
    rows_t, grads_t, grads, gate_scr, result_acc, back_acc, first_acc, second_acc,
):
    count, width = slots_ref.shape
    tile = weights_ref.shape[-1]
    chunk = rows_t.shape[2]
    step = pl.program_id(0)
    first = weights_ref[:, :, 0, 0].reshape(width, tile)
    second = weights_ref[:, :, 0, 1].reshape(width, tile)

    @pl.when(step == 0)
    def _():
        def prepare(r, carry):
            here = pl.ds(pl.multiple_of(r * chunk, 16), chunk)
            slots = slots_ref[here]
            gates = router_gates(slots, router_ref[...])
            lane = lax.broadcasted_iota(jnp.int32, gates.shape, 1)
            gate = jnp.sum(jnp.where(lane == expert_ref[0], gates, 0.0), -1, keepdims=True)
            gate_scr[here] = jnp.broadcast_to(gate, gates.shape)
            low = (cots_ref[here].astype(jnp.float32) * gate).astype(jnp.bfloat16)
            grads[here] = low
            rows_t[r] = slots.T
            grads_t[r] = low.T
            result_acc[here] = jnp.zeros((chunk, width), jnp.float32)
            back_acc[here] = jnp.zeros((chunk, width), jnp.float32)
            return carry

        lax.fori_loop(0, count // chunk, prepare, 0)

    first_acc[...] = jnp.zeros_like(first_acc)
    second_acc[...] = jnp.zeros_like(second_acc)

    def work(r, carry):
        here = pl.ds(pl.multiple_of(r * chunk, 16), chunk)
        pre = mm(slots_ref[here], first)
        square = pre * pre
        half = 0.5 + 0.5 * jnp.tanh(pre * (GELU_C + (GELU_C * GELU_A) * square))
        hidden = (pre * half).astype(jnp.bfloat16)
        slope = half + 2.0 * half * (1.0 - half) * pre * (GELU_C + (3.0 * GELU_C * GELU_A) * square)
        hidden_grad = mm(grads[here], second)
        pre_grad = (hidden_grad * slope).astype(jnp.bfloat16)
        result_acc[here] += mm(hidden, second, NT)
        back_acc[here] += mm(pre_grad, first, NT)
        first_acc[...] += mm(rows_t[r], pre_grad)
        second_acc[...] += mm(grads_t[r], hidden)
        return carry

    lax.fori_loop(0, count // chunk, work, 0)
    block = weights_ref.shape[:2] + weights_ref.shape[4:]
    dweights_ref[:, :, 0, 0] = first_acc[...].astype(jnp.bfloat16).reshape(block)
    dweights_ref[:, :, 0, 1] = second_acc[...].astype(jnp.bfloat16).reshape(block)

    @pl.when(step == pl.num_programs(0) - 1)
    def _():
        def finish(r, carry):
            here = pl.ds(pl.multiple_of(r * chunk, 16), chunk)
            result = result_acc[here]
            gate = gate_scr[here][:, 0:1]
            result_ref[here] = (result * gate).astype(jnp.bfloat16)
            gate_grad = jnp.sum(cots_ref[here].astype(jnp.float32) * result, -1, keepdims=True)
            lane = lax.broadcasted_iota(jnp.int32, (chunk, LANES), 1)
            back_ref[here, 0:width] = back_acc[here].astype(jnp.bfloat16)
            back_ref[here, width:width + LANES] = jnp.where(
                lane == expert_ref[0], gate_grad, 0.0).astype(jnp.bfloat16)
            return carry

        lax.fori_loop(0, count // chunk, finish, 0)


def run_expert(expert, slots, cots, weights, router):
    count, width = slots.shape
    planes, inner, parts, _, depth, extent = weights.shape
    tile = min(512, extent)
    per_part = extent // tile
    chunk = 480

    def whole(shape):
        return pl.BlockSpec(shape, lambda s, e: (0,) * len(shape))

    weight_spec = pl.BlockSpec(
        (planes, inner, 1, 2, depth, tile), lambda s, e: (0, 0, s // per_part, 0, 0, s % per_part))
    return pl.pallas_call(
        expert_kernel,
        grid_spec=pltpu.PrefetchScalarGridSpec(
            num_scalar_prefetch=1,
            grid=(parts * per_part,),
            in_specs=[whole(slots.shape), whole(cots.shape), weight_spec, whole(router.shape)],
            out_specs=[whole((count, width)), whole((count, width + LANES)), weight_spec],
            scratch_shapes=[
                pltpu.VMEM((count // chunk, width, chunk), jnp.bfloat16),
                pltpu.VMEM((count // chunk, width, chunk), jnp.bfloat16),
                pltpu.VMEM((count, width), jnp.bfloat16),
                pltpu.VMEM((count, LANES), jnp.float32),
                pltpu.VMEM((count, width), jnp.float32),
                pltpu.VMEM((count, width), jnp.float32),
                pltpu.VMEM((width, tile), jnp.float32),
                pltpu.VMEM((width, tile), jnp.float32),
            ],
        ),
        out_shape=[
            jax.ShapeDtypeStruct((count, width), jnp.bfloat16),
            jax.ShapeDtypeStruct((count, width + LANES), jnp.bfloat16),
            jax.ShapeDtypeStruct(weights.shape, jnp.bfloat16),
        ],
        compiler_params=pltpu.CompilerParams(vmem_limit_bytes=VMEM),
        cost_estimate=pl.CostEstimate(
            flops=12 * count * width * extent * parts,
            bytes_accessed=4 * 2 * width * extent * parts + count * width * 8,
            transcendentals=count * extent * parts),
        name="expert",
    )(expert, slots, cots, weights, router)


def flipped(position, bit):
    return position + bit - 2 * bit * lax.rem(position // bit, 2)


def to_peer(source, target, sends, receives, where):
    return pltpu.make_async_remote_copy(
        src_ref=source, dst_ref=target, send_sem=sends, recv_sem=receives, device_id=where,
        device_id_type=pl.DeviceIdType.MESH)


class Dispatch:
    def __init__(self, index_ref, shared, staged, out, sends, receives, keep, inner, parts, local):
        self.index_ref, self.shared, self.staged, self.out = index_ref, shared, staged, out
        self.sends, self.receives, self.keep = sends, receives, keep
        self.inner, self.parts, self.local = inner, parts, local
        self.at_i, self.at_t = lax.axis_index("i"), lax.axis_index("t")

    def copy(self, m, d, k):
        home = lax.rem(self.at_i + d, self.inner)
        target = self.out.at[k, pl.ds(pl.multiple_of((m * self.inner + self.at_i) * CAP, 8), CAP)]
        return to_peer(self.staged.at[m, d, k], target, self.sends.at[m, d, k],
                       self.receives.at[m, d, k], {"i": home})

    def kept(self, m, k):
        target = self.out.at[k, pl.ds(pl.multiple_of((m * self.inner + self.at_i) * CAP, 8), CAP)]
        return pltpu.make_async_copy(self.staged.at[m, 0, k], target, self.keep.at[m, k])

    def fill(self, m, d):
        home = lax.rem(self.at_i + d, self.inner)
        count = self.local * CAP
        base = (home * self.parts + self.at_t) * count
        places = base + lax.broadcasted_iota(jnp.int32, (count, 1), 0)
        total = None
        for half in range(2):
            first = self.index_ref[m, 0, half:half + 1]
            second = self.index_ref[m, 1, half:half + 1]
            hits = jnp.where((first == places) | (second == places), 1.0, 0.0).astype(jnp.bfloat16)
            part = mm(hits, self.shared[m, half])
            total = part if total is None else total + part
        for k in range(self.local):
            self.staged[m, d, k] = total[k * CAP:(k + 1) * CAP].astype(jnp.bfloat16)

    def send(self, m):
        def step(d, carry):
            self.fill(m, d)
            for k in range(self.local):
                self.copy(m, d, k).start()
            return carry

        lax.fori_loop(1, self.inner, step, 0)
        self.fill(m, 0)
        for k in range(self.local):
            self.kept(m, k).start()

    def finish(self, m):
        def step(d, carry):
            for k in range(self.local):
                self.copy(m, d, k).wait()
            return carry

        lax.fori_loop(1, self.inner, step, 0)
        for k in range(self.local):
            self.kept(m, k).wait()


def spread_kernel(
    local, pack_ref, cot_ref, index_ref,
    mats_ref, norms_ref, parts_ref, router_ref, cots_ref,
    gathered, loose, shared, staged,
    load, ring_send, ring_recv, pair_send, pair_recv, slot_send, slot_recv, slot_keep,
):
    at_o, at_i, at_t = (lax.axis_index(name) for name in ("o", "i", "t"))
    micros = cot_ref.shape[0]
    pieces, kinds, width, columns = mats_ref.shape
    depth = width // 16
    fill = pltpu.make_async_copy(pack_ref, gathered.at[0], load)
    fill.start()
    stages = [
        {"t": 1 - at_t}, {"o": 1 - at_o}, {"i": flipped(at_i, 4)}, {"i": flipped(at_i, 2)},
        {"i": flipped(at_i, 1)},
    ]

    def stage(j):
        size = 2 ** j
        return to_peer(gathered.at[pl.ds(0, size)], gathered.at[pl.ds(size, size)],
                       ring_send.at[j], ring_recv.at[j], stages[j])

    def swap(m):
        return to_peer(shared.at[m, 0], shared.at[m, 1], pair_send.at[m], pair_recv.at[m],
                       {"t": 1 - at_t})

    plan = Dispatch(index_ref, shared, staged, cots_ref, slot_send, slot_recv, slot_keep, 8, 2, local)
    fill.wait()
    stage(0).start()
    for m in range(micros):
        shared[m, 0] = cot_ref[m].astype(jnp.bfloat16)
    stage(0).wait()
    stage(1).start()
    for m in range(micros):
        swap(m).start()
    stage(1).wait()
    stage(2).start()
    stage(2).wait()
    stage(3).start()
    stage(3).wait()
    stage(4).start()
    swap(0).wait()
    plan.send(0)
    stage(4).wait()

    def place(r, carry):
        o = flipped_if(at_o, 1, lax.rem(r // 2, 2))
        i = flipped_if(at_i, 4, lax.rem(r // 4, 2))
        i = flipped_if(i, 2, lax.rem(r // 8, 2))
        i = flipped_if(i, 1, lax.rem(r // 16, 2))
        t = flipped_if(at_t, 1, lax.rem(r, 2))
        row = pl.multiple_of((o * 8 + i) * depth, depth)
        for c in range(kinds):
            mats_ref[t, c, pl.ds(row, depth)] = gathered[r, c * depth:(c + 1) * depth]
        loose[(o * 8 + i) * 2 + t] = gathered[r, kinds * depth:, 0:LANES].astype(jnp.float32)
        return carry

    lax.fori_loop(0, gathered.shape[0], place, 0)
    turned = loose[...].reshape(width, LANES).T
    norms_ref[...] = turned[96:104] + turned[104:112] + turned[112:120]
    low = turned[0:96].astype(jnp.bfloat16)
    parts_ref[...] = jnp.concatenate([low, jnp.zeros((32, width), jnp.bfloat16)], 0)
    router_ref[0:32] = turned[0:32] + turned[32:64] + turned[64:96]
    router_ref[32:] = jnp.zeros((96, width), jnp.float32)
    for m in range(1, micros):
        swap(m).wait()
        plan.send(m)
    for m in range(micros):
        plan.finish(m)


def flipped_if(position, bit, on):
    return position + on * (bit - 2 * bit * lax.rem(position // bit, 2))


def spread(pack, cot, index, local):
    micros, own_rows, width = cot.shape
    columns = pack.shape[1]
    anywhere = pl.BlockSpec(memory_space=pl.ANY)
    vector = pl.BlockSpec(memory_space=pltpu.VMEM)
    dma = pltpu.SemaphoreType.DMA
    return pl.pallas_call(
        functools.partial(spread_kernel, local),
        in_specs=[anywhere, vector, vector],
        out_specs=[vector] * 4 + [anywhere],
        out_shape=[
            jax.ShapeDtypeStruct((2, 4, width, columns), jnp.bfloat16),
            jax.ShapeDtypeStruct((8, width), jnp.float32),
            jax.ShapeDtypeStruct((LANES, width), jnp.bfloat16),
            jax.ShapeDtypeStruct((LANES, width), jnp.float32),
            jax.ShapeDtypeStruct((local, micros * 8 * CAP, width), jnp.bfloat16),
        ],
        scratch_shapes=[
            pltpu.VMEM((32,) + pack.shape, jnp.bfloat16),
            pltpu.VMEM((32, width // 32, LANES), jnp.float32),
            pltpu.VMEM((micros, 2, own_rows, width), jnp.bfloat16),
            pltpu.VMEM((micros, 8, local, CAP, width), jnp.bfloat16),
            dma, dma((5,)), dma((5,)), dma((micros,)), dma((micros,)),
            dma((micros, 8, local)), dma((micros, 8, local)), dma((micros, local)),
        ],
        compiler_params=pltpu.CompilerParams(vmem_limit_bytes=VMEM, has_side_effects=True),
        cost_estimate=pl.CostEstimate(flops=1000, bytes_accessed=1000, transcendentals=0),
        name="spread",
    )(pack, cot, index)


def front_kernel(
    local, per_step, tok_ref, bias_ref, mats_ref, norms_ref, parts_ref, index_ref,
    middle_ref, proj_ref, mixed_ref, gates_ref, slots_ref,
    shared, staged, pair_send, pair_recv, slot_send, slot_recv, slot_keep,
):
    at_t = lax.axis_index("t")
    images, length, width = tok_ref.shape
    micros, _, own_rows, _ = shared.shape
    rows = per_step * length
    steps = own_rows // rows

    def swap(m, s):
        here = pl.ds(pl.multiple_of(s * rows, 16), rows)
        return to_peer(shared.at[m, 0, here], shared.at[m, 1, here], pair_send.at[m, s],
                       pair_recv.at[m, s], {"t": 1 - at_t})

    def attend(n, carry):
        m, s = n // steps, lax.rem(n, steps)
        _, low = forward_rows(n * per_step, per_step, tok_ref, bias_ref, mats_ref, norms_ref, parts_ref,
                              middle_ref, proj_ref, mixed_ref, gates_ref)
        shared[m, 0, pl.ds(pl.multiple_of(s * rows, 16), rows)] = low
        swap(m, s).start()
        return carry

    lax.fori_loop(0, micros * steps, attend, 0)
    plan = Dispatch(index_ref, shared, staged, slots_ref, slot_send, slot_recv, slot_keep, 8, 2, local)
    for m in range(micros):
        for s in range(steps):
            swap(m, s).wait()
        plan.send(m)
    for m in range(micros):
        plan.finish(m)


def front(tok, bias, mats, norms, parts, index, local, per_step):
    images, length, width = tok.shape
    micros, _, _, own_rows = index.shape
    steps = own_rows // (per_step * length)
    anywhere = pl.BlockSpec(memory_space=pl.ANY)
    vector = pl.BlockSpec(memory_space=pltpu.VMEM)
    dma = pltpu.SemaphoreType.DMA
    shapes = [(width, jnp.float32), (3 * width, jnp.bfloat16), (width, jnp.bfloat16), (LANES, jnp.float32)]
    return pl.pallas_call(
        functools.partial(front_kernel, local, per_step),
        in_specs=[vector] * 6,
        out_specs=[vector] * 4 + [anywhere],
        out_shape=[jax.ShapeDtypeStruct((images, length, n), kind) for n, kind in shapes] + [
            jax.ShapeDtypeStruct((local, micros * 8 * CAP, width), jnp.bfloat16)],
        scratch_shapes=[
            pltpu.VMEM((micros, 2, own_rows, width), jnp.bfloat16),
            pltpu.VMEM((micros, 8, local, CAP, width), jnp.bfloat16),
            dma((micros, steps)), dma((micros, steps)),
            dma((micros, 8, local)), dma((micros, 8, local)), dma((micros, local)),
        ],
        compiler_params=pltpu.CompilerParams(vmem_limit_bytes=VMEM, has_side_effects=True),
        cost_estimate=pl.CostEstimate(flops=1000, bytes_accessed=1000, transcendentals=0),
        name="front",
    )(tok, bias, mats, norms, parts, index)


def per_device(planes, inner, parts, tokens, key_mask, expert_ids, slot_ids, norm1_gain, norm1_bias,
               qkv_weight, out_weight, norm2_gain, norm2_bias, router_weight, expert_in, expert_out,
               cotangent):
    micros, own_rows, width = tokens.shape
    length = key_mask.shape[2]
    group_rows = own_rows * parts
    images = own_rows // length
    total = micros * images
    experts = expert_in.shape[0]
    homes = inner * parts
    local = experts // homes
    depth, extent = expert_in.shape[1:]
    small = norm1_gain.shape[0]
    every = ("o", "i", "t")
    plane_at, inner_at, part_at = (lax.axis_index(name) for name in every)
    low = jnp.bfloat16

    loose = jnp.concatenate([
        jnp.stack([norm1_gain, norm1_bias, norm2_gain, norm2_bias], 1), router_weight], 1)
    loose_count = 3 * loose.size
    columns = qkv_weight.shape[2]
    loose_rows = -(-loose_count // (16 * columns)) * 16
    loose_low = jnp.concatenate([p.reshape(-1) for p in three_parts(loose)])
    loose_low = jnp.pad(loose_low, (0, loose_rows * columns - loose_count)).reshape(loose_rows, columns)
    packed = jnp.concatenate([
        qkv_weight.transpose(1, 0, 2).reshape(3 * depth, columns), out_weight.T, loose_low], 0)
    gathered = lax.all_gather(packed, ("o", "i"), axis=0)
    gathered = lax.all_gather(gathered, "t", axis=0)
    mats = gathered[:, :, :4 * depth].reshape(parts, planes * inner, 4, depth, columns)
    mats = mats.transpose(2, 1, 3, 0, 4).reshape(1, 4, width, width)
    loose_all = gathered[:, :, 4 * depth:].reshape(parts, planes * inner, loose_rows * columns)
    loose_all = loose_all[:, :, :loose_count].astype(jnp.float32)
    loose_all = loose_all.reshape(parts, planes * inner, 3, small, 4 + experts)
    loose_all = (loose_all[:, :, 0] + loose_all[:, :, 1]) + loose_all[:, :, 2]
    loose_all = loose_all.transpose(1, 0, 2, 3).reshape(width, 4 + experts)
    norms = loose_all[:, :4].T
    router = jnp.pad(loose_all[:, 4:], ((0, 0), (0, LANES - experts)))
    router_parts = jnp.concatenate(three_parts(router[:, :experts]), 1).T
    router_parts = jnp.pad(router_parts, ((0, LANES - 3 * experts), (0, 0)))

    weights = []
    first_in = expert_in.reshape(homes, local, depth, extent)
    second_in = expert_out.transpose(0, 2, 1).reshape(homes, local, depth, extent)
    for k in range(local):
        both = jnp.stack([first_in[:, k], second_in[:, k]], 1)
        mine = lax.all_to_all(both, ("i", "t"), 0, 0, tiled=True)
        if planes == 2:
            other = lax.ppermute(mine, "o", [(0, 1), (1, 0)])
            full = jnp.where(plane_at == 0, jnp.stack([mine, other]), jnp.stack([other, mine]))
        else:
            full = lax.all_gather(mine, "o", axis=0)
        weights.append(full.reshape(planes, inner, parts, 2, depth, extent))

    own_first = part_at * own_rows
    slot_index = jnp.where(slot_ids >= 0, expert_ids * CAP + slot_ids, -1)
    if parts == 2:
        slot_index = jnp.concatenate([
            lax.dynamic_slice_in_dim(slot_index, own_first, own_rows, 1),
            lax.dynamic_slice_in_dim(slot_index, own_rows - own_first, own_rows, 1)], 1)
    homes_i = lax.broadcasted_iota(jnp.int32, (inner, local, CAP), 0)
    locals_i = lax.broadcasted_iota(jnp.int32, (inner, local, CAP), 1)
    cap_i = lax.broadcasted_iota(jnp.int32, (inner, local, CAP), 2)
    places = ((homes_i * parts + part_at) * local + locals_i) * CAP + cap_i

    def table(m, positions, rows=slice(None)):
        index = slot_index[m, rows]
        flat = positions.reshape(1, -1)
        return ((index[:, 0:1] == flat) | (index[:, 1:2] == flat)).astype(low)

    def share(rows):
        if parts == 2:
            return jnp.concatenate([rows, lax.ppermute(rows, "t", [(0, 1), (1, 0)])], 1)
        return lax.all_gather(rows, "t", axis=1, tiled=True)

    def dispatch(shared):
        sent = []
        for m in range(micros):
            slots = mm(table(m, places), shared[m], TN).astype(low)
            slots = lax.all_to_all(slots.reshape(inner, local * CAP, width), "i", 0, 0, tiled=True)
            sent.append(slots.reshape(inner, local, CAP, width))
        return [
            jnp.concatenate([s[:, k].reshape(inner * CAP, width) for s in sent], 0) for k in range(local)]

    cot_slots = dispatch(share(cotangent.astype(low)))

    flags = lax.dynamic_slice_in_dim(key_mask, part_at * images, images, 1).reshape(total, 1, length)
    bias = jnp.where(flags > 0, 0.0, -1e30).astype(jnp.float32)
    tok = tokens.reshape(total, length, width)
    per_step = 2 if total % 2 == 0 else 1
    middle, routed, proj, mixed, gates = attention_forward(tok, bias, mats, norms, router_parts, per_step)

    row_slots = dispatch(share(routed.reshape(micros, own_rows, width)))

    first_out, second_out, results, backs = [], [], [], []
    for k in range(local):
        expert = ((inner_at * parts + part_at) * local + k).astype(jnp.int32).reshape(1)
        result, back, dweights = run_expert(expert, row_slots[k], cot_slots[k], weights[k], router_parts)
        results.append(result.reshape(micros, inner, CAP, width))
        backs.append(back.reshape(micros, inner, CAP, width + LANES))
        dweights = dweights.reshape(planes, homes, 2, depth, extent)
        if planes == 2:
            theirs = lax.dynamic_index_in_dim(dweights, 1 - plane_at, 0, keepdims=False)
            ours = lax.dynamic_index_in_dim(dweights, plane_at, 0, keepdims=False)
            summed = ours.astype(jnp.float32) + lax.ppermute(
                theirs, "o", [(0, 1), (1, 0)]).astype(jnp.float32)
            summed = summed.astype(low)
        else:
            summed = lax.psum_scatter(dweights, "o", scatter_dimension=0, tiled=True)[0]
        final = lax.all_to_all(summed, ("i", "t"), 0, 0, tiled=True)
        first_out.append(final[:, 0])
        second_out.append(final[:, 1])
    first_grad = jnp.stack(first_out, 1).reshape(experts, depth, extent).astype(jnp.float32)
    second_grad = jnp.stack(second_out, 1).reshape(experts, depth, extent).astype(jnp.float32)
    second_grad = second_grad.transpose(0, 2, 1)

    def collect(values):
        size = values[0].shape[-1]
        answers = []
        for m in range(micros):
            back = jnp.stack([v[m] for v in values], 1).reshape(inner, local * CAP, size)
            back = lax.all_to_all(back, "i", 0, 0, tiled=True).reshape(inner * local * CAP, size)
            if parts == 2:
                away = mm(table(m, places, slice(own_rows, None)), back).astype(low)
                here = mm(table(m, places, slice(0, own_rows)), back)
                answers.append(here + lax.ppermute(away, "t", [(0, 1), (1, 0)]).astype(jnp.float32))
            else:
                whole = mm(table(m, places), back).astype(low)
                answers.append(lax.psum_scatter(
                    whole, "t", scatter_dimension=0, tiled=True).astype(jnp.float32))
        return jnp.stack(answers)

    grad = collect(backs)
    combined = collect(results)
    block_out = middle.reshape(micros, own_rows, width) + combined

    input_grad, dmats, dnorms, drouter = attention_backward(
        tok, middle, cotangent.reshape(total, length, width), grad.reshape(total, length, width + LANES),
        gates, proj, mixed, bias, mats, norms, router.T, per_step)
    input_grad = input_grad.reshape(micros, own_rows, width)

    dmats = dmats.reshape(4, planes, inner, depth, parts, columns).transpose(2, 4, 1, 0, 3, 5)
    dmats = dmats.reshape(homes, planes, 4 * depth, columns)
    dloose = jnp.concatenate([dnorms.T, drouter[:, :experts]], 1)
    dloose = dloose.reshape(planes, inner, parts, small * (4 + experts)).transpose(1, 2, 0, 3)
    dloose = jnp.concatenate(three_parts(dloose), -1)
    dloose = jnp.pad(dloose, ((0, 0),) * 3 + ((0, loose_rows * columns - loose_count),))
    dloose = dloose.reshape(homes, planes, loose_rows, columns)
    payload = jnp.concatenate([dmats, dloose], 2)
    payload = lax.all_to_all(payload, ("i", "t"), 0, 0, tiled=True)
    payload = jnp.sum(payload.astype(jnp.float32), 0)
    if planes == 2:
        theirs = lax.dynamic_index_in_dim(payload, 1 - plane_at, 0, keepdims=False)
        ours = lax.dynamic_index_in_dim(payload, plane_at, 0, keepdims=False)
        reduced = ours + lax.ppermute(theirs, "o", [(0, 1), (1, 0)])
    else:
        reduced = lax.psum_scatter(payload, "o", scatter_dimension=0, tiled=True)[0]
    matrices = reduced[:4 * depth].reshape(4, depth, columns)
    qkv_grad = matrices[:3].transpose(1, 0, 2)
    out_grad = matrices[3].T
    tail = reduced[4 * depth:].reshape(-1)[:loose_count].reshape(3, small, 4 + experts)
    tail = (tail[0] + tail[1]) + tail[2]
    return (
        block_out, input_grad, tail[:, 0], tail[:, 1], qkv_grad, out_grad, tail[:, 2], tail[:, 3],
        tail[:, 4:], first_grad, second_grad,
    )


def per_device_halves(tokens, key_mask, expert_ids, slot_ids, norm1_gain, norm1_bias,
                      qkv_weight, out_weight, norm2_gain, norm2_bias, router_weight, expert_in, expert_out,
                      cotangent):
    micros, own_rows, width = tokens.shape
    length = key_mask.shape[2]
    images = own_rows // length
    total = micros * images
    planes, inner, parts = 2, 8, 2
    experts = expert_in.shape[0]
    homes = inner * parts
    local = experts // homes
    depth, extent = expert_in.shape[1:]
    columns = qkv_weight.shape[2]
    plane_at, inner_at, part_at = (lax.axis_index(name) for name in ("o", "i", "t"))
    low = jnp.bfloat16
    across = [(0, 1), (1, 0)]

    first_in = expert_in.reshape(homes, local, depth, extent)
    second_in = expert_out.transpose(0, 2, 1).reshape(homes, local, depth, extent)
    weights = []
    for k in range(local):
        both = jnp.stack([first_in[:, k], second_in[:, k]], 1)
        mine = lax.all_to_all(both, ("i", "t"), 0, 0, tiled=True)
        other = lax.ppermute(mine, "o", across)
        full = jnp.where(plane_at == 0, jnp.stack([mine, other]), jnp.stack([other, mine]))
        weights.append(full.reshape(planes, inner, parts, 2, depth, extent))

    norms_in = jnp.stack([norm1_gain, norm1_bias, norm2_gain, norm2_bias], 1)
    loose = [p for p in three_parts(router_weight)]
    loose += [jnp.pad(p, ((0, 0), (0, 4))) for p in three_parts(norms_in)]
    loose = jnp.concatenate(loose, 1)
    loose = jnp.pad(loose, ((0, 0), (0, columns - loose.shape[1])))
    packed = jnp.concatenate([
        qkv_weight.transpose(1, 0, 2).reshape(3 * depth, columns), out_weight.T, loose], 0)
    slot_index = jnp.where(slot_ids >= 0, expert_ids * CAP + slot_ids, -1).transpose(0, 2, 1)
    own_first = part_at * own_rows
    index = jnp.stack([
        lax.dynamic_slice_in_dim(slot_index, own_first, own_rows, 2),
        lax.dynamic_slice_in_dim(slot_index, own_rows - own_first, own_rows, 2)], 2)
    mats, norms, router_parts, router_t, cot_slots = spread(packed, cotangent, index, local)

    flags = lax.dynamic_slice_in_dim(key_mask, part_at * images, images, 1).reshape(total, 1, length)
    bias = jnp.where(flags > 0, 0.0, -1e30).astype(jnp.float32)
    tok = tokens.reshape(total, length, width)
    middle, proj, mixed, gates, row_slots = front(tok, bias, mats, norms, router_parts, index, local, 2)

    results, backs, finals = [], [], []
    for k in range(local):
        expert = ((inner_at * parts + part_at) * local + k).astype(jnp.int32).reshape(1)
        result, back, dweights = run_expert(expert, row_slots[k], cot_slots[k], weights[k], router_parts)
        results.append(result.reshape(micros, inner, CAP, width))
        backs.append(back.reshape(micros, inner, CAP, width + LANES))
        dweights = dweights.reshape(planes, homes, 2, depth, extent)
        theirs = lax.dynamic_index_in_dim(dweights, 1 - plane_at, 0, keepdims=False)
        ours = lax.dynamic_index_in_dim(dweights, plane_at, 0, keepdims=False)
        summed = ours.astype(jnp.float32) + lax.ppermute(theirs, "o", across).astype(jnp.float32)
        finals.append(lax.all_to_all(summed.astype(low), ("i", "t"), 0, 0, tiled=True))
    first_grad = jnp.stack([f[:, 0] for f in finals], 1).reshape(experts, depth, extent)
    second_grad = jnp.stack([f[:, 1] for f in finals], 1).reshape(experts, depth, extent)
    first_grad = first_grad.astype(jnp.float32)
    second_grad = second_grad.astype(jnp.float32).transpose(0, 2, 1)

    homes_i = lax.broadcasted_iota(jnp.int32, (inner, local, CAP), 0)
    locals_i = lax.broadcasted_iota(jnp.int32, (inner, local, CAP), 1)
    cap_i = lax.broadcasted_iota(jnp.int32, (inner, local, CAP), 2)
    places = (((homes_i * parts + part_at) * local + locals_i) * CAP + cap_i).reshape(1, -1)

    def table(m, half):
        first, second = index[m, 0, half][:, None], index[m, 1, half][:, None]
        return ((first == places) | (second == places)).astype(low)

    def collect(values):
        size = values[0].shape[-1]
        answers = []
        for m in range(micros):
            back = jnp.stack([v[m] for v in values], 1).reshape(inner, local * CAP, size)
            back = lax.all_to_all(back, "i", 0, 0, tiled=True).reshape(inner * local * CAP, size)
            away = mm(table(m, 1), back).astype(low)
            here = mm(table(m, 0), back)
            answers.append(here + lax.ppermute(away, "t", across).astype(jnp.float32))
        return jnp.stack(answers)

    grad = collect(backs)
    combined = collect(results)
    block_out = middle.reshape(micros, own_rows, width) + combined

    input_grad, dmats, dnorms, drouter = attention_backward(
        tok, middle, cotangent.reshape(total, length, width), grad.reshape(total, length, width + LANES),
        gates, proj, mixed, bias, mats, norms, router_t, 2)
    input_grad = input_grad.reshape(micros, own_rows, width)

    small = norm1_gain.shape[0]
    loose_count = 3 * small * (4 + experts)
    loose_rows = -(-loose_count // (16 * columns)) * 16
    dmats = dmats.reshape(parts, 4, planes, inner, depth, columns).transpose(3, 0, 2, 1, 4, 5)
    dmats = dmats.reshape(homes, planes, 4 * depth, columns)
    dloose = jnp.concatenate([dnorms.T, drouter[:, :experts]], 1)
    dloose = dloose.reshape(planes, inner, parts, small * (4 + experts)).transpose(1, 2, 0, 3)
    dloose = jnp.concatenate(three_parts(dloose), -1)
    dloose = jnp.pad(dloose, ((0, 0),) * 3 + ((0, loose_rows * columns - loose_count),))
    dloose = dloose.reshape(homes, planes, loose_rows, columns)
    payload = jnp.concatenate([dmats, dloose], 2)
    payload = lax.all_to_all(payload, ("i", "t"), 0, 0, tiled=True)
    payload = jnp.sum(payload.astype(jnp.float32), 0)
    theirs = lax.dynamic_index_in_dim(payload, 1 - plane_at, 0, keepdims=False)
    ours = lax.dynamic_index_in_dim(payload, plane_at, 0, keepdims=False)
    reduced = ours + lax.ppermute(theirs, "o", across)
    matrices = reduced[:4 * depth].reshape(4, depth, columns)
    qkv_grad = matrices[:3].transpose(1, 0, 2)
    out_grad = matrices[3].T
    tail = reduced[4 * depth:].reshape(-1)[:loose_count].reshape(3, small, 4 + experts)
    tail = (tail[0] + tail[1]) + tail[2]
    return (
        block_out, input_grad, tail[:, 0], tail[:, 1], qkv_grad, out_grad, tail[:, 2], tail[:, 3],
        tail[:, 4:], first_grad, second_grad,
    )


def solution(mesh):
    dp, parts = mesh.shape["dp"], mesh.shape["tensor"]
    inner = min(8, 32 // parts, dp)
    planes = dp // inner
    fine = Mesh(mesh.devices.reshape(planes, inner, parts), ("o", "i", "t"))
    dps = ("o", "i")
    every = ("o", "i", "t")
    rows = P(None, every, None)
    step = functools.partial(per_device, planes, inner, parts)
    if (planes, inner, parts) == (2, 8, 2):
        step = per_device_halves
    return jax.shard_map(
        step,
        mesh=fine,
        in_specs=(
            rows, P(None, dps, None), P(None, dps, None), P(None, dps, None), P(every), P(every),
            P(dps, None, "t"), P("t", dps), P(every), P(every), P(every, None),
            P(None, dps, "t"), P(None, "t", dps), rows,
        ),
        out_specs=(
            rows, rows, P(every), P(every), P(dps, None, "t"), P("t", dps), P(every), P(every),
            P(every, None), P(None, dps, "t"), P(None, "t", dps),
        ),
        check_vma=False,
    )
```

```python
import functools

import jax
import jax.numpy as jnp
from jax import lax
from jax.experimental import pallas as pl
from jax.experimental.pallas import tpu as pltpu
from jax.sharding import Mesh, PartitionSpec as P

HEAD = 64
CAP = 120
EPSILON = 1e-06
LANES = 128
VMEM = 60 * 1024 * 1024
NN = (((1,), (0,)), ((), ()))
NT = (((1,), (1,)), ((), ()))
TN = (((0,), (0,)), ((), ()))
HIGH = lax.Precision.HIGHEST
GELU_C = 0.7978845608028654
GELU_A = 0.044715


def mm(a, b, dims=NN, precision=None):
    return lax.dot_general(a, b, dims, precision=precision, preferred_element_type=jnp.float32)


def three_parts(value):
    high = value.astype(jnp.bfloat16)
    rest = value - high.astype(jnp.float32)
    middle = rest.astype(jnp.bfloat16)
    last = (rest - middle.astype(jnp.float32)).astype(jnp.bfloat16)
    return high, middle, last


def standardize(values):
    center = jnp.mean(values, -1, keepdims=True)
    shifted = values - center
    spread = jnp.mean(shifted * shifted, -1, keepdims=True)
    inverse = lax.rsqrt(spread + EPSILON)
    return shifted * inverse, inverse


def norm_back(grad, unit, inverse):
    return inverse * (
        grad
        - jnp.mean(grad, -1, keepdims=True)
        - unit * jnp.mean(grad * unit, -1, keepdims=True)
    )


def even_lanes(shape):
    return lax.broadcasted_iota(jnp.int32, shape, 1) < HEAD


def router_gates(routed, parts):
    logits = mm(routed, parts, NT)
    logits = logits + pltpu.roll(logits, LANES - 32, 1) + pltpu.roll(logits, LANES - 64, 1)
    lane = lax.broadcasted_iota(jnp.int32, logits.shape, 1)
    logits = jnp.where(lane < 32, logits, -1e30)
    lifted = jnp.exp(logits - jnp.max(logits, -1, keepdims=True))
    return lifted / jnp.sum(lifted, -1, keepdims=True)


def forward_rows(first, images, tok_ref, bias_ref, mats_ref, norms_ref, parts_ref,
                 middle_ref, proj_ref, mixed_ref, gates_ref):
    _, length, width = tok_ref.shape
    pieces, _, _, columns = mats_ref.shape
    rows = images * length
    here = pl.ds(first, images)
    tok = tok_ref[here].reshape(rows, width)
    unit, _ = standardize(tok)
    normed = (unit * norms_ref[0:1] + norms_ref[1:2]).astype(jnp.bfloat16)
    for c in range(3):
        for p in range(pieces):
            part = mm(normed, mats_ref[p, c]).reshape(images, length, columns)
            base = c * width + p * columns
            for b in range(images):
                proj_ref[first + b, :, base:base + columns] = part[b].astype(jnp.bfloat16)
    even = even_lanes((length, LANES))
    scale = jnp.bfloat16(HEAD ** -0.5)
    zero = jnp.zeros((), jnp.bfloat16)
    attended = []
    for b in range(images):
        bias = bias_ref[first + b]
        parts = []
        for pair in range(width // LANES):
            lanes = slice(pair * LANES, (pair + 1) * LANES)
            query = proj_ref[first + b, :, lanes] * scale
            keyed = proj_ref[first + b, :, width + pair * LANES:width + (pair + 1) * LANES]
            valued = proj_ref[first + b, :, 2 * width + pair * LANES:2 * width + (pair + 1) * LANES]
            halves = []
            for odd in range(2):
                chosen = jnp.where(even != bool(odd), query, zero)
                scores = mm(chosen, keyed, NT) + bias
                lifted = jnp.exp(scores - jnp.max(scores, -1, keepdims=True))
                probs = lifted * (1.0 / jnp.sum(lifted, -1, keepdims=True))
                halves.append(mm(probs.astype(jnp.bfloat16), valued))
            both = jnp.where(even, halves[0], halves[1])
            mixed_ref[first + b, :, lanes] = both.astype(jnp.bfloat16)
            parts.append(both)
        attended.append(jnp.concatenate(parts, 1))
    joined = jnp.concatenate(attended, 0).astype(jnp.bfloat16)
    middle = tok
    for p in range(pieces):
        middle += mm(joined[:, p * columns:(p + 1) * columns], mats_ref[p, 3], NT)
    middle_ref[here] = middle.reshape(images, length, width)
    unit, _ = standardize(middle)
    routed = unit * norms_ref[2:3] + norms_ref[3:4]
    low = routed.astype(jnp.bfloat16)
    gates_ref[here] = router_gates(low, parts_ref[...]).reshape(images, length, LANES)
    return routed, low


def forward_kernel(
    tok_ref, bias_ref, mats_ref, norms_ref, parts_ref,
    middle_ref, routed_ref, proj_ref, mixed_ref, gates_ref,
):
    images, length, width = tok_ref.shape
    routed, _ = forward_rows(0, images, tok_ref, bias_ref, mats_ref, norms_ref, parts_ref,
                             middle_ref, proj_ref, mixed_ref, gates_ref)
    routed_ref[...] = routed.reshape(images, length, width).astype(jnp.bfloat16)


def attention_forward(tok, bias, mats, norms, router, per_step):
    images, length, width = tok.shape

    def rows(last):
        return pl.BlockSpec((per_step, length, last), lambda s: (s, 0, 0))

    def whole(a):
        return pl.BlockSpec(a.shape, lambda s: (0,) * a.ndim)

    shapes = [
        (width, jnp.float32), (width, jnp.bfloat16), (3 * width, jnp.bfloat16),
        (width, jnp.bfloat16), (LANES, jnp.float32),
    ]
    return pl.pallas_call(
        forward_kernel,
        grid=(images // per_step,),
        in_specs=[
            rows(width), pl.BlockSpec((per_step, 1, length), lambda s: (s, 0, 0)),
            whole(mats), whole(norms), whole(router),
        ],
        out_specs=[rows(n) for n, _ in shapes],
        out_shape=[jax.ShapeDtypeStruct((images, length, n), kind) for n, kind in shapes],
        compiler_params=pltpu.CompilerParams(vmem_limit_bytes=VMEM),
        cost_estimate=pl.CostEstimate(
            flops=images * length * width * width * 10, bytes_accessed=images * length * width * 16,
            transcendentals=images * length * length * 8),
        name="attention_forward",
    )(tok, bias, mats, norms, router)


def backward_rows(first, images, grad, tok_ref, middle_ref, cot_ref, gates_ref, proj_ref, mixed_ref,
                  bias_ref, mats_ref, norms_ref, router_t_ref,
                  input_ref, dnorms_ref, drouter_ref, dproj_ref, dmats_acc):
    _, length, width = tok_ref.shape
    rows = images * length
    here = pl.ds(first, images)

    def flat(ref):
        return ref[here].reshape(rows, ref.shape[2])

    middle = flat(middle_ref)
    unit, inverse = standardize(middle)
    gates = flat(gates_ref)
    gate_cot = grad[:, width:]
    logit_grad = gates * (gate_cot - jnp.sum(gates * gate_cot, -1, keepdims=True))
    routed = (unit * norms_ref[2:3] + norms_ref[3:4]).astype(jnp.bfloat16)
    drouter_ref[...] += mm(routed.astype(jnp.float32), logit_grad, TN, HIGH)
    routed_grad = grad[:, :width] + mm(logit_grad, router_t_ref[...], NN, HIGH)
    dnorms_ref[2:3] += jnp.sum(routed_grad * unit, 0, keepdims=True)
    dnorms_ref[3:4] += jnp.sum(routed_grad, 0, keepdims=True)
    middle_grad = flat(cot_ref) + norm_back(routed_grad * norms_ref[2:3], unit, inverse)
    attn_cot = middle_grad.astype(jnp.bfloat16)
    joined = jnp.concatenate([mixed_ref[first + b].astype(jnp.float32) for b in range(images)], 0)
    joined = joined.astype(jnp.bfloat16)
    pieces, _, _, columns = mats_ref.shape
    spans = [slice(p * columns, (p + 1) * columns) for p in range(pieces)]
    for p in range(pieces):
        dmats_acc[p, 3] += mm(attn_cot, joined[:, spans[p]], TN)
    mixed_grad = jnp.concatenate([mm(attn_cot, mats_ref[p, 3]) for p in range(pieces)], 1)
    mixed_grad = mixed_grad.reshape(images, length, width)
    even = even_lanes((length, LANES))
    zero = jnp.zeros((), jnp.bfloat16)
    scale = jnp.bfloat16(HEAD ** -0.5)
    for b in range(images):
        bias = bias_ref[first + b]
        mixed_low = mixed_grad[b].astype(jnp.bfloat16)
        for pair in range(width // LANES):
            lanes = slice(pair * LANES, (pair + 1) * LANES)
            query = proj_ref[first + b, :, lanes] * scale
            keyed = proj_ref[first + b, :, width + pair * LANES:width + (pair + 1) * LANES]
            valued = proj_ref[first + b, :, 2 * width + pair * LANES:2 * width + (pair + 1) * LANES]
            out_cot = mixed_low[:, lanes]
            query_grad = keyed_grad = value_grad = None
            for odd in range(2):
                mask = even != bool(odd)
                query_half = jnp.where(mask, query, zero)
                keyed_half = jnp.where(mask, keyed, zero)
                cot_half = jnp.where(mask, out_cot, zero)
                scores = mm(query_half, keyed, NT) + bias
                lifted = jnp.exp(scores - jnp.max(scores, -1, keepdims=True))
                probs = lifted * (1.0 / jnp.sum(lifted, -1, keepdims=True))
                prob_grad = mm(cot_half, valued, NT)
                value_part = mm(probs.astype(jnp.bfloat16), cot_half, TN)
                inner = jnp.sum(probs * prob_grad, -1, keepdims=True)
                score_grad = (probs * (prob_grad - inner)).astype(jnp.bfloat16)
                query_part = mm(score_grad, keyed_half)
                keyed_part = mm(score_grad, query_half, TN)
                if odd:
                    query_grad, keyed_grad, value_grad = (
                        query_grad + query_part, keyed_grad + keyed_part, value_grad + value_part)
                else:
                    query_grad, keyed_grad, value_grad = query_part, keyed_part, value_part
            base = pair * LANES
            rows_here = slice(b * length, (b + 1) * length)
            dproj_ref[rows_here, base:base + LANES] = query_grad * (HEAD ** -0.5)
            dproj_ref[rows_here, width + base:width + base + LANES] = keyed_grad
            dproj_ref[rows_here, 2 * width + base:2 * width + base + LANES] = value_grad
    tok = flat(tok_ref)
    unit, inverse = standardize(tok)
    normed = (unit * norms_ref[0:1] + norms_ref[1:2]).astype(jnp.bfloat16)
    normed_grad = jnp.zeros((rows, width), jnp.float32)
    for c in range(3):
        part = dproj_ref[:, c * width:(c + 1) * width].astype(jnp.bfloat16)
        for p in range(pieces):
            dmats_acc[p, c] += mm(normed, part[:, spans[p]], TN)
            normed_grad += mm(part[:, spans[p]], mats_ref[p, c], NT)
    dnorms_ref[0:1] += jnp.sum(normed_grad * unit, 0, keepdims=True)
    dnorms_ref[1:2] += jnp.sum(normed_grad, 0, keepdims=True)
    input_grad = middle_grad + norm_back(normed_grad * norms_ref[0:1], unit, inverse)
    input_ref[here] = input_grad.reshape(images, length, width)


def backward_kernel(
    tok_ref, middle_ref, cot_ref, grad_ref, gates_ref, proj_ref, mixed_ref,
    bias_ref, mats_ref, norms_ref, router_t_ref,
    input_ref, dmats_ref, dnorms_ref, drouter_ref,
    dproj_ref, dmats_acc,
):
    images, length, width = tok_ref.shape
    rows = images * length
    step = pl.program_id(0)

    @pl.when(step == 0)
    def _():
        dmats_acc[...] = jnp.zeros_like(dmats_acc)
        dnorms_ref[...] = jnp.zeros_like(dnorms_ref)
        drouter_ref[...] = jnp.zeros_like(drouter_ref)

    backward_rows(0, images, grad_ref[...].reshape(rows, grad_ref.shape[2]), tok_ref, middle_ref, cot_ref,
                  gates_ref, proj_ref, mixed_ref, bias_ref, mats_ref, norms_ref, router_t_ref,
                  input_ref, dnorms_ref, drouter_ref, dproj_ref, dmats_acc)

    @pl.when(step == pl.num_programs(0) - 1)
    def _():
        dmats_ref[...] = dmats_acc[...].astype(jnp.bfloat16)


def attention_backward(tok, middle, cot, grad, gates, proj, mixed, bias, mats, norms, router_t, per_step):
    images, length, width = tok.shape

    def rows(last):
        return pl.BlockSpec((per_step, length, last), lambda s: (s, 0, 0))

    def whole(shape):
        return pl.BlockSpec(shape, lambda s: (0,) * len(shape))

    return pl.pallas_call(
        backward_kernel,
        grid=(images // per_step,),
        in_specs=[
            rows(width), rows(width), rows(width), rows(width + LANES), rows(LANES),
            rows(3 * width), rows(width), pl.BlockSpec((per_step, 1, length), lambda s: (s, 0, 0)),
            whole(mats.shape), whole(norms.shape), whole(router_t.shape),
        ],
        out_specs=[
            rows(width), whole(mats.shape), whole((4, width)), whole((width, LANES)),
        ],
        out_shape=[
            jax.ShapeDtypeStruct((images, length, width), jnp.float32),
            jax.ShapeDtypeStruct(mats.shape, jnp.bfloat16),
            jax.ShapeDtypeStruct((4, width), jnp.float32),
            jax.ShapeDtypeStruct((width, LANES), jnp.float32),
        ],
        scratch_shapes=[
            pltpu.VMEM((per_step * length, 3 * width), jnp.float32),
            pltpu.VMEM(mats.shape, jnp.float32),
        ],
        compiler_params=pltpu.CompilerParams(vmem_limit_bytes=VMEM),
        cost_estimate=pl.CostEstimate(
            flops=images * length * width * width * 30, bytes_accessed=images * length * width * 30,
            transcendentals=images * length * length * 8),
        name="attention_backward",
    )(tok, middle, cot, grad, gates, proj, mixed, bias, mats, norms, router_t)


def expert_kernel(
    expert_ref, slots_ref, cots_ref, weights_ref, router_ref,
    result_ref, back_ref, dweights_ref,
    rows_t, grads_t, grads, gate_scr, result_acc, back_acc, first_acc, second_acc,
):
    count, width = slots_ref.shape
    tile = weights_ref.shape[-1]
    chunk = rows_t.shape[2]
    step = pl.program_id(0)
    first = weights_ref[:, :, 0, 0].reshape(width, tile)
    second = weights_ref[:, :, 0, 1].reshape(width, tile)

    @pl.when(step == 0)
    def _():
        def prepare(r, carry):
            here = pl.ds(pl.multiple_of(r * chunk, 16), chunk)
            slots = slots_ref[here]
            gates = router_gates(slots, router_ref[...])
            lane = lax.broadcasted_iota(jnp.int32, gates.shape, 1)
            gate = jnp.sum(jnp.where(lane == expert_ref[0], gates, 0.0), -1, keepdims=True)
            gate_scr[here] = jnp.broadcast_to(gate, gates.shape)
            low = (cots_ref[here].astype(jnp.float32) * gate).astype(jnp.bfloat16)
            grads[here] = low
            rows_t[r] = slots.T
            grads_t[r] = low.T
            result_acc[here] = jnp.zeros((chunk, width), jnp.float32)
            back_acc[here] = jnp.zeros((chunk, width), jnp.float32)
            return carry

        lax.fori_loop(0, count // chunk, prepare, 0)

    first_acc[...] = jnp.zeros_like(first_acc)
    second_acc[...] = jnp.zeros_like(second_acc)

    def work(r, carry):
        here = pl.ds(pl.multiple_of(r * chunk, 16), chunk)
        pre = mm(slots_ref[here], first)
        square = pre * pre
        half = 0.5 + 0.5 * jnp.tanh(pre * (GELU_C + (GELU_C * GELU_A) * square))
        hidden = (pre * half).astype(jnp.bfloat16)
        slope = half + 2.0 * half * (1.0 - half) * pre * (GELU_C + (3.0 * GELU_C * GELU_A) * square)
        hidden_grad = mm(grads[here], second)
        pre_grad = (hidden_grad * slope).astype(jnp.bfloat16)
        result_acc[here] += mm(hidden, second, NT)
        back_acc[here] += mm(pre_grad, first, NT)
        first_acc[...] += mm(rows_t[r], pre_grad)
        second_acc[...] += mm(grads_t[r], hidden)
        return carry

    lax.fori_loop(0, count // chunk, work, 0)
    block = weights_ref.shape[:2] + weights_ref.shape[4:]
    dweights_ref[:, :, 0, 0] = first_acc[...].astype(jnp.bfloat16).reshape(block)
    dweights_ref[:, :, 0, 1] = second_acc[...].astype(jnp.bfloat16).reshape(block)

    @pl.when(step == pl.num_programs(0) - 1)
    def _():
        def finish(r, carry):
            here = pl.ds(pl.multiple_of(r * chunk, 16), chunk)
            result = result_acc[here]
            gate = gate_scr[here][:, 0:1]
            result_ref[here] = (result * gate).astype(jnp.bfloat16)
            gate_grad = jnp.sum(cots_ref[here].astype(jnp.float32) * result, -1, keepdims=True)
            lane = lax.broadcasted_iota(jnp.int32, (chunk, LANES), 1)
            back_ref[here, 0:width] = back_acc[here].astype(jnp.bfloat16)
            back_ref[here, width:width + LANES] = jnp.where(
                lane == expert_ref[0], gate_grad, 0.0).astype(jnp.bfloat16)
            return carry

        lax.fori_loop(0, count // chunk, finish, 0)


def run_expert(expert, slots, cots, weights, router):
    count, width = slots.shape
    planes, inner, parts, _, depth, extent = weights.shape
    tile = min(512, extent)
    per_part = extent // tile
    chunk = 480

    def whole(shape):
        return pl.BlockSpec(shape, lambda s, e: (0,) * len(shape))

    weight_spec = pl.BlockSpec(
        (planes, inner, 1, 2, depth, tile), lambda s, e: (0, 0, s // per_part, 0, 0, s % per_part))
    return pl.pallas_call(
        expert_kernel,
        grid_spec=pltpu.PrefetchScalarGridSpec(
            num_scalar_prefetch=1,
            grid=(parts * per_part,),
            in_specs=[whole(slots.shape), whole(cots.shape), weight_spec, whole(router.shape)],
            out_specs=[whole((count, width)), whole((count, width + LANES)), weight_spec],
            scratch_shapes=[
                pltpu.VMEM((count // chunk, width, chunk), jnp.bfloat16),
                pltpu.VMEM((count // chunk, width, chunk), jnp.bfloat16),
                pltpu.VMEM((count, width), jnp.bfloat16),
                pltpu.VMEM((count, LANES), jnp.float32),
                pltpu.VMEM((count, width), jnp.float32),
                pltpu.VMEM((count, width), jnp.float32),
                pltpu.VMEM((width, tile), jnp.float32),
                pltpu.VMEM((width, tile), jnp.float32),
            ],
        ),
        out_shape=[
            jax.ShapeDtypeStruct((count, width), jnp.bfloat16),
            jax.ShapeDtypeStruct((count, width + LANES), jnp.bfloat16),
            jax.ShapeDtypeStruct(weights.shape, jnp.bfloat16),
        ],
        compiler_params=pltpu.CompilerParams(vmem_limit_bytes=VMEM),
        cost_estimate=pl.CostEstimate(
            flops=12 * count * width * extent * parts,
            bytes_accessed=4 * 2 * width * extent * parts + count * width * 8,
            transcendentals=count * extent * parts),
        name="expert",
    )(expert, slots, cots, weights, router)


def flipped(position, bit):
    return position + bit - 2 * bit * lax.rem(position // bit, 2)


def to_peer(source, target, sends, receives, where):
    return pltpu.make_async_remote_copy(
        src_ref=source, dst_ref=target, send_sem=sends, recv_sem=receives, device_id=where,
        device_id_type=pl.DeviceIdType.MESH)


class Dispatch:
    def __init__(self, index_ref, shared, staged, out, sends, receives, keep, inner, parts, local):
        self.index_ref, self.shared, self.staged, self.out = index_ref, shared, staged, out
        self.sends, self.receives, self.keep = sends, receives, keep
        self.inner, self.parts, self.local = inner, parts, local
        self.at_i, self.at_t = lax.axis_index("i"), lax.axis_index("t")

    def copy(self, m, d, k):
        home = lax.rem(self.at_i + d, self.inner)
        target = self.out.at[k, pl.ds(pl.multiple_of((m * self.inner + self.at_i) * CAP, 8), CAP)]
        return to_peer(self.staged.at[m, d, k], target, self.sends.at[m, d, k],
                       self.receives.at[m, d, k], {"i": home})

    def kept(self, m, k):
        target = self.out.at[k, pl.ds(pl.multiple_of((m * self.inner + self.at_i) * CAP, 8), CAP)]
        return pltpu.make_async_copy(self.staged.at[m, 0, k], target, self.keep.at[m, k])

    def fill(self, m, d):
        home = lax.rem(self.at_i + d, self.inner)
        count = self.local * CAP
        base = (home * self.parts + self.at_t) * count
        places = base + lax.broadcasted_iota(jnp.int32, (count, 1), 0)
        total = None
        for half in range(2):
            first = self.index_ref[m, 0, half:half + 1]
            second = self.index_ref[m, 1, half:half + 1]
            hits = jnp.where((first == places) | (second == places), 1.0, 0.0).astype(jnp.bfloat16)
            part = mm(hits, self.shared[m, half])
            total = part if total is None else total + part
        for k in range(self.local):
            self.staged[m, d, k] = total[k * CAP:(k + 1) * CAP].astype(jnp.bfloat16)

    def send(self, m):
        def step(d, carry):
            self.fill(m, d)
            for k in range(self.local):
                self.copy(m, d, k).start()
            return carry

        lax.fori_loop(1, self.inner, step, 0)
        self.fill(m, 0)
        for k in range(self.local):
            self.kept(m, k).start()

    def finish(self, m):
        def step(d, carry):
            for k in range(self.local):
                self.copy(m, d, k).wait()
            return carry

        lax.fori_loop(1, self.inner, step, 0)
        for k in range(self.local):
            self.kept(m, k).wait()


def flipped_if(position, bit, on):
    return position + on * (bit - 2 * bit * lax.rem(position // bit, 2))


class Answer:
    def __init__(self, staged, out, sends, receives, keep, inner):
        self.staged, self.out, self.sends, self.receives, self.keep = staged, out, sends, receives, keep
        self.inner = inner
        self.at_i = lax.axis_index("i")

    def target(self, k, m):
        return self.out.at[k, m, pl.ds(pl.multiple_of(self.at_i * CAP, 8), CAP)]

    def copy(self, k, m, d):
        group = lax.rem(self.at_i + d, self.inner)
        return to_peer(self.staged.at[m, group, k], self.target(k, m), self.sends.at[k, m, d],
                       self.receives.at[k, m, d], {"i": group})

    def kept(self, k, m):
        return pltpu.make_async_copy(self.staged.at[m, self.at_i, k], self.target(k, m), self.keep.at[k, m])

    def send(self, k, m):
        def step(d, carry):
            self.copy(k, m, d).start()
            return carry

        lax.fori_loop(1, self.inner, step, 0)
        self.kept(k, m).start()

    def finish(self, k, m):
        def step(d, carry):
            self.copy(k, m, d).wait()
            return carry

        lax.fori_loop(1, self.inner, step, 0)
        self.kept(k, m).wait()


def device_at(n, origin):
    o, i, t = origin
    return lax.rem(o + n // 16, 2), lax.rem(i + lax.rem(n // 2, 8), 8), lax.rem(t + lax.rem(n, 2), 2)


class Weights:
    def __init__(self, local, sources, target, sends, receives, keep):
        self.local, self.sources, self.target = local, sources, target
        self.sends, self.receives, self.keep = sends, receives, keep
        self.origin = tuple(lax.axis_index(name) for name in ("o", "i", "t"))

    def place(self, k, part):
        o, i, t = self.origin
        return self.target.at[k, o, i, t, part]

    def copy(self, k, n, part):
        o, i, t = device_at(n, self.origin)
        expert = (i * 2 + t) * self.local + k
        return to_peer(self.sources[part].at[expert], self.place(k, part), self.sends.at[k, n, part],
                       self.receives.at[k, n, part], {"o": o, "i": i, "t": t})

    def kept(self, k, part):
        _, i, t = self.origin
        expert = (i * 2 + t) * self.local + k
        return pltpu.make_async_copy(
            self.sources[part].at[expert], self.place(k, part), self.keep.at[k, part])

    def send(self, k):
        def step(n, carry):
            for part in range(2):
                self.copy(k, 32 - n, part).start()
            return carry

        lax.fori_loop(1, 32, step, 0)
        for part in range(2):
            self.kept(k, part).start()

    def finish(self, k):
        def step(n, carry):
            for part in range(2):
                self.copy(k, n, part).wait()
            return carry

        lax.fori_loop(1, 32, step, 0)
        for part in range(2):
            self.kept(k, part).wait()


class Gradients:
    def __init__(self, local, source, target, sends, receives, keep):
        self.local, self.source, self.target = local, source, target
        self.sends, self.receives, self.keep = sends, receives, keep
        self.origin = tuple(lax.axis_index(name) for name in ("o", "i", "t"))

    def place(self, k, part):
        o, i, t = self.origin
        return self.target.at[o, (i * 2 + t) * self.local + k, part]

    def copy(self, k, n, part):
        o, i, t = device_at(n, self.origin)
        return to_peer(self.source.at[k, o, i, t, part], self.place(k, part), self.sends.at[k, n, part],
                       self.receives.at[k, n, part], {"o": o, "i": i, "t": t})

    def kept(self, k, part):
        o, i, t = self.origin
        return pltpu.make_async_copy(
            self.source.at[k, o, i, t, part], self.place(k, part), self.keep.at[k, part])

    send = Weights.send
    finish = Weights.finish


def expert_scratch(count, width, tile, chunk):
    steps = count // chunk
    return [
        pltpu.VMEM((count, width), jnp.bfloat16), pltpu.VMEM((count, width), jnp.bfloat16),
        pltpu.VMEM((steps, width, chunk), jnp.bfloat16), pltpu.VMEM((steps, width, chunk), jnp.bfloat16),
        pltpu.VMEM((count, width), jnp.bfloat16), pltpu.VMEM((count, LANES), jnp.float32),
        pltpu.VMEM((count, width), jnp.float32), pltpu.VMEM((count, width), jnp.float32),
        pltpu.VMEM((2, width, tile), jnp.float32), pltpu.VMEM((2, width, tile), jnp.bfloat16),
        pltpu.SemaphoreType.DMA((2,)),
    ]


def expert_phase(k, expert, slots_hbm, cots_hbm, held, parts_ref, answers, scratch):
    slots, cots, rows_t, grads_t, grads, gate_scr, result_acc, back_acc, sums, tiles, load = scratch
    count, width = slots.shape
    chunk = rows_t.shape[2]
    tile = tiles.shape[2]
    micros, groups = answers[0].staged.shape[:2]
    loads = [pltpu.make_async_copy(slots_hbm.at[k], slots, load.at[0]),
             pltpu.make_async_copy(cots_hbm.at[k], cots, load.at[1])]
    for copy in loads:
        copy.start()
    for copy in loads:
        copy.wait()

    def prepare(r, carry):
        here = pl.ds(pl.multiple_of(r * chunk, 16), chunk)
        rows = slots[here]
        gates = router_gates(rows, parts_ref[...])
        lane = lax.broadcasted_iota(jnp.int32, gates.shape, 1)
        gate = jnp.sum(jnp.where(lane == expert, gates, 0.0), -1, keepdims=True)
        gate_scr[here] = jnp.broadcast_to(gate, gates.shape)
        low = (cots[here].astype(jnp.float32) * gate).astype(jnp.bfloat16)
        grads[here] = low
        rows_t[r] = rows.T
        grads_t[r] = low.T
        result_acc[here] = jnp.zeros((chunk, width), jnp.float32)
        back_acc[here] = jnp.zeros((chunk, width), jnp.float32)
        return carry

    lax.fori_loop(0, count // chunk, prepare, 0)
    per_part = held.shape[6] // tile

    def one_tile(n, carry):
        t = n // per_part
        span = pl.ds(pl.multiple_of(lax.rem(n, per_part) * tile, tile), tile)
        for part in range(2):
            tiles[part] = held[k, :, :, t, part, :, span].reshape(width, tile)
        sums[...] = jnp.zeros_like(sums)

        def work(r, inside):
            here = pl.ds(pl.multiple_of(r * chunk, 16), chunk)
            pre = mm(slots[here], tiles[0])
            square = pre * pre
            half = 0.5 + 0.5 * jnp.tanh(pre * (GELU_C + (GELU_C * GELU_A) * square))
            hidden = (pre * half).astype(jnp.bfloat16)
            slope = half + 2.0 * half * (1.0 - half) * pre * (
                GELU_C + (3.0 * GELU_C * GELU_A) * square)
            pre_grad = (mm(grads[here], tiles[1]) * slope).astype(jnp.bfloat16)
            result_acc[here] += mm(hidden, tiles[1], NT)
            back_acc[here] += mm(pre_grad, tiles[0], NT)
            sums[0] += mm(rows_t[r], pre_grad)
            sums[1] += mm(grads_t[r], hidden)
            return inside

        lax.fori_loop(0, count // chunk, work, 0)
        block = held.shape[1:3] + (held.shape[5], tile)
        for part in range(2):
            held[k, :, :, t, part, :, span] = sums[part].astype(jnp.bfloat16).reshape(block)
        return carry

    lax.fori_loop(0, held.shape[3] * per_part, one_tile, 0)
    per_chunk = chunk // CAP
    back, result = answers

    def finish(n, carry):
        here = pl.ds(pl.multiple_of(n * chunk, 16), chunk)
        m, r = n // (groups // per_chunk), lax.rem(n, groups // per_chunk)
        value = result_acc[here]
        gate_grad = jnp.sum(cots[here].astype(jnp.float32) * value, -1, keepdims=True)
        lane = lax.broadcasted_iota(jnp.int32, (chunk, LANES), 1)
        spread = jnp.where(lane == expert, gate_grad, 0.0)
        value = value * gate_scr[here][:, 0:1]
        grad = back_acc[here]
        for q in range(per_chunk):
            rows = slice(q * CAP, (q + 1) * CAP)
            at = r * per_chunk + q
            result.staged[m, at, k] = value[rows].astype(jnp.bfloat16)
            back.staged[m, at, k, :, 0:width] = grad[rows].astype(jnp.bfloat16)
            back.staged[m, at, k, :, width:width + LANES] = spread[rows].astype(jnp.bfloat16)
        return carry

    lax.fori_loop(0, micros * groups // per_chunk, finish, 0)
    for m in range(micros):
        back.send(k, m)
    for m in range(micros):
        result.send(k, m)


def opening_kernel(
    local, per_step, pack_ref, cot_ref, index_ref, table_ref, tok_ref, bias_ref, first_ref, second_ref,
    small_ref, block_out, input_out, dweights_ref, middle_out, proj_out, mixed_out, gates_out,
    slots_ref, cots_ref, back_ref, result_ref,
    gathered, partial, loose, mats_ref, norms_ref, parts_ref, router_ref, shared_c, shared_r, away_g,
    staged_c, staged_r, held, staged_back,
    load, ring_send, ring_recv, pair_send, pair_recv, pair_send_r, pair_recv_r,
    cot_send, cot_recv, cot_keep, row_send, row_recv, row_keep,
    weight_send, weight_recv, weight_keep, grad_send, grad_recv, grad_keep,
    back_send, back_recv, back_keep, result_send, result_recv, result_keep, store,
    away_send, away_recv, fold_send, fold_recv, fetch,
):
    at_o, at_i, at_t = (lax.axis_index(name) for name in ("o", "i", "t"))
    micros, _, own_rows, width = shared_c.shape
    images, length, _ = tok_ref.shape
    kinds, columns = mats_ref.shape[1], mats_ref.shape[3]
    depth = width // 16
    rows = per_step * length
    steps = own_rows // rows
    stages = [
        {"t": 1 - at_t}, {"o": 1 - at_o}, {"i": flipped(at_i, 4)}, {"i": flipped(at_i, 2)},
        {"i": flipped(at_i, 1)},
    ]
    cot_plan = Dispatch(index_ref, shared_c, staged_c, cots_ref, cot_send, cot_recv, cot_keep, 8, 2, local)
    row_plan = Dispatch(index_ref, shared_r, staged_r, slots_ref, row_send, row_recv, row_keep, 8, 2, local)
    weights = Weights(local, (first_ref, second_ref), held, weight_send, weight_recv, weight_keep)
    gradients = Gradients(local, held, dweights_ref, grad_send, grad_recv, grad_keep)

    def stage(j):
        size = 2 ** j
        return to_peer(gathered.at[pl.ds(0, size)], gathered.at[pl.ds(size, size)],
                       ring_send.at[j], ring_recv.at[j], stages[j])

    def swap_c(m):
        return to_peer(shared_c.at[m, 0], shared_c.at[m, 1], pair_send.at[m], pair_recv.at[m],
                       {"t": 1 - at_t})

    def swap_r(m, s):
        here = pl.ds(pl.multiple_of(s * rows, 16), rows)
        return to_peer(shared_r.at[m, 0, here], shared_r.at[m, 1, here], pair_send_r.at[m, s],
                       pair_recv_r.at[m, s], {"t": 1 - at_t})

    def relative(r):
        o = flipped_if(at_o, 1, lax.rem(r // 2, 2))
        i = flipped_if(at_i, 4, lax.rem(r // 4, 2))
        i = flipped_if(i, 2, lax.rem(r // 8, 2))
        i = flipped_if(i, 1, lax.rem(r // 16, 2))
        return o, i, flipped_if(at_t, 1, lax.rem(r, 2))

    def opening(tok, cot, proj, mixed, gates):
        fill = pltpu.make_async_copy(pack_ref, gathered.at[0], load.at[0])
        take_cot = pltpu.make_async_copy(cot_ref, cot, load.at[1])
        take_tok = pltpu.make_async_copy(tok_ref, tok, load.at[2])
        fill.start()
        take_cot.start()
        take_tok.start()
        fill.wait()
        stage(0).start()
        take_cot.wait()
        shared_c[0, 0] = cot[0:images // 2].reshape(own_rows, width).astype(jnp.bfloat16)
        swap_c(0).start()
        stage(0).wait()
        stage(1).start()
        shared_c[1, 0] = cot[images // 2:].reshape(own_rows, width).astype(jnp.bfloat16)
        swap_c(1).start()
        stage(1).wait()
        stage(2).start()
        stage(2).wait()
        stage(3).start()
        weights.send(0)
        swap_c(0).wait()
        cot_plan.send(0)
        stage(3).wait()
        stage(4).start()
        swap_c(1).wait()
        cot_plan.send(1)
        stage(4).wait()

        def place(r, carry):
            o, i, t = relative(r)
            row = pl.multiple_of((o * 8 + i) * depth, depth)
            for c in range(kinds):
                mats_ref[t, c, pl.ds(row, depth)] = gathered[r, c * depth:(c + 1) * depth]
            loose[(o * 8 + i) * 2 + t] = gathered[r, kinds * depth:, 0:LANES].astype(jnp.float32)
            return carry

        lax.fori_loop(0, gathered.shape[0], place, 0)
        turned = loose[...].reshape(width, LANES).T
        norms_ref[...] = turned[96:104] + turned[104:112] + turned[112:120]
        low = turned[0:96].astype(jnp.bfloat16)
        parts_ref[...] = jnp.concatenate([low, jnp.zeros((32, width), jnp.bfloat16)], 0)
        router_ref[0:32] = turned[0:32] + turned[32:64] + turned[64:96]
        router_ref[32:] = jnp.zeros((96, width), jnp.float32)
        take_tok.wait()

        def attend(n, carry):
            m, s = n // steps, lax.rem(n, steps)
            _, routed = forward_rows(n * per_step, per_step, tok, bias_ref, mats_ref, norms_ref, parts_ref,
                                     tok, proj, mixed, gates)
            shared_r[m, 0, pl.ds(pl.multiple_of(s * rows, 16), rows)] = routed
            swap_r(m, s).start()
            return carry

        lax.fori_loop(0, micros * steps, attend, 0)
        outs = [(tok, middle_out), (proj, proj_out), (mixed, mixed_out), (gates, gates_out)]
        stores = [pltpu.make_async_copy(a, b, store.at[n]) for n, (a, b) in enumerate(outs)]
        for copy in stores:
            copy.start()
        for m in range(micros):
            for s in range(steps):
                swap_r(m, s).wait()
            row_plan.send(m)
        weights.send(1)
        for copy in stores:
            copy.wait()

    pl.run_scoped(
        opening,
        pltpu.VMEM(tok_ref.shape, jnp.float32),
        pltpu.VMEM(cot_ref.shape, jnp.float32),
        pltpu.VMEM((images, length, 3 * width), jnp.bfloat16),
        pltpu.VMEM((images, length, width), jnp.bfloat16),
        pltpu.VMEM((images, length, LANES), jnp.float32),
    )
    for m in range(micros):
        row_plan.finish(m)
        cot_plan.finish(m)
    back = Answer(staged_back, back_ref, back_send, back_recv, back_keep, 8)
    result = Answer(staged_c, result_ref, result_send, result_recv, result_keep, 8)
    count = slots_ref.shape[1]

    def experts(*scratch):
        def one(k, carry):
            weights.finish(k)
            expert = (at_i * 2 + at_t) * local + k
            expert_phase(k, expert, slots_ref, cots_ref, held, parts_ref, (back, result), scratch)
            gradients.send(k)
            return carry

        lax.fori_loop(0, local, one, 0)

    pl.run_scoped(experts, *expert_scratch(count, width, 512, 480))

    places = lax.broadcasted_iota(jnp.int32, (1, 8 * CAP), 1)
    block = sum((places >= q * CAP).astype(jnp.int32) for q in range(1, 8))
    places = places + block * (3 * CAP) + at_t * (2 * CAP)

    def taken(table, m, half, here, values):
        first, second = table[m, half, here, 0:1], table[m, half, here, 1:2]
        total = None
        for k in range(local):
            where = places + k * CAP
            hits = jnp.where((first == where) | (second == where), 1.0, 0.0).astype(jnp.bfloat16)
            part = mm(hits, values[k])
            total = part if total is None else total + part
        return total

    across = {"t": 1 - at_t}

    def away(m, s, which):
        here = pl.ds(pl.multiple_of(s * rows, 16), rows)
        buffer = (shared_r, away_g, shared_c)[which]
        return to_peer(buffer.at[m, 0, here], buffer.at[m, 1, here], away_send.at[which, m, s],
                       away_recv.at[which, m, s], across)

    def collect(own):
        def fetched(table, backs, results):
            take = pltpu.make_async_copy(table_ref, table, fetch.at[2])
            take.start()
            take.wait()
            for m in range(micros):
                for k in range(local):
                    back.finish(k, m)
                    pltpu.make_async_copy(back_ref.at[k, m], backs.at[k], fetch.at[k]).start()
                for k in range(local):
                    pltpu.make_async_copy(back_ref.at[k, m], backs.at[k], fetch.at[k]).wait()

                def leave(s, carry):
                    here = pl.ds(pl.multiple_of(s * rows, 16), rows)
                    total = taken(table, m, 1, here, backs).astype(jnp.bfloat16)
                    shared_r[m, 0, here] = total[:, :width]
                    away_g[m, 0, here] = total[:, width:]
                    away(m, s, 0).start()
                    away(m, s, 1).start()
                    return carry

                lax.fori_loop(0, steps, leave, 0)

                def stay(s, carry):
                    here = pl.ds(pl.multiple_of(s * rows, 16), rows)
                    own[m * steps + s] = taken(table, m, 0, here, backs)
                    return carry

                lax.fori_loop(0, steps, stay, 0)
            for m in range(micros):
                for k in range(local):
                    result.finish(k, m)
                    pltpu.make_async_copy(result_ref.at[k, m], results.at[k], fetch.at[k]).start()
                for k in range(local):
                    pltpu.make_async_copy(result_ref.at[k, m], results.at[k], fetch.at[k]).wait()

                def leave(s, carry):
                    here = pl.ds(pl.multiple_of(s * rows, 16), rows)
                    shared_c[m, 0, here] = taken(table, m, 1, here, results).astype(jnp.bfloat16)
                    away(m, s, 2).start()
                    return carry

                lax.fori_loop(0, steps, leave, 0)

        pl.run_scoped(
            fetched, pltpu.VMEM(table_ref.shape, jnp.int32), pltpu.VMEM((local, 8 * CAP, width + LANES), jnp.bfloat16),
            pltpu.VMEM((local, 8 * CAP, width), jnp.bfloat16))

        def backward(tok, middle, cot, proj, mixed, gates, dproj, dmats, dnorms, drouter):
            dmats[...] = jnp.zeros_like(dmats)
            dnorms[...] = jnp.zeros_like(dnorms)
            drouter[...] = jnp.zeros_like(drouter)
            pairs = [(tok_ref, tok), (middle_out, middle), (cot_ref, cot), (proj_out, proj),
                     (mixed_out, mixed), (gates_out, gates)]

            def micro(m, carry):
                ours = pl.ds(m * (images // micros), images // micros)
                takes = [pltpu.make_async_copy(a.at[ours], b, fetch.at[n]) for n, (a, b) in enumerate(pairs)]
                for copy in takes:
                    copy.start()
                for copy in takes:
                    copy.wait()

                def attend(s, inside):
                    away(m, s, 0).wait()
                    away(m, s, 1).wait()
                    here = pl.ds(pl.multiple_of(s * rows, 16), rows)
                    grad = own[m * steps + s] + jnp.concatenate([
                        shared_r[m, 1, here].astype(jnp.float32), away_g[m, 1, here].astype(jnp.float32)], 1)
                    backward_rows(s * per_step, per_step, grad, tok, middle, cot, gates, proj, mixed,
                                  bias_ref.at[ours], mats_ref, norms_ref, router_ref, cot, dnorms, drouter,
                                  dproj, dmats)
                    return inside

                lax.fori_loop(0, steps, attend, 0)
                keep = pltpu.make_async_copy(cot, input_out.at[ours], store.at[0])
                keep.start()
                keep.wait()
                return carry

            lax.fori_loop(0, micros, micro, 0)
            tail = jnp.concatenate(
                [jnp.zeros((96, width), jnp.float32), dnorms[...], jnp.zeros((24, width), jnp.float32)], 0)
            drouter[...] += tail.T

            def spread(r, carry):
                o, i, t = relative(r)
                row = pl.multiple_of((o * 8 + i) * depth, depth)
                for c in range(kinds):
                    gathered[r, c * depth:(c + 1) * depth] = dmats[t, c, pl.ds(row, depth)].astype(jnp.bfloat16)
                row = pl.multiple_of(((o * 8 + i) * 2 + t) * 16, 16)
                gathered[r, kinds * depth:, 0:LANES] = drouter[pl.ds(row, 16)].astype(jnp.bfloat16)
                gathered[r, kinds * depth:, LANES:] = jnp.zeros((16, columns - LANES), jnp.bfloat16)
                return carry

            lax.fori_loop(0, gathered.shape[0], spread, 0)

        some = images // micros
        pl.run_scoped(
            backward,
            pltpu.VMEM((some, length, width), jnp.float32),
            pltpu.VMEM((some, length, width), jnp.float32),
            pltpu.VMEM((some, length, width), jnp.float32),
            pltpu.VMEM((some, length, 3 * width), jnp.bfloat16),
            pltpu.VMEM((some, length, width), jnp.bfloat16),
            pltpu.VMEM((some, length, LANES), jnp.float32),
            pltpu.VMEM((rows, 3 * width), jnp.float32),
            pltpu.VMEM(mats_ref.shape, jnp.float32),
            pltpu.VMEM((8, width), jnp.float32),
            pltpu.VMEM((width, LANES), jnp.float32),
        )

    pl.run_scoped(collect, pltpu.VMEM((micros * steps, rows, width + LANES), jnp.float32))

    def fold(j):
        size = 2 ** j
        return to_peer(gathered.at[pl.ds(size, size)], partial.at[pl.ds(size, size)],
                       fold_send.at[j], fold_recv.at[j], stages[j])

    def folded(j):
        fold(j).wait()
        size = 2 ** j

        def add(r, carry):
            gathered[r] = (gathered[r].astype(jnp.float32) + partial[size + r].astype(jnp.float32)).astype(
                jnp.bfloat16)
            return carry

        lax.fori_loop(0, size, add, 0)

    def outputs(table, middle, results):
        fold(4).start()
        index_take = pltpu.make_async_copy(table_ref, table, fetch.at[3])
        index_take.start()
        take = pltpu.make_async_copy(middle_out, middle, fetch.at[2])
        take.start()
        for m in range(micros):
            for k in range(local):
                pltpu.make_async_copy(result_ref.at[k, m], results.at[k], fetch.at[k]).start()
            for k in range(local):
                pltpu.make_async_copy(result_ref.at[k, m], results.at[k], fetch.at[k]).wait()
            if m == 0:
                take.wait()
                index_take.wait()

            def stay(s, carry):
                n = m * steps + s
                here = pl.ds(pl.multiple_of(s * rows, 16), rows)
                away(m, s, 2).wait()
                total = taken(table, m, 0, here, results) + shared_c[m, 1, here].astype(jnp.float32)
                images_here = pl.ds(n * per_step, per_step)
                middle[images_here] = middle[images_here] + total.reshape(per_step, length, width)
                return carry

            lax.fori_loop(0, steps, stay, 0)
            folded(4 - m)
            fold(3 - m).start()
        keep = pltpu.make_async_copy(middle, block_out, store.at[0])
        keep.start()
        for j in (2, 1):
            folded(j)
            fold(j - 1).start()
        fold(0).wait()
        small_ref[...] = gathered[0].astype(jnp.float32) + partial[1].astype(jnp.float32)
        keep.wait()

    pl.run_scoped(
        outputs, pltpu.VMEM(table_ref.shape, jnp.int32), pltpu.VMEM(tok_ref.shape, jnp.float32),
        pltpu.VMEM((local, 8 * CAP, width), jnp.bfloat16))

    def close(k, carry):
        gradients.finish(k)
        return carry

    lax.fori_loop(0, local, close, 0)


def opening(pack, cot, index, table, tok, bias, first_in, second_in, local, per_step):
    micros, own_rows = index.shape[0], index.shape[3]
    images, length, width = tok.shape
    columns = pack.shape[1]
    experts, depth, extent = first_in.shape
    steps = own_rows // (per_step * length)
    slots = micros * 8 * CAP
    anywhere = pl.BlockSpec(memory_space=pl.ANY)
    vector = pl.BlockSpec(memory_space=pltpu.VMEM)
    dma = pltpu.SemaphoreType.DMA
    low, wide = jnp.bfloat16, jnp.float32
    weights = (local, 2, 8, 2, 2, depth, extent)
    shape = jax.ShapeDtypeStruct
    return pl.pallas_call(
        functools.partial(opening_kernel, local, per_step),
        in_specs=[anywhere, anywhere, vector, anywhere, anywhere, vector, anywhere, anywhere],
        out_specs=[vector] + [anywhere] * 11,
        out_shape=[
            shape(pack.shape, wide), shape(tok.shape, wide), shape(tok.shape, wide),
            shape((2, experts, 2, depth, extent), low),
            shape((images, length, width), wide), shape((images, length, 3 * width), low),
            shape((images, length, width), low), shape((images, length, LANES), wide),
            shape((local, slots, width), low), shape((local, slots, width), low),
            shape((local, micros, 8 * CAP, width + LANES), low), shape((local, micros, 8 * CAP, width), low),
        ],
        scratch_shapes=[
            pltpu.VMEM((32,) + pack.shape, low),
            pltpu.VMEM((32,) + pack.shape, low),
            pltpu.VMEM((32, width // 32, LANES), wide),
            pltpu.VMEM((2, 4, width, columns), low), pltpu.VMEM((8, width), wide),
            pltpu.VMEM((LANES, width), low), pltpu.VMEM((LANES, width), wide),
            pltpu.VMEM((micros, 2, own_rows, width), low),
            pltpu.VMEM((micros, 2, own_rows, width), low),
            pltpu.VMEM((micros, 2, own_rows, LANES), low),
            pltpu.VMEM((micros, 8, local, CAP, width), low),
            pltpu.VMEM((micros, 8, local, CAP, width), low),
            pltpu.VMEM(weights, low),
            pltpu.VMEM((micros, 8, local, CAP, width + LANES), low),
            dma((3,)), dma((5,)), dma((5,)), dma((micros,)), dma((micros,)),
            dma((micros, steps)), dma((micros, steps)),
            dma((micros, 8, local)), dma((micros, 8, local)), dma((micros, local)),
            dma((micros, 8, local)), dma((micros, 8, local)), dma((micros, local)),
            dma((local, 32, 2)), dma((local, 32, 2)), dma((local, 2)),
            dma((local, 32, 2)), dma((local, 32, 2)), dma((local, 2)),
            dma((local, micros, 8)), dma((local, micros, 8)), dma((local, micros)),
            dma((local, micros, 8)), dma((local, micros, 8)), dma((local, micros)), dma((4,)),
            dma((3, micros, steps)), dma((3, micros, steps)), dma((5,)), dma((5,)), dma((6,)),
        ],
        compiler_params=pltpu.CompilerParams(vmem_limit_bytes=67043328, has_side_effects=True),
        cost_estimate=pl.CostEstimate(flops=1000, bytes_accessed=1000, transcendentals=0),
        name="opening",
    )(pack, cot, index, table, tok, bias, first_in, second_in)


def per_device(planes, inner, parts, tokens, key_mask, expert_ids, slot_ids, norm1_gain, norm1_bias,
               qkv_weight, out_weight, norm2_gain, norm2_bias, router_weight, expert_in, expert_out,
               cotangent):
    micros, own_rows, width = tokens.shape
    length = key_mask.shape[2]
    group_rows = own_rows * parts
    images = own_rows // length
    total = micros * images
    experts = expert_in.shape[0]
    homes = inner * parts
    local = experts // homes
    depth, extent = expert_in.shape[1:]
    small = norm1_gain.shape[0]
    every = ("o", "i", "t")
    plane_at, inner_at, part_at = (lax.axis_index(name) for name in every)
    low = jnp.bfloat16

    loose = jnp.concatenate([
        jnp.stack([norm1_gain, norm1_bias, norm2_gain, norm2_bias], 1), router_weight], 1)
    loose_count = 3 * loose.size
    columns = qkv_weight.shape[2]
    loose_rows = -(-loose_count // (16 * columns)) * 16
    loose_low = jnp.concatenate([p.reshape(-1) for p in three_parts(loose)])
    loose_low = jnp.pad(loose_low, (0, loose_rows * columns - loose_count)).reshape(loose_rows, columns)
    packed = jnp.concatenate([
        qkv_weight.transpose(1, 0, 2).reshape(3 * depth, columns), out_weight.T, loose_low], 0)
    gathered = lax.all_gather(packed, ("o", "i"), axis=0)
    gathered = lax.all_gather(gathered, "t", axis=0)
    mats = gathered[:, :, :4 * depth].reshape(parts, planes * inner, 4, depth, columns)
    mats = mats.transpose(2, 1, 3, 0, 4).reshape(1, 4, width, width)
    loose_all = gathered[:, :, 4 * depth:].reshape(parts, planes * inner, loose_rows * columns)
    loose_all = loose_all[:, :, :loose_count].astype(jnp.float32)
    loose_all = loose_all.reshape(parts, planes * inner, 3, small, 4 + experts)
    loose_all = (loose_all[:, :, 0] + loose_all[:, :, 1]) + loose_all[:, :, 2]
    loose_all = loose_all.transpose(1, 0, 2, 3).reshape(width, 4 + experts)
    norms = loose_all[:, :4].T
    router = jnp.pad(loose_all[:, 4:], ((0, 0), (0, LANES - experts)))
    router_parts = jnp.concatenate(three_parts(router[:, :experts]), 1).T
    router_parts = jnp.pad(router_parts, ((0, LANES - 3 * experts), (0, 0)))

    weights = []
    first_in = expert_in.reshape(homes, local, depth, extent)
    second_in = expert_out.transpose(0, 2, 1).reshape(homes, local, depth, extent)
    for k in range(local):
        both = jnp.stack([first_in[:, k], second_in[:, k]], 1)
        mine = lax.all_to_all(both, ("i", "t"), 0, 0, tiled=True)
        if planes == 2:
            other = lax.ppermute(mine, "o", [(0, 1), (1, 0)])
            full = jnp.where(plane_at == 0, jnp.stack([mine, other]), jnp.stack([other, mine]))
        else:
            full = lax.all_gather(mine, "o", axis=0)
        weights.append(full.reshape(planes, inner, parts, 2, depth, extent))

    own_first = part_at * own_rows
    slot_index = jnp.where(slot_ids >= 0, expert_ids * CAP + slot_ids, -1)
    if parts == 2:
        slot_index = jnp.concatenate([
            lax.dynamic_slice_in_dim(slot_index, own_first, own_rows, 1),
            lax.dynamic_slice_in_dim(slot_index, own_rows - own_first, own_rows, 1)], 1)
    homes_i = lax.broadcasted_iota(jnp.int32, (inner, local, CAP), 0)
    locals_i = lax.broadcasted_iota(jnp.int32, (inner, local, CAP), 1)
    cap_i = lax.broadcasted_iota(jnp.int32, (inner, local, CAP), 2)
    places = ((homes_i * parts + part_at) * local + locals_i) * CAP + cap_i

    def table(m, positions, rows=slice(None)):
        index = slot_index[m, rows]
        flat = positions.reshape(1, -1)
        return ((index[:, 0:1] == flat) | (index[:, 1:2] == flat)).astype(low)

    def share(rows):
        if parts == 2:
            return jnp.concatenate([rows, lax.ppermute(rows, "t", [(0, 1), (1, 0)])], 1)
        return lax.all_gather(rows, "t", axis=1, tiled=True)

    def dispatch(shared):
        sent = []
        for m in range(micros):
            slots = mm(table(m, places), shared[m], TN).astype(low)
            slots = lax.all_to_all(slots.reshape(inner, local * CAP, width), "i", 0, 0, tiled=True)
            sent.append(slots.reshape(inner, local, CAP, width))
        return [
            jnp.concatenate([s[:, k].reshape(inner * CAP, width) for s in sent], 0) for k in range(local)]

    cot_slots = dispatch(share(cotangent.astype(low)))

    flags = lax.dynamic_slice_in_dim(key_mask, part_at * images, images, 1).reshape(total, 1, length)
    bias = jnp.where(flags > 0, 0.0, -1e30).astype(jnp.float32)
    tok = tokens.reshape(total, length, width)
    per_step = 2 if total % 2 == 0 else 1
    middle, routed, proj, mixed, gates = attention_forward(tok, bias, mats, norms, router_parts, per_step)

    row_slots = dispatch(share(routed.reshape(micros, own_rows, width)))

    first_out, second_out, results, backs = [], [], [], []
    for k in range(local):
        expert = ((inner_at * parts + part_at) * local + k).astype(jnp.int32).reshape(1)
        result, back, dweights = run_expert(expert, row_slots[k], cot_slots[k], weights[k], router_parts)
        results.append(result.reshape(micros, inner, CAP, width))
        backs.append(back.reshape(micros, inner, CAP, width + LANES))
        dweights = dweights.reshape(planes, homes, 2, depth, extent)
        if planes == 2:
            theirs = lax.dynamic_index_in_dim(dweights, 1 - plane_at, 0, keepdims=False)
            ours = lax.dynamic_index_in_dim(dweights, plane_at, 0, keepdims=False)
            summed = ours.astype(jnp.float32) + lax.ppermute(
                theirs, "o", [(0, 1), (1, 0)]).astype(jnp.float32)
            summed = summed.astype(low)
        else:
            summed = lax.psum_scatter(dweights, "o", scatter_dimension=0, tiled=True)[0]
        final = lax.all_to_all(summed, ("i", "t"), 0, 0, tiled=True)
        first_out.append(final[:, 0])
        second_out.append(final[:, 1])
    first_grad = jnp.stack(first_out, 1).reshape(experts, depth, extent).astype(jnp.float32)
    second_grad = jnp.stack(second_out, 1).reshape(experts, depth, extent).astype(jnp.float32)
    second_grad = second_grad.transpose(0, 2, 1)

    def collect(values):
        size = values[0].shape[-1]
        answers = []
        for m in range(micros):
            back = jnp.stack([v[m] for v in values], 1).reshape(inner, local * CAP, size)
            back = lax.all_to_all(back, "i", 0, 0, tiled=True).reshape(inner * local * CAP, size)
            if parts == 2:
                away = mm(table(m, places, slice(own_rows, None)), back).astype(low)
                here = mm(table(m, places, slice(0, own_rows)), back)
                answers.append(here + lax.ppermute(away, "t", [(0, 1), (1, 0)]).astype(jnp.float32))
            else:
                whole = mm(table(m, places), back).astype(low)
                answers.append(lax.psum_scatter(
                    whole, "t", scatter_dimension=0, tiled=True).astype(jnp.float32))
        return jnp.stack(answers)

    grad = collect(backs)
    combined = collect(results)
    block_out = middle.reshape(micros, own_rows, width) + combined

    input_grad, dmats, dnorms, drouter = attention_backward(
        tok, middle, cotangent.reshape(total, length, width), grad.reshape(total, length, width + LANES),
        gates, proj, mixed, bias, mats, norms, router.T, per_step)
    input_grad = input_grad.reshape(micros, own_rows, width)

    dmats = dmats.reshape(4, planes, inner, depth, parts, columns).transpose(2, 4, 1, 0, 3, 5)
    dmats = dmats.reshape(homes, planes, 4 * depth, columns)
    dloose = jnp.concatenate([dnorms.T, drouter[:, :experts]], 1)
    dloose = dloose.reshape(planes, inner, parts, small * (4 + experts)).transpose(1, 2, 0, 3)
    dloose = jnp.concatenate(three_parts(dloose), -1)
    dloose = jnp.pad(dloose, ((0, 0),) * 3 + ((0, loose_rows * columns - loose_count),))
    dloose = dloose.reshape(homes, planes, loose_rows, columns)
    payload = jnp.concatenate([dmats, dloose], 2)
    payload = lax.all_to_all(payload, ("i", "t"), 0, 0, tiled=True)
    payload = jnp.sum(payload.astype(jnp.float32), 0)
    if planes == 2:
        theirs = lax.dynamic_index_in_dim(payload, 1 - plane_at, 0, keepdims=False)
        ours = lax.dynamic_index_in_dim(payload, plane_at, 0, keepdims=False)
        reduced = ours + lax.ppermute(theirs, "o", [(0, 1), (1, 0)])
    else:
        reduced = lax.psum_scatter(payload, "o", scatter_dimension=0, tiled=True)[0]
    matrices = reduced[:4 * depth].reshape(4, depth, columns)
    qkv_grad = matrices[:3].transpose(1, 0, 2)
    out_grad = matrices[3].T
    tail = reduced[4 * depth:].reshape(-1)[:loose_count].reshape(3, small, 4 + experts)
    tail = (tail[0] + tail[1]) + tail[2]
    return (
        block_out, input_grad, tail[:, 0], tail[:, 1], qkv_grad, out_grad, tail[:, 2], tail[:, 3],
        tail[:, 4:], first_grad, second_grad,
    )


def per_device_halves(tokens, key_mask, expert_ids, slot_ids, norm1_gain, norm1_bias,
                      qkv_weight, out_weight, norm2_gain, norm2_bias, router_weight, expert_in, expert_out,
                      cotangent):
    micros, own_rows, width = tokens.shape
    length = key_mask.shape[2]
    images = own_rows // length
    total = micros * images
    planes, inner, parts = 2, 8, 2
    experts = expert_in.shape[0]
    homes = inner * parts
    local = experts // homes
    depth, extent = expert_in.shape[1:]
    columns = qkv_weight.shape[2]
    plane_at, inner_at, part_at = (lax.axis_index(name) for name in ("o", "i", "t"))
    low = jnp.bfloat16
    across = [(0, 1), (1, 0)]

    norms_in = jnp.stack([norm1_gain, norm1_bias, norm2_gain, norm2_bias], 1)
    loose = [p for p in three_parts(router_weight)]
    loose += [jnp.pad(p, ((0, 0), (0, 4))) for p in three_parts(norms_in)]
    loose = jnp.concatenate(loose, 1)
    loose = jnp.pad(loose, ((0, 0), (0, columns - loose.shape[1])))
    packed = jnp.concatenate([
        qkv_weight.transpose(1, 0, 2).reshape(3 * depth, columns), out_weight.T, loose], 0)
    slot_index = jnp.where(slot_ids >= 0, expert_ids * CAP + slot_ids, -1).transpose(0, 2, 1)
    own_first = part_at * own_rows
    index = jnp.stack([
        lax.dynamic_slice_in_dim(slot_index, own_first, own_rows, 2),
        lax.dynamic_slice_in_dim(slot_index, own_rows - own_first, own_rows, 2)], 2)

    flags = lax.dynamic_slice_in_dim(key_mask, part_at * images, images, 1).reshape(total, 1, length)
    bias = jnp.where(flags > 0, 0.0, -1e30).astype(jnp.float32)
    tok = tokens.reshape(total, length, width)
    table = jnp.pad(index.transpose(0, 2, 3, 1), ((0, 0), (0, 0), (0, 0), (0, LANES - 2)))
    reduced, block_out, input_grad, dweights = opening(
        packed, cotangent.reshape(tok.shape), index, table, tok, bias, expert_in, expert_out.transpose(0, 2, 1), local, 2)[:4]
    dweights = dweights[0].astype(jnp.float32) + dweights[1].astype(jnp.float32)
    first_grad = dweights[:, 0]
    second_grad = dweights[:, 1].transpose(0, 2, 1)
    matrices = reduced[:4 * depth].reshape(4, depth, columns)
    qkv_grad = matrices[:3].transpose(1, 0, 2)
    out_grad = matrices[3].T
    tail = reduced[4 * depth:]
    shape = (micros, own_rows, width)
    return (
        block_out.reshape(shape), input_grad.reshape(shape), tail[:, 96], tail[:, 97], qkv_grad, out_grad,
        tail[:, 98], tail[:, 99], tail[:, :experts], first_grad, second_grad,
    )


def solution(mesh):
    dp, parts = mesh.shape["dp"], mesh.shape["tensor"]
    inner = min(8, 32 // parts, dp)
    planes = dp // inner
    fine = Mesh(mesh.devices.reshape(planes, inner, parts), ("o", "i", "t"))
    dps = ("o", "i")
    every = ("o", "i", "t")
    rows = P(None, every, None)
    step = functools.partial(per_device, planes, inner, parts)
    if (planes, inner, parts) == (2, 8, 2):
        step = per_device_halves
    return jax.shard_map(
        step,
        mesh=fine,
        in_specs=(
            rows, P(None, dps, None), P(None, dps, None), P(None, dps, None), P(every), P(every),
            P(dps, None, "t"), P("t", dps), P(every), P(every), P(every, None),
            P(None, dps, "t"), P(None, "t", dps), rows,
        ),
        out_specs=(
            rows, rows, P(every), P(every), P(dps, None, "t"), P("t", dps), P(every), P(every),
            P(every, None), P(None, dps, "t"), P(None, "t", dps),
        ),
        check_vma=False,
    )
```

```python
import functools

import jax
import jax.numpy as jnp
from jax import lax
from jax.experimental import pallas as pl
from jax.experimental.pallas import tpu as pltpu
from jax.sharding import Mesh, PartitionSpec as P

HEAD = 64
CAP = 120
EPSILON = 1e-06
LANES = 128
VMEM = 60 * 1024 * 1024
NN = (((1,), (0,)), ((), ()))
NT = (((1,), (1,)), ((), ()))
TN = (((0,), (0,)), ((), ()))
HIGH = lax.Precision.HIGHEST
GELU_C = 0.7978845608028654
GELU_A = 0.044715


def mm(a, b, dims=NN, precision=None):
    return lax.dot_general(a, b, dims, precision=precision, preferred_element_type=jnp.float32)


def three_parts(value):
    high = value.astype(jnp.bfloat16)
    rest = value - high.astype(jnp.float32)
    middle = rest.astype(jnp.bfloat16)
    last = (rest - middle.astype(jnp.float32)).astype(jnp.bfloat16)
    return high, middle, last


def standardize(values):
    center = jnp.mean(values, -1, keepdims=True)
    shifted = values - center
    spread = jnp.mean(shifted * shifted, -1, keepdims=True)
    inverse = lax.rsqrt(spread + EPSILON)
    return shifted * inverse, inverse


def norm_back(grad, unit, inverse):
    return inverse * (
        grad
        - jnp.mean(grad, -1, keepdims=True)
        - unit * jnp.mean(grad * unit, -1, keepdims=True)
    )


def even_lanes(shape):
    return lax.broadcasted_iota(jnp.int32, shape, 1) < HEAD


def router_gates(routed, parts):
    logits = mm(routed, parts, NT)
    logits = logits + pltpu.roll(logits, LANES - 32, 1) + pltpu.roll(logits, LANES - 64, 1)
    lane = lax.broadcasted_iota(jnp.int32, logits.shape, 1)
    logits = jnp.where(lane < 32, logits, -1e30)
    lifted = jnp.exp(logits - jnp.max(logits, -1, keepdims=True))
    return lifted / jnp.sum(lifted, -1, keepdims=True)


def forward_rows(first, images, tok_ref, bias_ref, mats_ref, norms_ref, parts_ref,
                 middle_ref, proj_ref, mixed_ref, gates_ref):
    _, length, width = tok_ref.shape
    pieces, _, _, columns = mats_ref.shape
    rows = images * length
    here = pl.ds(first, images)
    tok = tok_ref[here].reshape(rows, width)
    unit, _ = standardize(tok)
    normed = (unit * norms_ref[0:1] + norms_ref[1:2]).astype(jnp.bfloat16)
    for c in range(3):
        for p in range(pieces):
            part = mm(normed, mats_ref[p, c]).reshape(images, length, columns)
            base = c * width + p * columns
            for b in range(images):
                proj_ref[first + b, :, base:base + columns] = part[b].astype(jnp.bfloat16)
    even = even_lanes((length, LANES))
    scale = jnp.bfloat16(HEAD ** -0.5)
    zero = jnp.zeros((), jnp.bfloat16)
    attended = []
    for b in range(images):
        bias = bias_ref[first + b]
        parts = []
        for pair in range(width // LANES):
            lanes = slice(pair * LANES, (pair + 1) * LANES)
            query = proj_ref[first + b, :, lanes] * scale
            keyed = proj_ref[first + b, :, width + pair * LANES:width + (pair + 1) * LANES]
            valued = proj_ref[first + b, :, 2 * width + pair * LANES:2 * width + (pair + 1) * LANES]
            halves = []
            for odd in range(2):
                chosen = jnp.where(even != bool(odd), query, zero)
                scores = mm(chosen, keyed, NT) + bias
                lifted = jnp.exp(scores - jnp.max(scores, -1, keepdims=True))
                probs = lifted * (1.0 / jnp.sum(lifted, -1, keepdims=True))
                halves.append(mm(probs.astype(jnp.bfloat16), valued))
            both = jnp.where(even, halves[0], halves[1])
            mixed_ref[first + b, :, lanes] = both.astype(jnp.bfloat16)
            parts.append(both)
        attended.append(jnp.concatenate(parts, 1))
    joined = jnp.concatenate(attended, 0).astype(jnp.bfloat16)
    middle = tok
    for p in range(pieces):
        middle += mm(joined[:, p * columns:(p + 1) * columns], mats_ref[p, 3], NT)
    middle_ref[here] = middle.reshape(images, length, width)
    unit, _ = standardize(middle)
    routed = unit * norms_ref[2:3] + norms_ref[3:4]
    low = routed.astype(jnp.bfloat16)
    gates_ref[here] = router_gates(low, parts_ref[...]).reshape(images, length, LANES)
    return routed, low


def forward_kernel(
    tok_ref, bias_ref, mats_ref, norms_ref, parts_ref,
    middle_ref, routed_ref, proj_ref, mixed_ref, gates_ref,
):
    images, length, width = tok_ref.shape
    routed, _ = forward_rows(0, images, tok_ref, bias_ref, mats_ref, norms_ref, parts_ref,
                             middle_ref, proj_ref, mixed_ref, gates_ref)
    routed_ref[...] = routed.reshape(images, length, width).astype(jnp.bfloat16)


def attention_forward(tok, bias, mats, norms, router, per_step):
    images, length, width = tok.shape

    def rows(last):
        return pl.BlockSpec((per_step, length, last), lambda s: (s, 0, 0))

    def whole(a):
        return pl.BlockSpec(a.shape, lambda s: (0,) * a.ndim)

    shapes = [
        (width, jnp.float32), (width, jnp.bfloat16), (3 * width, jnp.bfloat16),
        (width, jnp.bfloat16), (LANES, jnp.float32),
    ]
    return pl.pallas_call(
        forward_kernel,
        grid=(images // per_step,),
        in_specs=[
            rows(width), pl.BlockSpec((per_step, 1, length), lambda s: (s, 0, 0)),
            whole(mats), whole(norms), whole(router),
        ],
        out_specs=[rows(n) for n, _ in shapes],
        out_shape=[jax.ShapeDtypeStruct((images, length, n), kind) for n, kind in shapes],
        compiler_params=pltpu.CompilerParams(vmem_limit_bytes=VMEM),
        cost_estimate=pl.CostEstimate(
            flops=images * length * width * width * 10, bytes_accessed=images * length * width * 16,
            transcendentals=images * length * length * 8),
        name="attention_forward",
    )(tok, bias, mats, norms, router)


def backward_rows(first, images, grad, tok_ref, middle_ref, cot_ref, gates_ref, proj_ref, mixed_ref,
                  bias_ref, mats_ref, norms_ref, router_t_ref,
                  input_ref, dnorms_ref, drouter_ref, dproj_ref, dmats_acc):
    _, length, width = tok_ref.shape
    rows = images * length
    here = pl.ds(first, images)

    def flat(ref):
        return ref[here].reshape(rows, ref.shape[2])

    middle = flat(middle_ref)
    unit, inverse = standardize(middle)
    gates = flat(gates_ref)
    gate_cot = grad[:, width:]
    logit_grad = gates * (gate_cot - jnp.sum(gates * gate_cot, -1, keepdims=True))
    routed = (unit * norms_ref[2:3] + norms_ref[3:4]).astype(jnp.bfloat16)
    drouter_ref[...] += mm(routed.astype(jnp.float32), logit_grad, TN, HIGH)
    routed_grad = grad[:, :width] + mm(logit_grad, router_t_ref[...], NN, HIGH)
    dnorms_ref[2:3] += jnp.sum(routed_grad * unit, 0, keepdims=True)
    dnorms_ref[3:4] += jnp.sum(routed_grad, 0, keepdims=True)
    middle_grad = flat(cot_ref) + norm_back(routed_grad * norms_ref[2:3], unit, inverse)
    attn_cot = middle_grad.astype(jnp.bfloat16)
    joined = jnp.concatenate([mixed_ref[first + b].astype(jnp.float32) for b in range(images)], 0)
    joined = joined.astype(jnp.bfloat16)
    pieces, _, _, columns = mats_ref.shape
    spans = [slice(p * columns, (p + 1) * columns) for p in range(pieces)]
    for p in range(pieces):
        dmats_acc[p, 3] += mm(attn_cot, joined[:, spans[p]], TN)
    mixed_grad = jnp.concatenate([mm(attn_cot, mats_ref[p, 3]) for p in range(pieces)], 1)
    mixed_grad = mixed_grad.reshape(images, length, width)
    even = even_lanes((length, LANES))
    zero = jnp.zeros((), jnp.bfloat16)
    scale = jnp.bfloat16(HEAD ** -0.5)
    for b in range(images):
        bias = bias_ref[first + b]
        mixed_low = mixed_grad[b].astype(jnp.bfloat16)
        for pair in range(width // LANES):
            lanes = slice(pair * LANES, (pair + 1) * LANES)
            query = proj_ref[first + b, :, lanes] * scale
            keyed = proj_ref[first + b, :, width + pair * LANES:width + (pair + 1) * LANES]
            valued = proj_ref[first + b, :, 2 * width + pair * LANES:2 * width + (pair + 1) * LANES]
            out_cot = mixed_low[:, lanes]
            query_grad = keyed_grad = value_grad = None
            for odd in range(2):
                mask = even != bool(odd)
                query_half = jnp.where(mask, query, zero)
                keyed_half = jnp.where(mask, keyed, zero)
                cot_half = jnp.where(mask, out_cot, zero)
                scores = mm(query_half, keyed, NT) + bias
                lifted = jnp.exp(scores - jnp.max(scores, -1, keepdims=True))
                probs = lifted * (1.0 / jnp.sum(lifted, -1, keepdims=True))
                prob_grad = mm(cot_half, valued, NT)
                value_part = mm(probs.astype(jnp.bfloat16), cot_half, TN)
                inner = jnp.sum(probs * prob_grad, -1, keepdims=True)
                score_grad = (probs * (prob_grad - inner)).astype(jnp.bfloat16)
                query_part = mm(score_grad, keyed_half)
                keyed_part = mm(score_grad, query_half, TN)
                if odd:
                    query_grad, keyed_grad, value_grad = (
                        query_grad + query_part, keyed_grad + keyed_part, value_grad + value_part)
                else:
                    query_grad, keyed_grad, value_grad = query_part, keyed_part, value_part
            base = pair * LANES
            rows_here = slice(b * length, (b + 1) * length)
            dproj_ref[rows_here, base:base + LANES] = query_grad * (HEAD ** -0.5)
            dproj_ref[rows_here, width + base:width + base + LANES] = keyed_grad
            dproj_ref[rows_here, 2 * width + base:2 * width + base + LANES] = value_grad
    tok = flat(tok_ref)
    unit, inverse = standardize(tok)
    normed = (unit * norms_ref[0:1] + norms_ref[1:2]).astype(jnp.bfloat16)
    normed_grad = jnp.zeros((rows, width), jnp.float32)
    for c in range(3):
        part = dproj_ref[:, c * width:(c + 1) * width].astype(jnp.bfloat16)
        for p in range(pieces):
            dmats_acc[p, c] += mm(normed, part[:, spans[p]], TN)
            normed_grad += mm(part[:, spans[p]], mats_ref[p, c], NT)
    dnorms_ref[0:1] += jnp.sum(normed_grad * unit, 0, keepdims=True)
    dnorms_ref[1:2] += jnp.sum(normed_grad, 0, keepdims=True)
    input_grad = middle_grad + norm_back(normed_grad * norms_ref[0:1], unit, inverse)
    input_ref[here] = input_grad.reshape(images, length, width)


def backward_kernel(
    tok_ref, middle_ref, cot_ref, grad_ref, gates_ref, proj_ref, mixed_ref,
    bias_ref, mats_ref, norms_ref, router_t_ref,
    input_ref, dmats_ref, dnorms_ref, drouter_ref,
    dproj_ref, dmats_acc,
):
    images, length, width = tok_ref.shape
    rows = images * length
    step = pl.program_id(0)

    @pl.when(step == 0)
    def _():
        dmats_acc[...] = jnp.zeros_like(dmats_acc)
        dnorms_ref[...] = jnp.zeros_like(dnorms_ref)
        drouter_ref[...] = jnp.zeros_like(drouter_ref)

    backward_rows(0, images, grad_ref[...].reshape(rows, grad_ref.shape[2]), tok_ref, middle_ref, cot_ref,
                  gates_ref, proj_ref, mixed_ref, bias_ref, mats_ref, norms_ref, router_t_ref,
                  input_ref, dnorms_ref, drouter_ref, dproj_ref, dmats_acc)

    @pl.when(step == pl.num_programs(0) - 1)
    def _():
        dmats_ref[...] = dmats_acc[...].astype(jnp.bfloat16)


def attention_backward(tok, middle, cot, grad, gates, proj, mixed, bias, mats, norms, router_t, per_step):
    images, length, width = tok.shape

    def rows(last):
        return pl.BlockSpec((per_step, length, last), lambda s: (s, 0, 0))

    def whole(shape):
        return pl.BlockSpec(shape, lambda s: (0,) * len(shape))

    return pl.pallas_call(
        backward_kernel,
        grid=(images // per_step,),
        in_specs=[
            rows(width), rows(width), rows(width), rows(width + LANES), rows(LANES),
            rows(3 * width), rows(width), pl.BlockSpec((per_step, 1, length), lambda s: (s, 0, 0)),
            whole(mats.shape), whole(norms.shape), whole(router_t.shape),
        ],
        out_specs=[
            rows(width), whole(mats.shape), whole((4, width)), whole((width, LANES)),
        ],
        out_shape=[
            jax.ShapeDtypeStruct((images, length, width), jnp.float32),
            jax.ShapeDtypeStruct(mats.shape, jnp.bfloat16),
            jax.ShapeDtypeStruct((4, width), jnp.float32),
            jax.ShapeDtypeStruct((width, LANES), jnp.float32),
        ],
        scratch_shapes=[
            pltpu.VMEM((per_step * length, 3 * width), jnp.float32),
            pltpu.VMEM(mats.shape, jnp.float32),
        ],
        compiler_params=pltpu.CompilerParams(vmem_limit_bytes=VMEM),
        cost_estimate=pl.CostEstimate(
            flops=images * length * width * width * 30, bytes_accessed=images * length * width * 30,
            transcendentals=images * length * length * 8),
        name="attention_backward",
    )(tok, middle, cot, grad, gates, proj, mixed, bias, mats, norms, router_t)


def expert_kernel(
    expert_ref, slots_ref, cots_ref, weights_ref, router_ref,
    result_ref, back_ref, dweights_ref,
    rows_t, grads_t, grads, gate_scr, result_acc, back_acc, first_acc, second_acc,
):
    count, width = slots_ref.shape
    tile = weights_ref.shape[-1]
    chunk = rows_t.shape[2]
    step = pl.program_id(0)
    first = weights_ref[:, :, 0, 0].reshape(width, tile)
    second = weights_ref[:, :, 0, 1].reshape(width, tile)

    @pl.when(step == 0)
    def _():
        def prepare(r, carry):
            here = pl.ds(pl.multiple_of(r * chunk, 16), chunk)
            slots = slots_ref[here]
            gates = router_gates(slots, router_ref[...])
            lane = lax.broadcasted_iota(jnp.int32, gates.shape, 1)
            gate = jnp.sum(jnp.where(lane == expert_ref[0], gates, 0.0), -1, keepdims=True)
            gate_scr[here] = jnp.broadcast_to(gate, gates.shape)
            low = (cots_ref[here].astype(jnp.float32) * gate).astype(jnp.bfloat16)
            grads[here] = low
            rows_t[r] = slots.T
            grads_t[r] = low.T
            result_acc[here] = jnp.zeros((chunk, width), jnp.float32)
            back_acc[here] = jnp.zeros((chunk, width), jnp.float32)
            return carry

        lax.fori_loop(0, count // chunk, prepare, 0)

    first_acc[...] = jnp.zeros_like(first_acc)
    second_acc[...] = jnp.zeros_like(second_acc)

    def work(r, carry):
        here = pl.ds(pl.multiple_of(r * chunk, 16), chunk)
        pre = mm(slots_ref[here], first)
        square = pre * pre
        half = 0.5 + 0.5 * jnp.tanh(pre * (GELU_C + (GELU_C * GELU_A) * square))
        hidden = (pre * half).astype(jnp.bfloat16)
        slope = half + 2.0 * half * (1.0 - half) * pre * (GELU_C + (3.0 * GELU_C * GELU_A) * square)
        hidden_grad = mm(grads[here], second)
        pre_grad = (hidden_grad * slope).astype(jnp.bfloat16)
        result_acc[here] += mm(hidden, second, NT)
        back_acc[here] += mm(pre_grad, first, NT)
        first_acc[...] += mm(rows_t[r], pre_grad)
        second_acc[...] += mm(grads_t[r], hidden)
        return carry

    lax.fori_loop(0, count // chunk, work, 0)
    block = weights_ref.shape[:2] + weights_ref.shape[4:]
    dweights_ref[:, :, 0, 0] = first_acc[...].astype(jnp.bfloat16).reshape(block)
    dweights_ref[:, :, 0, 1] = second_acc[...].astype(jnp.bfloat16).reshape(block)

    @pl.when(step == pl.num_programs(0) - 1)
    def _():
        def finish(r, carry):
            here = pl.ds(pl.multiple_of(r * chunk, 16), chunk)
            result = result_acc[here]
            gate = gate_scr[here][:, 0:1]
            result_ref[here] = (result * gate).astype(jnp.bfloat16)
            gate_grad = jnp.sum(cots_ref[here].astype(jnp.float32) * result, -1, keepdims=True)
            lane = lax.broadcasted_iota(jnp.int32, (chunk, LANES), 1)
            back_ref[here, 0:width] = back_acc[here].astype(jnp.bfloat16)
            back_ref[here, width:width + LANES] = jnp.where(
                lane == expert_ref[0], gate_grad, 0.0).astype(jnp.bfloat16)
            return carry

        lax.fori_loop(0, count // chunk, finish, 0)


def run_expert(expert, slots, cots, weights, router):
    count, width = slots.shape
    planes, inner, parts, _, depth, extent = weights.shape
    tile = min(512, extent)
    per_part = extent // tile
    chunk = 480

    def whole(shape):
        return pl.BlockSpec(shape, lambda s, e: (0,) * len(shape))

    weight_spec = pl.BlockSpec(
        (planes, inner, 1, 2, depth, tile), lambda s, e: (0, 0, s // per_part, 0, 0, s % per_part))
    return pl.pallas_call(
        expert_kernel,
        grid_spec=pltpu.PrefetchScalarGridSpec(
            num_scalar_prefetch=1,
            grid=(parts * per_part,),
            in_specs=[whole(slots.shape), whole(cots.shape), weight_spec, whole(router.shape)],
            out_specs=[whole((count, width)), whole((count, width + LANES)), weight_spec],
            scratch_shapes=[
                pltpu.VMEM((count // chunk, width, chunk), jnp.bfloat16),
                pltpu.VMEM((count // chunk, width, chunk), jnp.bfloat16),
                pltpu.VMEM((count, width), jnp.bfloat16),
                pltpu.VMEM((count, LANES), jnp.float32),
                pltpu.VMEM((count, width), jnp.float32),
                pltpu.VMEM((count, width), jnp.float32),
                pltpu.VMEM((width, tile), jnp.float32),
                pltpu.VMEM((width, tile), jnp.float32),
            ],
        ),
        out_shape=[
            jax.ShapeDtypeStruct((count, width), jnp.bfloat16),
            jax.ShapeDtypeStruct((count, width + LANES), jnp.bfloat16),
            jax.ShapeDtypeStruct(weights.shape, jnp.bfloat16),
        ],
        compiler_params=pltpu.CompilerParams(vmem_limit_bytes=VMEM),
        cost_estimate=pl.CostEstimate(
            flops=12 * count * width * extent * parts,
            bytes_accessed=4 * 2 * width * extent * parts + count * width * 8,
            transcendentals=count * extent * parts),
        name="expert",
    )(expert, slots, cots, weights, router)


def flipped(position, bit):
    return position + bit - 2 * bit * lax.rem(position // bit, 2)


def to_peer(source, target, sends, receives, where):
    return pltpu.make_async_remote_copy(
        src_ref=source, dst_ref=target, send_sem=sends, recv_sem=receives, device_id=where,
        device_id_type=pl.DeviceIdType.MESH)


class Dispatch:
    def __init__(self, index_ref, shared, staged, out, sends, receives, keep, inner, parts, local):
        self.index_ref, self.shared, self.staged, self.out = index_ref, shared, staged, out
        self.sends, self.receives, self.keep = sends, receives, keep
        self.inner, self.parts, self.local = inner, parts, local
        self.at_i, self.at_t = lax.axis_index("i"), lax.axis_index("t")

    def copy(self, m, d, k):
        home = lax.rem(self.at_i + d, self.inner)
        target = self.out.at[k, pl.ds(pl.multiple_of((m * self.inner + self.at_i) * CAP, 8), CAP)]
        return to_peer(self.staged.at[m, d, k], target, self.sends.at[m, d, k],
                       self.receives.at[m, d, k], {"i": home})

    def kept(self, m, k):
        target = self.out.at[k, pl.ds(pl.multiple_of((m * self.inner + self.at_i) * CAP, 8), CAP)]
        return pltpu.make_async_copy(self.staged.at[m, 0, k], target, self.keep.at[m, k])

    def fill(self, m, d):
        home = lax.rem(self.at_i + d, self.inner)
        count = self.local * CAP
        base = (home * self.parts + self.at_t) * count
        places = base + lax.broadcasted_iota(jnp.int32, (count, 1), 0)
        total = None
        for half in range(2):
            first = self.index_ref[m, 0, half:half + 1]
            second = self.index_ref[m, 1, half:half + 1]
            hits = jnp.where((first == places) | (second == places), 1.0, 0.0).astype(jnp.bfloat16)
            part = mm(hits, self.shared[m, half])
            total = part if total is None else total + part
        for k in range(self.local):
            self.staged[m, d, k] = total[k * CAP:(k + 1) * CAP].astype(jnp.bfloat16)

    def send(self, m, beside=None):
        def step(d, carry):
            self.fill(m, d)
            for k in range(self.local):
                self.copy(m, d, k).start()
            if beside is not None:
                beside(d)
            return carry

        lax.fori_loop(1, self.inner, step, 0)
        self.fill(m, 0)
        for k in range(self.local):
            self.kept(m, k).start()

    def finish(self, m):
        def step(d, carry):
            for k in range(self.local):
                self.copy(m, d, k).wait()
            return carry

        lax.fori_loop(1, self.inner, step, 0)
        for k in range(self.local):
            self.kept(m, k).wait()


def flipped_if(position, bit, on):
    return position + on * (bit - 2 * bit * lax.rem(position // bit, 2))


class Answer:
    def __init__(self, staged, out, sends, receives, keep, inner):
        self.staged, self.out, self.sends, self.receives, self.keep = staged, out, sends, receives, keep
        self.inner = inner
        self.at_i = lax.axis_index("i")

    def target(self, k, m):
        return self.out.at[k, m, pl.ds(pl.multiple_of(self.at_i * CAP, 8), CAP)]

    def copy(self, k, m, d):
        group = lax.rem(self.at_i + d, self.inner)
        return to_peer(self.staged.at[m, group, k], self.target(k, m), self.sends.at[k, m, d],
                       self.receives.at[k, m, d], {"i": group})

    def kept(self, k, m):
        return pltpu.make_async_copy(self.staged.at[m, self.at_i, k], self.target(k, m), self.keep.at[k, m])

    def send(self, k, m, beside=None):
        def step(d, carry):
            self.copy(k, m, d).start()
            if beside is not None:
                beside(d)
            return carry

        lax.fori_loop(1, self.inner, step, 0)
        self.kept(k, m).start()

    def finish(self, k, m):
        def step(d, carry):
            self.copy(k, m, d).wait()
            return carry

        lax.fori_loop(1, self.inner, step, 0)
        self.kept(k, m).wait()


def device_at(n, origin):
    o, i, t = origin
    return lax.rem(o + n // 16, 2), lax.rem(i + lax.rem(n // 2, 8), 8), lax.rem(t + lax.rem(n, 2), 2)


class Weights:
    def __init__(self, local, sources, target, sends, receives, keep):
        self.local, self.sources, self.target = local, sources, target
        self.sends, self.receives, self.keep = sends, receives, keep
        self.origin = tuple(lax.axis_index(name) for name in ("o", "i", "t"))

    def place(self, k, part):
        o, i, t = self.origin
        return self.target.at[k, o, i, t, part]

    def copy(self, k, n, part):
        o, i, t = device_at(n, self.origin)
        expert = (i * 2 + t) * self.local + k
        return to_peer(self.sources[part].at[expert], self.place(k, part), self.sends.at[k, n, part],
                       self.receives.at[k, n, part], {"o": o, "i": i, "t": t})

    def kept(self, k, part):
        _, i, t = self.origin
        expert = (i * 2 + t) * self.local + k
        return pltpu.make_async_copy(
            self.sources[part].at[expert], self.place(k, part), self.keep.at[k, part])

    def give(self, k, n):
        for part in range(2):
            self.copy(k, n, part).start()

    def give_all(self, k, first, last):
        def step(n, carry):
            self.give(k, n)
            return carry

        lax.fori_loop(first, last, step, 0)

    def keep_own(self, k):
        for part in range(2):
            self.kept(k, part).start()

    def finish(self, k):
        def step(n, carry):
            for part in range(2):
                self.copy(k, n, part).wait()
            return carry

        lax.fori_loop(1, 32, step, 0)
        for part in range(2):
            self.kept(k, part).wait()


class Gradients:
    def __init__(self, local, source, target, sends, receives, keep):
        self.local, self.source, self.target = local, source, target
        self.sends, self.receives, self.keep = sends, receives, keep
        self.origin = tuple(lax.axis_index(name) for name in ("o", "i", "t"))

    def place(self, k, part):
        o, i, t = self.origin
        return self.target.at[o, (i * 2 + t) * self.local + k, part]

    def copy(self, k, n, part):
        o, i, t = device_at(n, self.origin)
        return to_peer(self.source.at[k, o, i, t, part], self.place(k, part), self.sends.at[k, n, part],
                       self.receives.at[k, n, part], {"o": o, "i": i, "t": t})

    def kept(self, k, part):
        o, i, t = self.origin
        return pltpu.make_async_copy(
            self.source.at[k, o, i, t, part], self.place(k, part), self.keep.at[k, part])

    give = Weights.give
    give_all = Weights.give_all
    keep_own = Weights.keep_own
    finish = Weights.finish


def expert_scratch(count, width, tile, chunk):
    steps = count // chunk
    return [
        pltpu.VMEM((count, width), jnp.bfloat16), pltpu.VMEM((count, width), jnp.bfloat16),
        pltpu.VMEM((steps, width, chunk), jnp.bfloat16), pltpu.VMEM((steps, width, chunk), jnp.bfloat16),
        pltpu.VMEM((count, width), jnp.bfloat16), pltpu.VMEM((count, LANES), jnp.float32),
        pltpu.VMEM((count, width), jnp.float32), pltpu.VMEM((count, width), jnp.float32),
        pltpu.VMEM((2, width, tile), jnp.float32), pltpu.VMEM((2, width, tile), jnp.bfloat16),
        pltpu.SemaphoreType.DMA((2,)),
    ]


def expert_phase(k, expert, slots_hbm, cots_hbm, held, parts_ref, answers, gradients, scratch):
    slots, cots, rows_t, grads_t, grads, gate_scr, result_acc, back_acc, sums, tiles, load = scratch
    count, width = slots.shape
    chunk = rows_t.shape[2]
    tile = tiles.shape[2]
    micros, groups = answers[0].staged.shape[:2]
    loads = [pltpu.make_async_copy(slots_hbm.at[k], slots, load.at[0]),
             pltpu.make_async_copy(cots_hbm.at[k], cots, load.at[1])]
    for copy in loads:
        copy.start()
    for copy in loads:
        copy.wait()

    def prepare(r, carry):
        here = pl.ds(pl.multiple_of(r * chunk, 16), chunk)
        rows = slots[here]
        gates = router_gates(rows, parts_ref[...])
        lane = lax.broadcasted_iota(jnp.int32, gates.shape, 1)
        gate = jnp.sum(jnp.where(lane == expert, gates, 0.0), -1, keepdims=True)
        gate_scr[here] = jnp.broadcast_to(gate, gates.shape)
        low = (cots[here].astype(jnp.float32) * gate).astype(jnp.bfloat16)
        grads[here] = low
        rows_t[r] = rows.T
        grads_t[r] = low.T
        result_acc[here] = jnp.zeros((chunk, width), jnp.float32)
        back_acc[here] = jnp.zeros((chunk, width), jnp.float32)
        return carry

    lax.fori_loop(0, count // chunk, prepare, 0)
    per_part = held.shape[6] // tile

    def one_tile(n, carry):
        t = n // per_part
        span = pl.ds(pl.multiple_of(lax.rem(n, per_part) * tile, tile), tile)
        for part in range(2):
            tiles[part] = held[k, :, :, t, part, :, span].reshape(width, tile)
        sums[...] = jnp.zeros_like(sums)

        def work(r, inside):
            here = pl.ds(pl.multiple_of(r * chunk, 16), chunk)
            pre = mm(slots[here], tiles[0])
            square = pre * pre
            half = 0.5 + 0.5 * jnp.tanh(pre * (GELU_C + (GELU_C * GELU_A) * square))
            hidden = (pre * half).astype(jnp.bfloat16)
            slope = half + 2.0 * half * (1.0 - half) * pre * (
                GELU_C + (3.0 * GELU_C * GELU_A) * square)
            pre_grad = (mm(grads[here], tiles[1]) * slope).astype(jnp.bfloat16)
            result_acc[here] += mm(hidden, tiles[1], NT)
            back_acc[here] += mm(pre_grad, tiles[0], NT)
            sums[0] += mm(rows_t[r], pre_grad)
            sums[1] += mm(grads_t[r], hidden)
            return inside

        lax.fori_loop(0, count // chunk, work, 0)
        block = held.shape[1:3] + (held.shape[5], tile)
        for part in range(2):
            held[k, :, :, t, part, :, span] = sums[part].astype(jnp.bfloat16).reshape(block)
        return carry

    lax.fori_loop(0, held.shape[3] * per_part, one_tile, 0)
    per_chunk = chunk // CAP
    back, result = answers

    def finish(n, carry):
        here = pl.ds(pl.multiple_of(n * chunk, 16), chunk)
        m, r = n // (groups // per_chunk), lax.rem(n, groups // per_chunk)
        value = result_acc[here]
        gate_grad = jnp.sum(cots[here].astype(jnp.float32) * value, -1, keepdims=True)
        lane = lax.broadcasted_iota(jnp.int32, (chunk, LANES), 1)
        spread = jnp.where(lane == expert, gate_grad, 0.0)
        value = value * gate_scr[here][:, 0:1]
        grad = back_acc[here]
        for q in range(per_chunk):
            rows = slice(q * CAP, (q + 1) * CAP)
            at = r * per_chunk + q
            result.staged[m, at, k] = value[rows].astype(jnp.bfloat16)
            back.staged[m, at, k, :, 0:width] = grad[rows].astype(jnp.bfloat16)
            back.staged[m, at, k, :, width:width + LANES] = spread[rows].astype(jnp.bfloat16)
        return carry

    lax.fori_loop(0, micros * groups // per_chunk, finish, 0)

    def one_more(d):
        @pl.when(k == 0)
        def _():
            gradients.give(0, 15 + d)

    for m in range(micros):
        back.send(k, m, one_more if m == 0 else None)

    @pl.when(k == 0)
    def _():
        gradients.give_all(0, 23, 26)


def opening_kernel(
    local, per_step, pack_ref, cot_ref, index_ref, table_ref, tok_ref, bias_ref, first_ref, second_ref,
    small_ref, block_out, input_out, dweights_ref, middle_out, proj_out, mixed_out, gates_out,
    slots_ref, cots_ref, back_ref, result_ref,
    gathered, partial, loose, mats_ref, norms_ref, parts_ref, router_ref, shared_c, shared_r, away_g,
    staged_c, staged_r, held, staged_back,
    load, ring_send, ring_recv, pair_send, pair_recv, pair_send_r, pair_recv_r,
    cot_send, cot_recv, cot_keep, row_send, row_recv, row_keep,
    weight_send, weight_recv, weight_keep, grad_send, grad_recv, grad_keep,
    back_send, back_recv, back_keep, result_send, result_recv, result_keep, store,
    away_send, away_recv, fold_send, fold_recv, fetch,
):
    at_o, at_i, at_t = (lax.axis_index(name) for name in ("o", "i", "t"))
    micros, _, own_rows, width = shared_c.shape
    images, length, _ = tok_ref.shape
    kinds, columns = mats_ref.shape[1], mats_ref.shape[3]
    depth = width // 16
    rows = per_step * length
    steps = own_rows // rows
    stages = [
        {"t": 1 - at_t}, {"o": 1 - at_o}, {"i": flipped(at_i, 4)}, {"i": flipped(at_i, 2)},
        {"i": flipped(at_i, 1)},
    ]
    cot_plan = Dispatch(index_ref, shared_c, staged_c, cots_ref, cot_send, cot_recv, cot_keep, 8, 2, local)
    row_plan = Dispatch(index_ref, shared_r, staged_r, slots_ref, row_send, row_recv, row_keep, 8, 2, local)
    weights = Weights(local, (first_ref, second_ref), held, weight_send, weight_recv, weight_keep)
    gradients = Gradients(local, held, dweights_ref, grad_send, grad_recv, grad_keep)

    def stage(j):
        size = 2 ** j
        return to_peer(gathered.at[pl.ds(0, size)], gathered.at[pl.ds(size, size)],
                       ring_send.at[j], ring_recv.at[j], stages[j])

    def swap_c(m):
        return to_peer(shared_c.at[m, 0], shared_c.at[m, 1], pair_send.at[m], pair_recv.at[m],
                       {"t": 1 - at_t})

    def swap_r(m, s):
        here = pl.ds(pl.multiple_of(s * rows, 16), rows)
        return to_peer(shared_r.at[m, 0, here], shared_r.at[m, 1, here], pair_send_r.at[m, s],
                       pair_recv_r.at[m, s], {"t": 1 - at_t})

    def relative(r):
        o = flipped_if(at_o, 1, lax.rem(r // 2, 2))
        i = flipped_if(at_i, 4, lax.rem(r // 4, 2))
        i = flipped_if(i, 2, lax.rem(r // 8, 2))
        i = flipped_if(i, 1, lax.rem(r // 16, 2))
        return o, i, flipped_if(at_t, 1, lax.rem(r, 2))

    def opening(tok, cot, proj, mixed, gates):
        fill = pltpu.make_async_copy(pack_ref, gathered.at[0], load.at[0])
        take_cot = pltpu.make_async_copy(cot_ref, cot, load.at[1])
        take_tok = pltpu.make_async_copy(tok_ref, tok, load.at[2])
        fill.start()
        take_cot.start()
        take_tok.start()
        fill.wait()
        stage(0).start()
        take_cot.wait()
        shared_c[0, 0] = cot[0:images // 2].reshape(own_rows, width).astype(jnp.bfloat16)
        swap_c(0).start()
        stage(0).wait()
        stage(1).start()
        shared_c[1, 0] = cot[images // 2:].reshape(own_rows, width).astype(jnp.bfloat16)
        swap_c(1).start()
        stage(1).wait()
        stage(2).start()
        stage(2).wait()
        stage(3).start()
        weights.give_all(0, 30, 32)
        swap_c(0).wait()
        cot_plan.send(0, lambda d: weights.give(0, d + 15))
        stage(3).wait()
        stage(4).start()
        swap_c(1).wait()
        cot_plan.send(1, lambda d: weights.give(0, d + 22))
        weights.give_all(0, 1, 16)
        weights.keep_own(0)
        stage(4).wait()

        def place(r, carry):
            o, i, t = relative(r)
            row = pl.multiple_of((o * 8 + i) * depth, depth)
            for c in range(kinds):
                mats_ref[t, c, pl.ds(row, depth)] = gathered[r, c * depth:(c + 1) * depth]
            loose[(o * 8 + i) * 2 + t] = gathered[r, kinds * depth:, 0:LANES].astype(jnp.float32)
            return carry

        lax.fori_loop(0, gathered.shape[0], place, 0)
        turned = loose[...].reshape(width, LANES).T
        norms_ref[...] = turned[96:104] + turned[104:112] + turned[112:120]
        low = turned[0:96].astype(jnp.bfloat16)
        parts_ref[...] = jnp.concatenate([low, jnp.zeros((32, width), jnp.bfloat16)], 0)
        router_ref[0:32] = turned[0:32] + turned[32:64] + turned[64:96]
        router_ref[32:] = jnp.zeros((96, width), jnp.float32)
        take_tok.wait()

        def attend(n, carry):
            m, s = n // steps, lax.rem(n, steps)
            _, routed = forward_rows(n * per_step, per_step, tok, bias_ref, mats_ref, norms_ref, parts_ref,
                                     tok, proj, mixed, gates)
            shared_r[m, 0, pl.ds(pl.multiple_of(s * rows, 16), rows)] = routed
            swap_r(m, s).start()
            return carry

        lax.fori_loop(0, micros * steps, attend, 0)
        outs = [(tok, middle_out), (proj, proj_out), (mixed, mixed_out), (gates, gates_out)]
        stores = [pltpu.make_async_copy(a, b, store.at[n]) for n, (a, b) in enumerate(outs)]
        for copy in stores:
            copy.start()
        for m in range(micros):
            for s in range(steps):
                swap_r(m, s).wait()
            row_plan.send(m, (lambda d: weights.give(1, d + 15)) if m == 0 else None)
        weights.give_all(1, 23, 32)
        weights.give_all(1, 1, 16)
        weights.keep_own(1)
        for copy in stores:
            copy.wait()

    pl.run_scoped(
        opening,
        pltpu.VMEM(tok_ref.shape, jnp.float32),
        pltpu.VMEM(cot_ref.shape, jnp.float32),
        pltpu.VMEM((images, length, 3 * width), jnp.bfloat16),
        pltpu.VMEM((images, length, width), jnp.bfloat16),
        pltpu.VMEM((images, length, LANES), jnp.float32),
    )
    for m in range(micros):
        row_plan.finish(m)
        cot_plan.finish(m)
    back = Answer(staged_back, back_ref, back_send, back_recv, back_keep, 8)
    result = Answer(staged_c, result_ref, result_send, result_recv, result_keep, 8)
    count = slots_ref.shape[1]

    def experts(*scratch):
        def one(k, carry):
            weights.finish(k)
            expert = (at_i * 2 + at_t) * local + k
            expert_phase(k, expert, slots_ref, cots_ref, held, parts_ref, (back, result), gradients, scratch)
            return carry

        lax.fori_loop(0, local, one, 0)

    pl.run_scoped(experts, *expert_scratch(count, width, 512, 480))

    gradients.give_all(0, 26, 32)
    result.send(0, 0, lambda d: gradients.give(1, 15 + d))
    result.send(0, 1, lambda d: gradients.give(1, 22 + d))
    gradients.give_all(1, 30, 32)
    for m in range(micros):
        result.send(1, m)

    def rest(k, carry):
        gradients.give_all(k, 1, 16)
        gradients.keep_own(k)
        return carry

    lax.fori_loop(0, local, rest, 0)

    places = lax.broadcasted_iota(jnp.int32, (1, 8 * CAP), 1)
    block = sum((places >= q * CAP).astype(jnp.int32) for q in range(1, 8))
    places = places + block * (3 * CAP) + at_t * (2 * CAP)

    def taken(table, m, half, here, values):
        first, second = table[m, half, here, 0:1], table[m, half, here, 1:2]
        total = None
        for k in range(local):
            where = places + k * CAP
            hits = jnp.where((first == where) | (second == where), 1.0, 0.0).astype(jnp.bfloat16)
            part = mm(hits, values[k])
            total = part if total is None else total + part
        return total

    across = {"t": 1 - at_t}

    def away(m, s, which):
        here = pl.ds(pl.multiple_of(s * rows, 16), rows)
        buffer = (shared_r, away_g, shared_c)[which]
        return to_peer(buffer.at[m, 0, here], buffer.at[m, 1, here], away_send.at[which, m, s],
                       away_recv.at[which, m, s], across)

    def collect(own):
        def fetched(table, backs):
            take = pltpu.make_async_copy(table_ref, table, fetch.at[2])
            take.start()
            take.wait()
            for m in range(micros):
                for k in range(local):
                    back.finish(k, m)
                    pltpu.make_async_copy(back_ref.at[k, m], backs.at[k], fetch.at[k]).start()
                for k in range(local):
                    pltpu.make_async_copy(back_ref.at[k, m], backs.at[k], fetch.at[k]).wait()

                def leave(s, carry):
                    here = pl.ds(pl.multiple_of(s * rows, 16), rows)
                    total = taken(table, m, 1, here, backs).astype(jnp.bfloat16)
                    shared_r[m, 0, here] = total[:, :width]
                    away_g[m, 0, here] = total[:, width:]
                    away(m, s, 0).start()
                    away(m, s, 1).start()
                    return carry

                lax.fori_loop(0, steps, leave, 0)

                def stay(s, carry):
                    here = pl.ds(pl.multiple_of(s * rows, 16), rows)
                    own[m * steps + s] = taken(table, m, 0, here, backs)
                    return carry

                lax.fori_loop(0, steps, stay, 0)

        pl.run_scoped(
            fetched, pltpu.VMEM(table_ref.shape, jnp.int32), pltpu.VMEM((local, 8 * CAP, width + LANES), jnp.bfloat16))

        def backward(tok, middle, cot, proj, mixed, gates, dproj, dmats, dnorms, drouter):
            dmats[...] = jnp.zeros_like(dmats)
            dnorms[...] = jnp.zeros_like(dnorms)
            drouter[...] = jnp.zeros_like(drouter)
            pairs = [(tok_ref, tok), (middle_out, middle), (cot_ref, cot), (proj_out, proj),
                     (mixed_out, mixed), (gates_out, gates)]

            def micro(m, carry):
                ours = pl.ds(m * (images // micros), images // micros)
                takes = [pltpu.make_async_copy(a.at[ours], b, fetch.at[n]) for n, (a, b) in enumerate(pairs)]
                for copy in takes:
                    copy.start()
                for copy in takes:
                    copy.wait()

                def attend(s, inside):
                    away(m, s, 0).wait()
                    away(m, s, 1).wait()
                    here = pl.ds(pl.multiple_of(s * rows, 16), rows)
                    grad = own[m * steps + s] + jnp.concatenate([
                        shared_r[m, 1, here].astype(jnp.float32), away_g[m, 1, here].astype(jnp.float32)], 1)
                    backward_rows(s * per_step, per_step, grad, tok, middle, cot, gates, proj, mixed,
                                  bias_ref.at[ours], mats_ref, norms_ref, router_ref, cot, dnorms, drouter,
                                  dproj, dmats)
                    return inside

                lax.fori_loop(0, steps, attend, 0)
                keep = pltpu.make_async_copy(cot, input_out.at[ours], store.at[0])
                keep.start()
                keep.wait()
                return carry

            lax.fori_loop(0, micros, micro, 0)
            tail = jnp.concatenate(
                [jnp.zeros((96, width), jnp.float32), dnorms[...], jnp.zeros((24, width), jnp.float32)], 0)
            drouter[...] += tail.T

            def spread(r, carry):
                o, i, t = relative(r)
                row = pl.multiple_of((o * 8 + i) * depth, depth)
                for c in range(kinds):
                    gathered[r, c * depth:(c + 1) * depth] = dmats[t, c, pl.ds(row, depth)].astype(jnp.bfloat16)
                row = pl.multiple_of(((o * 8 + i) * 2 + t) * 16, 16)
                gathered[r, kinds * depth:, 0:LANES] = drouter[pl.ds(row, 16)].astype(jnp.bfloat16)
                gathered[r, kinds * depth:, LANES:] = jnp.zeros((16, columns - LANES), jnp.bfloat16)
                return carry

            lax.fori_loop(0, gathered.shape[0], spread, 0)

        some = images // micros
        pl.run_scoped(
            backward,
            pltpu.VMEM((some, length, width), jnp.float32),
            pltpu.VMEM((some, length, width), jnp.float32),
            pltpu.VMEM((some, length, width), jnp.float32),
            pltpu.VMEM((some, length, 3 * width), jnp.bfloat16),
            pltpu.VMEM((some, length, width), jnp.bfloat16),
            pltpu.VMEM((some, length, LANES), jnp.float32),
            pltpu.VMEM((rows, 3 * width), jnp.float32),
            pltpu.VMEM(mats_ref.shape, jnp.float32),
            pltpu.VMEM((8, width), jnp.float32),
            pltpu.VMEM((width, LANES), jnp.float32),
        )

    pl.run_scoped(collect, pltpu.VMEM((micros * steps, rows, width + LANES), jnp.float32))

    def fold(j):
        size = 2 ** j
        return to_peer(gathered.at[pl.ds(size, size)], partial.at[pl.ds(size, size)],
                       fold_send.at[j], fold_recv.at[j], stages[j])

    def folded(j):
        fold(j).wait()
        size = 2 ** j

        def add(r, carry):
            gathered[r] = (gathered[r].astype(jnp.float32) + partial[size + r].astype(jnp.float32)).astype(
                jnp.bfloat16)
            return carry

        lax.fori_loop(0, size, add, 0)

    def outputs(table, middle, results):
        fold(4).start()
        index_take = pltpu.make_async_copy(table_ref, table, fetch.at[3])
        index_take.start()
        take = pltpu.make_async_copy(middle_out, middle, fetch.at[2])
        take.start()
        def load(m, k):
            return pltpu.make_async_copy(result_ref.at[k, m], results.at[m, k], fetch.at[4 + k])

        index_take.wait()
        for m in range(micros):
            for k in range(local):
                result.finish(k, m)
                load(m, k).start()
            for k in range(local):
                load(m, k).wait()

            def leave(s, carry):
                here = pl.ds(pl.multiple_of(s * rows, 16), rows)
                shared_c[m, 0, here] = taken(table, m, 1, here, results.at[m]).astype(jnp.bfloat16)
                away(m, s, 2).start()
                return carry

            lax.fori_loop(0, steps, leave, 0)
        folded(4)
        fold(3).start()
        take.wait()
        for m in range(micros):
            def stay(s, carry):
                n = m * steps + s
                here = pl.ds(pl.multiple_of(s * rows, 16), rows)
                away(m, s, 2).wait()
                total = taken(table, m, 0, here, results.at[m]) + shared_c[m, 1, here].astype(jnp.float32)
                images_here = pl.ds(n * per_step, per_step)
                middle[images_here] = middle[images_here] + total.reshape(per_step, length, width)
                return carry

            lax.fori_loop(0, steps, stay, 0)
            if m == 0:
                folded(3)
                fold(2).start()
        keep = pltpu.make_async_copy(middle, block_out, store.at[0])
        keep.start()
        for j in (2, 1):
            folded(j)
            fold(j - 1).start()
        fold(0).wait()
        small_ref[...] = gathered[0].astype(jnp.float32) + partial[1].astype(jnp.float32)
        keep.wait()

    pl.run_scoped(
        outputs, pltpu.VMEM(table_ref.shape, jnp.int32), pltpu.VMEM(tok_ref.shape, jnp.float32),
        pltpu.VMEM((micros, local, 8 * CAP, width), jnp.bfloat16))

    def close(k, carry):
        gradients.finish(k)
        return carry

    lax.fori_loop(0, local, close, 0)


def opening(pack, cot, index, table, tok, bias, first_in, second_in, local, per_step):
    micros, own_rows = index.shape[0], index.shape[3]
    images, length, width = tok.shape
    columns = pack.shape[1]
    experts, depth, extent = first_in.shape
    steps = own_rows // (per_step * length)
    slots = micros * 8 * CAP
    anywhere = pl.BlockSpec(memory_space=pl.ANY)
    vector = pl.BlockSpec(memory_space=pltpu.VMEM)
    dma = pltpu.SemaphoreType.DMA
    low, wide = jnp.bfloat16, jnp.float32
    weights = (local, 2, 8, 2, 2, depth, extent)
    shape = jax.ShapeDtypeStruct
    return pl.pallas_call(
        functools.partial(opening_kernel, local, per_step),
        in_specs=[anywhere, anywhere, vector, anywhere, anywhere, vector, anywhere, anywhere],
        out_specs=[vector] + [anywhere] * 11,
        out_shape=[
            shape(pack.shape, wide), shape(tok.shape, wide), shape(tok.shape, wide),
            shape((2, experts, 2, depth, extent), low),
            shape((images, length, width), wide), shape((images, length, 3 * width), low),
            shape((images, length, width), low), shape((images, length, LANES), wide),
            shape((local, slots, width), low), shape((local, slots, width), low),
            shape((local, micros, 8 * CAP, width + LANES), low), shape((local, micros, 8 * CAP, width), low),
        ],
        scratch_shapes=[
            pltpu.VMEM((32,) + pack.shape, low),
            pltpu.VMEM((32,) + pack.shape, low),
            pltpu.VMEM((32, width // 32, LANES), wide),
            pltpu.VMEM((2, 4, width, columns), low), pltpu.VMEM((8, width), wide),
            pltpu.VMEM((LANES, width), low), pltpu.VMEM((LANES, width), wide),
            pltpu.VMEM((micros, 2, own_rows, width), low),
            pltpu.VMEM((micros, 2, own_rows, width), low),
            pltpu.VMEM((micros, 2, own_rows, LANES), low),
            pltpu.VMEM((micros, 8, local, CAP, width), low),
            pltpu.VMEM((micros, 8, local, CAP, width), low),
            pltpu.VMEM(weights, low),
            pltpu.VMEM((micros, 8, local, CAP, width + LANES), low),
            dma((3,)), dma((5,)), dma((5,)), dma((micros,)), dma((micros,)),
            dma((micros, steps)), dma((micros, steps)),
            dma((micros, 8, local)), dma((micros, 8, local)), dma((micros, local)),
            dma((micros, 8, local)), dma((micros, 8, local)), dma((micros, local)),
            dma((local, 32, 2)), dma((local, 32, 2)), dma((local, 2)),
            dma((local, 32, 2)), dma((local, 32, 2)), dma((local, 2)),
            dma((local, micros, 8)), dma((local, micros, 8)), dma((local, micros)),
            dma((local, micros, 8)), dma((local, micros, 8)), dma((local, micros)), dma((4,)),
            dma((3, micros, steps)), dma((3, micros, steps)), dma((5,)), dma((5,)), dma((6,)),
        ],
        compiler_params=pltpu.CompilerParams(vmem_limit_bytes=67043328, has_side_effects=True),
        cost_estimate=pl.CostEstimate(flops=1000, bytes_accessed=1000, transcendentals=0),
        name="opening",
    )(pack, cot, index, table, tok, bias, first_in, second_in)


def per_device(planes, inner, parts, tokens, key_mask, expert_ids, slot_ids, norm1_gain, norm1_bias,
               qkv_weight, out_weight, norm2_gain, norm2_bias, router_weight, expert_in, expert_out,
               cotangent):
    micros, own_rows, width = tokens.shape
    length = key_mask.shape[2]
    group_rows = own_rows * parts
    images = own_rows // length
    total = micros * images
    experts = expert_in.shape[0]
    homes = inner * parts
    local = experts // homes
    depth, extent = expert_in.shape[1:]
    small = norm1_gain.shape[0]
    every = ("o", "i", "t")
    plane_at, inner_at, part_at = (lax.axis_index(name) for name in every)
    low = jnp.bfloat16

    loose = jnp.concatenate([
        jnp.stack([norm1_gain, norm1_bias, norm2_gain, norm2_bias], 1), router_weight], 1)
    loose_count = 3 * loose.size
    columns = qkv_weight.shape[2]
    loose_rows = -(-loose_count // (16 * columns)) * 16
    loose_low = jnp.concatenate([p.reshape(-1) for p in three_parts(loose)])
    loose_low = jnp.pad(loose_low, (0, loose_rows * columns - loose_count)).reshape(loose_rows, columns)
    packed = jnp.concatenate([
        qkv_weight.transpose(1, 0, 2).reshape(3 * depth, columns), out_weight.T, loose_low], 0)
    gathered = lax.all_gather(packed, ("o", "i"), axis=0)
    gathered = lax.all_gather(gathered, "t", axis=0)
    mats = gathered[:, :, :4 * depth].reshape(parts, planes * inner, 4, depth, columns)
    mats = mats.transpose(2, 1, 3, 0, 4).reshape(1, 4, width, width)
    loose_all = gathered[:, :, 4 * depth:].reshape(parts, planes * inner, loose_rows * columns)
    loose_all = loose_all[:, :, :loose_count].astype(jnp.float32)
    loose_all = loose_all.reshape(parts, planes * inner, 3, small, 4 + experts)
    loose_all = (loose_all[:, :, 0] + loose_all[:, :, 1]) + loose_all[:, :, 2]
    loose_all = loose_all.transpose(1, 0, 2, 3).reshape(width, 4 + experts)
    norms = loose_all[:, :4].T
    router = jnp.pad(loose_all[:, 4:], ((0, 0), (0, LANES - experts)))
    router_parts = jnp.concatenate(three_parts(router[:, :experts]), 1).T
    router_parts = jnp.pad(router_parts, ((0, LANES - 3 * experts), (0, 0)))

    weights = []
    first_in = expert_in.reshape(homes, local, depth, extent)
    second_in = expert_out.transpose(0, 2, 1).reshape(homes, local, depth, extent)
    for k in range(local):
        both = jnp.stack([first_in[:, k], second_in[:, k]], 1)
        mine = lax.all_to_all(both, ("i", "t"), 0, 0, tiled=True)
        if planes == 2:
            other = lax.ppermute(mine, "o", [(0, 1), (1, 0)])
            full = jnp.where(plane_at == 0, jnp.stack([mine, other]), jnp.stack([other, mine]))
        else:
            full = lax.all_gather(mine, "o", axis=0)
        weights.append(full.reshape(planes, inner, parts, 2, depth, extent))

    own_first = part_at * own_rows
    slot_index = jnp.where(slot_ids >= 0, expert_ids * CAP + slot_ids, -1)
    if parts == 2:
        slot_index = jnp.concatenate([
            lax.dynamic_slice_in_dim(slot_index, own_first, own_rows, 1),
            lax.dynamic_slice_in_dim(slot_index, own_rows - own_first, own_rows, 1)], 1)
    homes_i = lax.broadcasted_iota(jnp.int32, (inner, local, CAP), 0)
    locals_i = lax.broadcasted_iota(jnp.int32, (inner, local, CAP), 1)
    cap_i = lax.broadcasted_iota(jnp.int32, (inner, local, CAP), 2)
    places = ((homes_i * parts + part_at) * local + locals_i) * CAP + cap_i

    def table(m, positions, rows=slice(None)):
        index = slot_index[m, rows]
        flat = positions.reshape(1, -1)
        return ((index[:, 0:1] == flat) | (index[:, 1:2] == flat)).astype(low)

    def share(rows):
        if parts == 2:
            return jnp.concatenate([rows, lax.ppermute(rows, "t", [(0, 1), (1, 0)])], 1)
        return lax.all_gather(rows, "t", axis=1, tiled=True)

    def dispatch(shared):
        sent = []
        for m in range(micros):
            slots = mm(table(m, places), shared[m], TN).astype(low)
            slots = lax.all_to_all(slots.reshape(inner, local * CAP, width), "i", 0, 0, tiled=True)
            sent.append(slots.reshape(inner, local, CAP, width))
        return [
            jnp.concatenate([s[:, k].reshape(inner * CAP, width) for s in sent], 0) for k in range(local)]

    cot_slots = dispatch(share(cotangent.astype(low)))

    flags = lax.dynamic_slice_in_dim(key_mask, part_at * images, images, 1).reshape(total, 1, length)
    bias = jnp.where(flags > 0, 0.0, -1e30).astype(jnp.float32)
    tok = tokens.reshape(total, length, width)
    per_step = 2 if total % 2 == 0 else 1
    middle, routed, proj, mixed, gates = attention_forward(tok, bias, mats, norms, router_parts, per_step)

    row_slots = dispatch(share(routed.reshape(micros, own_rows, width)))

    first_out, second_out, results, backs = [], [], [], []
    for k in range(local):
        expert = ((inner_at * parts + part_at) * local + k).astype(jnp.int32).reshape(1)
        result, back, dweights = run_expert(expert, row_slots[k], cot_slots[k], weights[k], router_parts)
        results.append(result.reshape(micros, inner, CAP, width))
        backs.append(back.reshape(micros, inner, CAP, width + LANES))
        dweights = dweights.reshape(planes, homes, 2, depth, extent)
        if planes == 2:
            theirs = lax.dynamic_index_in_dim(dweights, 1 - plane_at, 0, keepdims=False)
            ours = lax.dynamic_index_in_dim(dweights, plane_at, 0, keepdims=False)
            summed = ours.astype(jnp.float32) + lax.ppermute(
                theirs, "o", [(0, 1), (1, 0)]).astype(jnp.float32)
            summed = summed.astype(low)
        else:
            summed = lax.psum_scatter(dweights, "o", scatter_dimension=0, tiled=True)[0]
        final = lax.all_to_all(summed, ("i", "t"), 0, 0, tiled=True)
        first_out.append(final[:, 0])
        second_out.append(final[:, 1])
    first_grad = jnp.stack(first_out, 1).reshape(experts, depth, extent).astype(jnp.float32)
    second_grad = jnp.stack(second_out, 1).reshape(experts, depth, extent).astype(jnp.float32)
    second_grad = second_grad.transpose(0, 2, 1)

    def collect(values):
        size = values[0].shape[-1]
        answers = []
        for m in range(micros):
            back = jnp.stack([v[m] for v in values], 1).reshape(inner, local * CAP, size)
            back = lax.all_to_all(back, "i", 0, 0, tiled=True).reshape(inner * local * CAP, size)
            if parts == 2:
                away = mm(table(m, places, slice(own_rows, None)), back).astype(low)
                here = mm(table(m, places, slice(0, own_rows)), back)
                answers.append(here + lax.ppermute(away, "t", [(0, 1), (1, 0)]).astype(jnp.float32))
            else:
                whole = mm(table(m, places), back).astype(low)
                answers.append(lax.psum_scatter(
                    whole, "t", scatter_dimension=0, tiled=True).astype(jnp.float32))
        return jnp.stack(answers)

    grad = collect(backs)
    combined = collect(results)
    block_out = middle.reshape(micros, own_rows, width) + combined

    input_grad, dmats, dnorms, drouter = attention_backward(
        tok, middle, cotangent.reshape(total, length, width), grad.reshape(total, length, width + LANES),
        gates, proj, mixed, bias, mats, norms, router.T, per_step)
    input_grad = input_grad.reshape(micros, own_rows, width)

    dmats = dmats.reshape(4, planes, inner, depth, parts, columns).transpose(2, 4, 1, 0, 3, 5)
    dmats = dmats.reshape(homes, planes, 4 * depth, columns)
    dloose = jnp.concatenate([dnorms.T, drouter[:, :experts]], 1)
    dloose = dloose.reshape(planes, inner, parts, small * (4 + experts)).transpose(1, 2, 0, 3)
    dloose = jnp.concatenate(three_parts(dloose), -1)
    dloose = jnp.pad(dloose, ((0, 0),) * 3 + ((0, loose_rows * columns - loose_count),))
    dloose = dloose.reshape(homes, planes, loose_rows, columns)
    payload = jnp.concatenate([dmats, dloose], 2)
    payload = lax.all_to_all(payload, ("i", "t"), 0, 0, tiled=True)
    payload = jnp.sum(payload.astype(jnp.float32), 0)
    if planes == 2:
        theirs = lax.dynamic_index_in_dim(payload, 1 - plane_at, 0, keepdims=False)
        ours = lax.dynamic_index_in_dim(payload, plane_at, 0, keepdims=False)
        reduced = ours + lax.ppermute(theirs, "o", [(0, 1), (1, 0)])
    else:
        reduced = lax.psum_scatter(payload, "o", scatter_dimension=0, tiled=True)[0]
    matrices = reduced[:4 * depth].reshape(4, depth, columns)
    qkv_grad = matrices[:3].transpose(1, 0, 2)
    out_grad = matrices[3].T
    tail = reduced[4 * depth:].reshape(-1)[:loose_count].reshape(3, small, 4 + experts)
    tail = (tail[0] + tail[1]) + tail[2]
    return (
        block_out, input_grad, tail[:, 0], tail[:, 1], qkv_grad, out_grad, tail[:, 2], tail[:, 3],
        tail[:, 4:], first_grad, second_grad,
    )


def per_device_halves(tokens, key_mask, expert_ids, slot_ids, norm1_gain, norm1_bias,
                      qkv_weight, out_weight, norm2_gain, norm2_bias, router_weight, expert_in, expert_out,
                      cotangent):
    micros, own_rows, width = tokens.shape
    length = key_mask.shape[2]
    images = own_rows // length
    total = micros * images
    planes, inner, parts = 2, 8, 2
    experts = expert_in.shape[0]
    homes = inner * parts
    local = experts // homes
    depth, extent = expert_in.shape[1:]
    columns = qkv_weight.shape[2]
    plane_at, inner_at, part_at = (lax.axis_index(name) for name in ("o", "i", "t"))
    low = jnp.bfloat16
    across = [(0, 1), (1, 0)]

    norms_in = jnp.stack([norm1_gain, norm1_bias, norm2_gain, norm2_bias], 1)
    loose = [p for p in three_parts(router_weight)]
    loose += [jnp.pad(p, ((0, 0), (0, 4))) for p in three_parts(norms_in)]
    loose = jnp.concatenate(loose, 1)
    loose = jnp.pad(loose, ((0, 0), (0, columns - loose.shape[1])))
    packed = jnp.concatenate([
        qkv_weight.transpose(1, 0, 2).reshape(3 * depth, columns), out_weight.T, loose], 0)
    slot_index = jnp.where(slot_ids >= 0, expert_ids * CAP + slot_ids, -1).transpose(0, 2, 1)
    own_first = part_at * own_rows
    index = jnp.stack([
        lax.dynamic_slice_in_dim(slot_index, own_first, own_rows, 2),
        lax.dynamic_slice_in_dim(slot_index, own_rows - own_first, own_rows, 2)], 2)

    flags = lax.dynamic_slice_in_dim(key_mask, part_at * images, images, 1).reshape(total, 1, length)
    bias = jnp.where(flags > 0, 0.0, -1e30).astype(jnp.float32)
    tok = tokens.reshape(total, length, width)
    table = jnp.pad(index.transpose(0, 2, 3, 1), ((0, 0), (0, 0), (0, 0), (0, LANES - 2)))
    reduced, block_out, input_grad, dweights = opening(
        packed, cotangent.reshape(tok.shape), index, table, tok, bias, expert_in, expert_out.transpose(0, 2, 1), local, 2)[:4]
    dweights = dweights[0].astype(jnp.float32) + dweights[1].astype(jnp.float32)
    first_grad = dweights[:, 0]
    second_grad = dweights[:, 1].transpose(0, 2, 1)
    matrices = reduced[:4 * depth].reshape(4, depth, columns)
    qkv_grad = matrices[:3].transpose(1, 0, 2)
    out_grad = matrices[3].T
    tail = reduced[4 * depth:]
    shape = (micros, own_rows, width)
    return (
        block_out.reshape(shape), input_grad.reshape(shape), tail[:, 96], tail[:, 97], qkv_grad, out_grad,
        tail[:, 98], tail[:, 99], tail[:, :experts], first_grad, second_grad,
    )


def solution(mesh):
    dp, parts = mesh.shape["dp"], mesh.shape["tensor"]
    inner = min(8, 32 // parts, dp)
    planes = dp // inner
    fine = Mesh(mesh.devices.reshape(planes, inner, parts), ("o", "i", "t"))
    dps = ("o", "i")
    every = ("o", "i", "t")
    rows = P(None, every, None)
    step = functools.partial(per_device, planes, inner, parts)
    if (planes, inner, parts) == (2, 8, 2):
        step = per_device_halves
    return jax.shard_map(
        step,
        mesh=fine,
        in_specs=(
            rows, P(None, dps, None), P(None, dps, None), P(None, dps, None), P(every), P(every),
            P(dps, None, "t"), P("t", dps), P(every), P(every), P(every, None),
            P(None, dps, "t"), P(None, "t", dps), rows,
        ),
        out_specs=(
            rows, rows, P(every), P(every), P(dps, None, "t"), P("t", dps), P(every), P(every),
            P(every, None), P(None, dps, "t"), P(None, "t", dps),
        ),
        check_vma=False,
    )
```

```python
import functools

import jax
import jax.numpy as jnp
from jax import lax
from jax.experimental import pallas as pl
from jax.experimental.pallas import tpu as pltpu
from jax.sharding import Mesh, PartitionSpec as P

HEAD = 64
CAP = 120
EPSILON = 1e-06
LANES = 128
VMEM = 60 * 1024 * 1024
NN = (((1,), (0,)), ((), ()))
NT = (((1,), (1,)), ((), ()))
TN = (((0,), (0,)), ((), ()))
HIGH = lax.Precision.HIGHEST
GELU_C = 0.7978845608028654
GELU_A = 0.044715


def mm(a, b, dims=NN, precision=None):
    return lax.dot_general(a, b, dims, precision=precision, preferred_element_type=jnp.float32)


def three_parts(value):
    high = value.astype(jnp.bfloat16)
    rest = value - high.astype(jnp.float32)
    middle = rest.astype(jnp.bfloat16)
    last = (rest - middle.astype(jnp.float32)).astype(jnp.bfloat16)
    return high, middle, last


def standardize(values):
    center = jnp.mean(values, -1, keepdims=True)
    shifted = values - center
    spread = jnp.mean(shifted * shifted, -1, keepdims=True)
    inverse = lax.rsqrt(spread + EPSILON)
    return shifted * inverse, inverse


def norm_back(grad, unit, inverse):
    return inverse * (
        grad
        - jnp.mean(grad, -1, keepdims=True)
        - unit * jnp.mean(grad * unit, -1, keepdims=True)
    )


def even_lanes(shape):
    return lax.broadcasted_iota(jnp.int32, shape, 1) < HEAD


def router_gates(routed, parts):
    logits = mm(routed, parts, NT)
    logits = logits + pltpu.roll(logits, LANES - 32, 1) + pltpu.roll(logits, LANES - 64, 1)
    lane = lax.broadcasted_iota(jnp.int32, logits.shape, 1)
    logits = jnp.where(lane < 32, logits, -1e30)
    lifted = jnp.exp(logits - jnp.max(logits, -1, keepdims=True))
    return lifted / jnp.sum(lifted, -1, keepdims=True)


def forward_rows(first, images, tok_ref, bias_ref, mats_ref, norms_ref, parts_ref,
                 middle_ref, proj_ref, mixed_ref, gates_ref):
    _, length, width = tok_ref.shape
    pieces, _, _, columns = mats_ref.shape
    rows = images * length
    here = pl.ds(first, images)
    tok = tok_ref[here].reshape(rows, width)
    unit, _ = standardize(tok)
    normed = (unit * norms_ref[0:1] + norms_ref[1:2]).astype(jnp.bfloat16)
    for c in range(3):
        for p in range(pieces):
            part = mm(normed, mats_ref[p, c]).reshape(images, length, columns)
            base = c * width + p * columns
            for b in range(images):
                proj_ref[first + b, :, base:base + columns] = part[b].astype(jnp.bfloat16)
    even = even_lanes((length, LANES))
    scale = jnp.bfloat16(HEAD ** -0.5)
    zero = jnp.zeros((), jnp.bfloat16)
    attended = []
    for b in range(images):
        bias = bias_ref[first + b]
        parts = []
        for pair in range(width // LANES):
            lanes = slice(pair * LANES, (pair + 1) * LANES)
            query = proj_ref[first + b, :, lanes] * scale
            keyed = proj_ref[first + b, :, width + pair * LANES:width + (pair + 1) * LANES]
            valued = proj_ref[first + b, :, 2 * width + pair * LANES:2 * width + (pair + 1) * LANES]
            halves = []
            for odd in range(2):
                chosen = jnp.where(even != bool(odd), query, zero)
                scores = mm(chosen, keyed, NT) + bias
                lifted = jnp.exp(scores - jnp.max(scores, -1, keepdims=True))
                probs = lifted * (1.0 / jnp.sum(lifted, -1, keepdims=True))
                halves.append(mm(probs.astype(jnp.bfloat16), valued))
            both = jnp.where(even, halves[0], halves[1])
            mixed_ref[first + b, :, lanes] = both.astype(jnp.bfloat16)
            parts.append(both)
        attended.append(jnp.concatenate(parts, 1))
    joined = jnp.concatenate(attended, 0).astype(jnp.bfloat16)
    middle = tok
    for p in range(pieces):
        middle += mm(joined[:, p * columns:(p + 1) * columns], mats_ref[p, 3], NT)
    middle_ref[here] = middle.reshape(images, length, width)
    unit, _ = standardize(middle)
    routed = unit * norms_ref[2:3] + norms_ref[3:4]
    low = routed.astype(jnp.bfloat16)
    gates_ref[here] = router_gates(low, parts_ref[...]).reshape(images, length, LANES)
    return routed, low


def forward_kernel(
    tok_ref, bias_ref, mats_ref, norms_ref, parts_ref,
    middle_ref, routed_ref, proj_ref, mixed_ref, gates_ref,
):
    images, length, width = tok_ref.shape
    routed, _ = forward_rows(0, images, tok_ref, bias_ref, mats_ref, norms_ref, parts_ref,
                             middle_ref, proj_ref, mixed_ref, gates_ref)
    routed_ref[...] = routed.reshape(images, length, width).astype(jnp.bfloat16)


def attention_forward(tok, bias, mats, norms, router, per_step):
    images, length, width = tok.shape

    def rows(last):
        return pl.BlockSpec((per_step, length, last), lambda s: (s, 0, 0))

    def whole(a):
        return pl.BlockSpec(a.shape, lambda s: (0,) * a.ndim)

    shapes = [
        (width, jnp.float32), (width, jnp.bfloat16), (3 * width, jnp.bfloat16),
        (width, jnp.bfloat16), (LANES, jnp.float32),
    ]
    return pl.pallas_call(
        forward_kernel,
        grid=(images // per_step,),
        in_specs=[
            rows(width), pl.BlockSpec((per_step, 1, length), lambda s: (s, 0, 0)),
            whole(mats), whole(norms), whole(router),
        ],
        out_specs=[rows(n) for n, _ in shapes],
        out_shape=[jax.ShapeDtypeStruct((images, length, n), kind) for n, kind in shapes],
        compiler_params=pltpu.CompilerParams(vmem_limit_bytes=VMEM),
        cost_estimate=pl.CostEstimate(
            flops=images * length * width * width * 10, bytes_accessed=images * length * width * 16,
            transcendentals=images * length * length * 8),
        name="attention_forward",
    )(tok, bias, mats, norms, router)


def backward_rows(first, images, grad, tok_ref, middle_ref, cot_ref, gates_ref, proj_ref, mixed_ref,
                  bias_ref, mats_ref, norms_ref, router_t_ref,
                  input_ref, dnorms_ref, drouter_ref, dproj_ref, dmats_acc):
    _, length, width = tok_ref.shape
    rows = images * length
    here = pl.ds(first, images)

    def flat(ref):
        return ref[here].reshape(rows, ref.shape[2])

    middle = flat(middle_ref)
    unit, inverse = standardize(middle)
    gates = flat(gates_ref)
    gate_cot = grad[:, width:]
    logit_grad = gates * (gate_cot - jnp.sum(gates * gate_cot, -1, keepdims=True))
    routed = (unit * norms_ref[2:3] + norms_ref[3:4]).astype(jnp.bfloat16)
    drouter_ref[...] += mm(routed.astype(jnp.float32), logit_grad, TN, HIGH)
    routed_grad = grad[:, :width] + mm(logit_grad, router_t_ref[...], NN, HIGH)
    dnorms_ref[2:3] += jnp.sum(routed_grad * unit, 0, keepdims=True)
    dnorms_ref[3:4] += jnp.sum(routed_grad, 0, keepdims=True)
    middle_grad = flat(cot_ref) + norm_back(routed_grad * norms_ref[2:3], unit, inverse)
    attn_cot = middle_grad.astype(jnp.bfloat16)
    joined = jnp.concatenate([mixed_ref[first + b].astype(jnp.float32) for b in range(images)], 0)
    joined = joined.astype(jnp.bfloat16)
    pieces, _, _, columns = mats_ref.shape
    spans = [slice(p * columns, (p + 1) * columns) for p in range(pieces)]
    for p in range(pieces):
        dmats_acc[p, 3] += mm(attn_cot, joined[:, spans[p]], TN)
    mixed_grad = jnp.concatenate([mm(attn_cot, mats_ref[p, 3]) for p in range(pieces)], 1)
    mixed_grad = mixed_grad.reshape(images, length, width)
    even = even_lanes((length, LANES))
    zero = jnp.zeros((), jnp.bfloat16)
    scale = jnp.bfloat16(HEAD ** -0.5)
    for b in range(images):
        bias = bias_ref[first + b]
        mixed_low = mixed_grad[b].astype(jnp.bfloat16)
        for pair in range(width // LANES):
            lanes = slice(pair * LANES, (pair + 1) * LANES)
            query = proj_ref[first + b, :, lanes] * scale
            keyed = proj_ref[first + b, :, width + pair * LANES:width + (pair + 1) * LANES]
            valued = proj_ref[first + b, :, 2 * width + pair * LANES:2 * width + (pair + 1) * LANES]
            out_cot = mixed_low[:, lanes]
            query_grad = keyed_grad = value_grad = None
            for odd in range(2):
                mask = even != bool(odd)
                query_half = jnp.where(mask, query, zero)
                keyed_half = jnp.where(mask, keyed, zero)
                cot_half = jnp.where(mask, out_cot, zero)
                scores = mm(query_half, keyed, NT) + bias
                lifted = jnp.exp(scores - jnp.max(scores, -1, keepdims=True))
                probs = lifted * (1.0 / jnp.sum(lifted, -1, keepdims=True))
                prob_grad = mm(cot_half, valued, NT)
                value_part = mm(probs.astype(jnp.bfloat16), cot_half, TN)
                inner = jnp.sum(probs * prob_grad, -1, keepdims=True)
                score_grad = (probs * (prob_grad - inner)).astype(jnp.bfloat16)
                query_part = mm(score_grad, keyed_half)
                keyed_part = mm(score_grad, query_half, TN)
                if odd:
                    query_grad, keyed_grad, value_grad = (
                        query_grad + query_part, keyed_grad + keyed_part, value_grad + value_part)
                else:
                    query_grad, keyed_grad, value_grad = query_part, keyed_part, value_part
            base = pair * LANES
            rows_here = slice(b * length, (b + 1) * length)
            dproj_ref[rows_here, base:base + LANES] = query_grad * (HEAD ** -0.5)
            dproj_ref[rows_here, width + base:width + base + LANES] = keyed_grad
            dproj_ref[rows_here, 2 * width + base:2 * width + base + LANES] = value_grad
    tok = flat(tok_ref)
    unit, inverse = standardize(tok)
    normed = (unit * norms_ref[0:1] + norms_ref[1:2]).astype(jnp.bfloat16)
    normed_grad = jnp.zeros((rows, width), jnp.float32)
    for c in range(3):
        part = dproj_ref[:, c * width:(c + 1) * width].astype(jnp.bfloat16)
        for p in range(pieces):
            dmats_acc[p, c] += mm(normed, part[:, spans[p]], TN)
            normed_grad += mm(part[:, spans[p]], mats_ref[p, c], NT)
    dnorms_ref[0:1] += jnp.sum(normed_grad * unit, 0, keepdims=True)
    dnorms_ref[1:2] += jnp.sum(normed_grad, 0, keepdims=True)
    input_grad = middle_grad + norm_back(normed_grad * norms_ref[0:1], unit, inverse)
    input_ref[here] = input_grad.reshape(images, length, width)


def backward_kernel(
    tok_ref, middle_ref, cot_ref, grad_ref, gates_ref, proj_ref, mixed_ref,
    bias_ref, mats_ref, norms_ref, router_t_ref,
    input_ref, dmats_ref, dnorms_ref, drouter_ref,
    dproj_ref, dmats_acc,
):
    images, length, width = tok_ref.shape
    rows = images * length
    step = pl.program_id(0)

    @pl.when(step == 0)
    def _():
        dmats_acc[...] = jnp.zeros_like(dmats_acc)
        dnorms_ref[...] = jnp.zeros_like(dnorms_ref)
        drouter_ref[...] = jnp.zeros_like(drouter_ref)

    backward_rows(0, images, grad_ref[...].reshape(rows, grad_ref.shape[2]), tok_ref, middle_ref, cot_ref,
                  gates_ref, proj_ref, mixed_ref, bias_ref, mats_ref, norms_ref, router_t_ref,
                  input_ref, dnorms_ref, drouter_ref, dproj_ref, dmats_acc)

    @pl.when(step == pl.num_programs(0) - 1)
    def _():
        dmats_ref[...] = dmats_acc[...].astype(jnp.bfloat16)


def attention_backward(tok, middle, cot, grad, gates, proj, mixed, bias, mats, norms, router_t, per_step):
    images, length, width = tok.shape

    def rows(last):
        return pl.BlockSpec((per_step, length, last), lambda s: (s, 0, 0))

    def whole(shape):
        return pl.BlockSpec(shape, lambda s: (0,) * len(shape))

    return pl.pallas_call(
        backward_kernel,
        grid=(images // per_step,),
        in_specs=[
            rows(width), rows(width), rows(width), rows(width + LANES), rows(LANES),
            rows(3 * width), rows(width), pl.BlockSpec((per_step, 1, length), lambda s: (s, 0, 0)),
            whole(mats.shape), whole(norms.shape), whole(router_t.shape),
        ],
        out_specs=[
            rows(width), whole(mats.shape), whole((4, width)), whole((width, LANES)),
        ],
        out_shape=[
            jax.ShapeDtypeStruct((images, length, width), jnp.float32),
            jax.ShapeDtypeStruct(mats.shape, jnp.bfloat16),
            jax.ShapeDtypeStruct((4, width), jnp.float32),
            jax.ShapeDtypeStruct((width, LANES), jnp.float32),
        ],
        scratch_shapes=[
            pltpu.VMEM((per_step * length, 3 * width), jnp.float32),
            pltpu.VMEM(mats.shape, jnp.float32),
        ],
        compiler_params=pltpu.CompilerParams(vmem_limit_bytes=VMEM),
        cost_estimate=pl.CostEstimate(
            flops=images * length * width * width * 30, bytes_accessed=images * length * width * 30,
            transcendentals=images * length * length * 8),
        name="attention_backward",
    )(tok, middle, cot, grad, gates, proj, mixed, bias, mats, norms, router_t)


def expert_kernel(
    expert_ref, slots_ref, cots_ref, weights_ref, router_ref,
    result_ref, back_ref, dweights_ref,
    rows_t, grads_t, grads, gate_scr, result_acc, back_acc, first_acc, second_acc,
):
    count, width = slots_ref.shape
    tile = weights_ref.shape[-1]
    chunk = rows_t.shape[2]
    step = pl.program_id(0)
    first = weights_ref[:, :, 0, 0].reshape(width, tile)
    second = weights_ref[:, :, 0, 1].reshape(width, tile)

    @pl.when(step == 0)
    def _():
        def prepare(r, carry):
            here = pl.ds(pl.multiple_of(r * chunk, 16), chunk)
            slots = slots_ref[here]
            gates = router_gates(slots, router_ref[...])
            lane = lax.broadcasted_iota(jnp.int32, gates.shape, 1)
            gate = jnp.sum(jnp.where(lane == expert_ref[0], gates, 0.0), -1, keepdims=True)
            gate_scr[here] = jnp.broadcast_to(gate, gates.shape)
            low = (cots_ref[here].astype(jnp.float32) * gate).astype(jnp.bfloat16)
            grads[here] = low
            rows_t[r] = slots.T
            grads_t[r] = low.T
            result_acc[here] = jnp.zeros((chunk, width), jnp.float32)
            back_acc[here] = jnp.zeros((chunk, width), jnp.float32)
            return carry

        lax.fori_loop(0, count // chunk, prepare, 0)

    first_acc[...] = jnp.zeros_like(first_acc)
    second_acc[...] = jnp.zeros_like(second_acc)

    def work(r, carry):
        here = pl.ds(pl.multiple_of(r * chunk, 16), chunk)
        pre = mm(slots_ref[here], first)
        square = pre * pre
        half = 0.5 + 0.5 * jnp.tanh(pre * (GELU_C + (GELU_C * GELU_A) * square))
        hidden = (pre * half).astype(jnp.bfloat16)
        slope = half + 2.0 * half * (1.0 - half) * pre * (GELU_C + (3.0 * GELU_C * GELU_A) * square)
        hidden_grad = mm(grads[here], second)
        pre_grad = (hidden_grad * slope).astype(jnp.bfloat16)
        result_acc[here] += mm(hidden, second, NT)
        back_acc[here] += mm(pre_grad, first, NT)
        first_acc[...] += mm(rows_t[r], pre_grad)
        second_acc[...] += mm(grads_t[r], hidden)
        return carry

    lax.fori_loop(0, count // chunk, work, 0)
    block = weights_ref.shape[:2] + weights_ref.shape[4:]
    dweights_ref[:, :, 0, 0] = first_acc[...].astype(jnp.bfloat16).reshape(block)
    dweights_ref[:, :, 0, 1] = second_acc[...].astype(jnp.bfloat16).reshape(block)

    @pl.when(step == pl.num_programs(0) - 1)
    def _():
        def finish(r, carry):
            here = pl.ds(pl.multiple_of(r * chunk, 16), chunk)
            result = result_acc[here]
            gate = gate_scr[here][:, 0:1]
            result_ref[here] = (result * gate).astype(jnp.bfloat16)
            gate_grad = jnp.sum(cots_ref[here].astype(jnp.float32) * result, -1, keepdims=True)
            lane = lax.broadcasted_iota(jnp.int32, (chunk, LANES), 1)
            back_ref[here, 0:width] = back_acc[here].astype(jnp.bfloat16)
            back_ref[here, width:width + LANES] = jnp.where(
                lane == expert_ref[0], gate_grad, 0.0).astype(jnp.bfloat16)
            return carry

        lax.fori_loop(0, count // chunk, finish, 0)


def run_expert(expert, slots, cots, weights, router):
    count, width = slots.shape
    planes, inner, parts, _, depth, extent = weights.shape
    tile = min(512, extent)
    per_part = extent // tile
    chunk = 480

    def whole(shape):
        return pl.BlockSpec(shape, lambda s, e: (0,) * len(shape))

    weight_spec = pl.BlockSpec(
        (planes, inner, 1, 2, depth, tile), lambda s, e: (0, 0, s // per_part, 0, 0, s % per_part))
    return pl.pallas_call(
        expert_kernel,
        grid_spec=pltpu.PrefetchScalarGridSpec(
            num_scalar_prefetch=1,
            grid=(parts * per_part,),
            in_specs=[whole(slots.shape), whole(cots.shape), weight_spec, whole(router.shape)],
            out_specs=[whole((count, width)), whole((count, width + LANES)), weight_spec],
            scratch_shapes=[
                pltpu.VMEM((count // chunk, width, chunk), jnp.bfloat16),
                pltpu.VMEM((count // chunk, width, chunk), jnp.bfloat16),
                pltpu.VMEM((count, width), jnp.bfloat16),
                pltpu.VMEM((count, LANES), jnp.float32),
                pltpu.VMEM((count, width), jnp.float32),
                pltpu.VMEM((count, width), jnp.float32),
                pltpu.VMEM((width, tile), jnp.float32),
                pltpu.VMEM((width, tile), jnp.float32),
            ],
        ),
        out_shape=[
            jax.ShapeDtypeStruct((count, width), jnp.bfloat16),
            jax.ShapeDtypeStruct((count, width + LANES), jnp.bfloat16),
            jax.ShapeDtypeStruct(weights.shape, jnp.bfloat16),
        ],
        compiler_params=pltpu.CompilerParams(vmem_limit_bytes=VMEM),
        cost_estimate=pl.CostEstimate(
            flops=12 * count * width * extent * parts,
            bytes_accessed=4 * 2 * width * extent * parts + count * width * 8,
            transcendentals=count * extent * parts),
        name="expert",
    )(expert, slots, cots, weights, router)


def flipped(position, bit):
    return position + bit - 2 * bit * lax.rem(position // bit, 2)


def to_peer(source, target, sends, receives, where):
    return pltpu.make_async_remote_copy(
        src_ref=source, dst_ref=target, send_sem=sends, recv_sem=receives, device_id=where,
        device_id_type=pl.DeviceIdType.MESH)


class Dispatch:
    def __init__(self, index_ref, shared, staged, out, sends, receives, keep, inner, parts, local):
        self.index_ref, self.shared, self.staged, self.out = index_ref, shared, staged, out
        self.sends, self.receives, self.keep = sends, receives, keep
        self.inner, self.parts, self.local = inner, parts, local
        self.at_i, self.at_t = lax.axis_index("i"), lax.axis_index("t")

    def copy(self, m, d, k):
        home = lax.rem(self.at_i + d, self.inner)
        target = self.out.at[k, pl.ds(pl.multiple_of((m * self.inner + self.at_i) * CAP, 8), CAP)]
        return to_peer(self.staged.at[m, d, k], target, self.sends.at[m, d, k],
                       self.receives.at[m, d, k], {"i": home})

    def kept(self, m, k):
        target = self.out.at[k, pl.ds(pl.multiple_of((m * self.inner + self.at_i) * CAP, 8), CAP)]
        return pltpu.make_async_copy(self.staged.at[m, 0, k], target, self.keep.at[m, k])

    def fill(self, m, d):
        home = lax.rem(self.at_i + d, self.inner)
        count = self.local * CAP
        base = (home * self.parts + self.at_t) * count
        places = base + lax.broadcasted_iota(jnp.int32, (count, 1), 0)
        total = None
        for half in range(2):
            first = self.index_ref[m, 0, half:half + 1]
            second = self.index_ref[m, 1, half:half + 1]
            hits = jnp.where((first == places) | (second == places), 1.0, 0.0).astype(jnp.bfloat16)
            part = mm(hits, self.shared[m, half])
            total = part if total is None else total + part
        for k in range(self.local):
            self.staged[m, d, k] = total[k * CAP:(k + 1) * CAP].astype(jnp.bfloat16)

    def send(self, m, beside=None):
        def step(d, carry):
            self.fill(m, d)
            for k in range(self.local):
                self.copy(m, d, k).start()
            if beside is not None:
                beside(d)
            return carry

        lax.fori_loop(1, self.inner, step, 0)
        self.fill(m, 0)
        for k in range(self.local):
            self.kept(m, k).start()

    def finish(self, m):
        def step(d, carry):
            for k in range(self.local):
                self.copy(m, d, k).wait()
            return carry

        lax.fori_loop(1, self.inner, step, 0)
        for k in range(self.local):
            self.kept(m, k).wait()


def flipped_if(position, bit, on):
    return position + on * (bit - 2 * bit * lax.rem(position // bit, 2))


class Answer:
    def __init__(self, staged, out, sends, receives, keep, inner):
        self.staged, self.out, self.sends, self.receives, self.keep = staged, out, sends, receives, keep
        self.inner = inner
        self.at_i = lax.axis_index("i")

    def target(self, k, m):
        return self.out.at[k, m, pl.ds(pl.multiple_of(self.at_i * CAP, 8), CAP)]

    def copy(self, k, m, d):
        group = lax.rem(self.at_i + d, self.inner)
        return to_peer(self.staged.at[m, group, k], self.target(k, m), self.sends.at[k, m, d],
                       self.receives.at[k, m, d], {"i": group})

    def kept(self, k, m):
        return pltpu.make_async_copy(self.staged.at[m, self.at_i, k], self.target(k, m), self.keep.at[k, m])

    def send(self, k, m, beside=None):
        def step(d, carry):
            self.copy(k, m, d).start()
            if beside is not None:
                beside(d)
            return carry

        lax.fori_loop(1, self.inner, step, 0)
        self.kept(k, m).start()

    def finish(self, k, m):
        def step(d, carry):
            self.copy(k, m, d).wait()
            return carry

        lax.fori_loop(1, self.inner, step, 0)
        self.kept(k, m).wait()


def device_at(n, origin):
    o, i, t = origin
    return lax.rem(o + n // 16, 2), lax.rem(i + lax.rem(n // 2, 8), 8), lax.rem(t + lax.rem(n, 2), 2)


class Weights:
    def __init__(self, local, sources, target, sends, receives, keep):
        self.local, self.sources, self.target = local, sources, target
        self.sends, self.receives, self.keep = sends, receives, keep
        self.origin = tuple(lax.axis_index(name) for name in ("o", "i", "t"))

    def place(self, k, part):
        o, i, t = self.origin
        return self.target.at[k, o, i, t, part]

    def copy(self, k, n, part):
        o, i, t = device_at(n, self.origin)
        expert = (i * 2 + t) * self.local + k
        return to_peer(self.sources[part].at[expert], self.place(k, part), self.sends.at[k, n, part],
                       self.receives.at[k, n, part], {"o": o, "i": i, "t": t})

    def kept(self, k, part):
        _, i, t = self.origin
        expert = (i * 2 + t) * self.local + k
        return pltpu.make_async_copy(
            self.sources[part].at[expert], self.place(k, part), self.keep.at[k, part])

    def give(self, k, n):
        for part in range(2):
            self.copy(k, n, part).start()

    def give_all(self, k, first, last):
        def step(n, carry):
            self.give(k, n)
            return carry

        lax.fori_loop(first, last, step, 0)

    def keep_own(self, k):
        for part in range(2):
            self.kept(k, part).start()

    def finish(self, k):
        def step(n, carry):
            for part in range(2):
                self.copy(k, n, part).wait()
            return carry

        lax.fori_loop(1, 32, step, 0)
        for part in range(2):
            self.kept(k, part).wait()


class Gradients:
    def __init__(self, local, source, target, sends, receives, keep):
        self.local, self.source, self.target = local, source, target
        self.sends, self.receives, self.keep = sends, receives, keep
        self.origin = tuple(lax.axis_index(name) for name in ("o", "i", "t"))

    def place(self, k, part):
        o, i, t = self.origin
        return self.target.at[o, (i * 2 + t) * self.local + k, part]

    def copy(self, k, n, part):
        o, i, t = device_at(n, self.origin)
        return to_peer(self.source.at[k, o, i, t, part], self.place(k, part), self.sends.at[k, n, part],
                       self.receives.at[k, n, part], {"o": o, "i": i, "t": t})

    def kept(self, k, part):
        o, i, t = self.origin
        return pltpu.make_async_copy(
            self.source.at[k, o, i, t, part], self.place(k, part), self.keep.at[k, part])

    give = Weights.give
    give_all = Weights.give_all
    keep_own = Weights.keep_own
    finish = Weights.finish


def expert_scratch(count, width, tile, chunk):
    steps = count // chunk
    return [
        pltpu.VMEM((count, width), jnp.bfloat16), pltpu.VMEM((count, width), jnp.bfloat16),
        pltpu.VMEM((steps, width, chunk), jnp.bfloat16), pltpu.VMEM((steps, width, chunk), jnp.bfloat16),
        pltpu.VMEM((count, width), jnp.bfloat16), pltpu.VMEM((count, LANES), jnp.float32),
        pltpu.VMEM((count, width), jnp.float32), pltpu.VMEM((count, width), jnp.float32),
        pltpu.VMEM((2, width, tile), jnp.float32), pltpu.VMEM((2, width, tile), jnp.bfloat16),
        pltpu.SemaphoreType.DMA((2,)),
    ]


def expert_phase(k, expert, slots_hbm, cots_hbm, held, parts_ref, answers, gradients, scratch):
    slots, cots, rows_t, grads_t, grads, gate_scr, result_acc, back_acc, sums, tiles, load = scratch
    count, width = slots.shape
    chunk = rows_t.shape[2]
    tile = tiles.shape[2]
    micros, groups = answers[0].staged.shape[:2]
    loads = [pltpu.make_async_copy(slots_hbm.at[k], slots, load.at[0]),
             pltpu.make_async_copy(cots_hbm.at[k], cots, load.at[1])]
    for copy in loads:
        copy.start()
    for copy in loads:
        copy.wait()

    def prepare(r, carry):
        here = pl.ds(pl.multiple_of(r * chunk, 16), chunk)
        rows = slots[here]
        gates = router_gates(rows, parts_ref[...])
        lane = lax.broadcasted_iota(jnp.int32, gates.shape, 1)
        gate = jnp.sum(jnp.where(lane == expert, gates, 0.0), -1, keepdims=True)
        gate_scr[here] = jnp.broadcast_to(gate, gates.shape)
        low = (cots[here].astype(jnp.float32) * gate).astype(jnp.bfloat16)
        grads[here] = low
        rows_t[r] = rows.T
        grads_t[r] = low.T
        result_acc[here] = jnp.zeros((chunk, width), jnp.float32)
        back_acc[here] = jnp.zeros((chunk, width), jnp.float32)
        return carry

    lax.fori_loop(0, count // chunk, prepare, 0)
    per_part = held.shape[6] // tile

    def one_tile(n, carry):
        t = n // per_part
        span = pl.ds(pl.multiple_of(lax.rem(n, per_part) * tile, tile), tile)
        for part in range(2):
            tiles[part] = held[k, :, :, t, part, :, span].reshape(width, tile)
        sums[...] = jnp.zeros_like(sums)

        def work(r, inside):
            here = pl.ds(pl.multiple_of(r * chunk, 16), chunk)
            pre = mm(slots[here], tiles[0])
            square = pre * pre
            half = 0.5 + 0.5 * jnp.tanh(pre * (GELU_C + (GELU_C * GELU_A) * square))
            hidden = (pre * half).astype(jnp.bfloat16)
            slope = half + 2.0 * half * (1.0 - half) * pre * (
                GELU_C + (3.0 * GELU_C * GELU_A) * square)
            pre_grad = (mm(grads[here], tiles[1]) * slope).astype(jnp.bfloat16)
            result_acc[here] += mm(hidden, tiles[1], NT)
            back_acc[here] += mm(pre_grad, tiles[0], NT)
            sums[0] += mm(rows_t[r], pre_grad)
            sums[1] += mm(grads_t[r], hidden)
            return inside

        lax.fori_loop(0, count // chunk, work, 0)
        block = held.shape[1:3] + (held.shape[5], tile)
        for part in range(2):
            held[k, :, :, t, part, :, span] = sums[part].astype(jnp.bfloat16).reshape(block)
        return carry

    lax.fori_loop(0, held.shape[3] * per_part, one_tile, 0)
    per_chunk = chunk // CAP
    back, result = answers

    def finish(n, carry):
        here = pl.ds(pl.multiple_of(n * chunk, 16), chunk)
        m, r = n // (groups // per_chunk), lax.rem(n, groups // per_chunk)
        value = result_acc[here]
        gate_grad = jnp.sum(cots[here].astype(jnp.float32) * value, -1, keepdims=True)
        lane = lax.broadcasted_iota(jnp.int32, (chunk, LANES), 1)
        spread = jnp.where(lane == expert, gate_grad, 0.0)
        value = value * gate_scr[here][:, 0:1]
        grad = back_acc[here]
        for q in range(per_chunk):
            rows = slice(q * CAP, (q + 1) * CAP)
            at = r * per_chunk + q
            result.staged[m, at, k] = value[rows].astype(jnp.bfloat16)
            back.staged[m, at, k, :, 0:width] = grad[rows].astype(jnp.bfloat16)
            back.staged[m, at, k, :, width:width + LANES] = spread[rows].astype(jnp.bfloat16)
        return carry

    lax.fori_loop(0, micros * groups // per_chunk, finish, 0)

    def one_more(d):
        @pl.when(k == 0)
        def _():
            gradients.give(0, 15 + d)

    for m in range(micros):
        back.send(k, m, one_more if m == 0 else None)

    @pl.when(k == 0)
    def _():
        gradients.give_all(0, 23, 26)


def opening_kernel(
    local, per_step, pack_ref, cot_ref, index_ref, table_ref, tok_ref, bias_ref, first_ref, second_ref,
    small_ref, block_out, input_out, dweights_ref, middle_out, proj_out, mixed_out, gates_out,
    slots_ref, cots_ref, back_ref, result_ref,
    gathered, partial, loose, mats_ref, norms_ref, parts_ref, router_ref, shared_c, shared_r, away_g,
    staged_c, staged_r, held, staged_back,
    load, ring_send, ring_recv, pair_send, pair_recv, pair_send_r, pair_recv_r,
    cot_send, cot_recv, cot_keep, row_send, row_recv, row_keep,
    weight_send, weight_recv, weight_keep, grad_send, grad_recv, grad_keep,
    back_send, back_recv, back_keep, result_send, result_recv, result_keep, store,
    away_send, away_recv, fold_send, fold_recv, fetch,
):
    at_o, at_i, at_t = (lax.axis_index(name) for name in ("o", "i", "t"))
    micros, _, own_rows, width = shared_c.shape
    images, length, _ = tok_ref.shape
    kinds, columns = mats_ref.shape[1], mats_ref.shape[3]
    depth = width // 16
    rows = per_step * length
    steps = own_rows // rows
    stages = [
        {"t": 1 - at_t}, {"o": 1 - at_o}, {"i": flipped(at_i, 4)}, {"i": flipped(at_i, 2)},
        {"i": flipped(at_i, 1)},
    ]
    cot_plan = Dispatch(index_ref, shared_c, staged_c, cots_ref, cot_send, cot_recv, cot_keep, 8, 2, local)
    row_plan = Dispatch(index_ref, shared_r, staged_r, slots_ref, row_send, row_recv, row_keep, 8, 2, local)
    weights = Weights(local, (first_ref, second_ref), held, weight_send, weight_recv, weight_keep)
    gradients = Gradients(local, held, dweights_ref, grad_send, grad_recv, grad_keep)

    def stage(j):
        size = 2 ** j
        return to_peer(gathered.at[pl.ds(0, size)], gathered.at[pl.ds(size, size)],
                       ring_send.at[j], ring_recv.at[j], stages[j])

    def swap_c(m):
        return to_peer(shared_c.at[m, 0], shared_c.at[m, 1], pair_send.at[m], pair_recv.at[m],
                       {"t": 1 - at_t})

    def swap_r(m, s):
        here = pl.ds(pl.multiple_of(s * rows, 16), rows)
        return to_peer(shared_r.at[m, 0, here], shared_r.at[m, 1, here], pair_send_r.at[m, s],
                       pair_recv_r.at[m, s], {"t": 1 - at_t})

    def relative(r):
        o = flipped_if(at_o, 1, lax.rem(r // 2, 2))
        i = flipped_if(at_i, 4, lax.rem(r // 4, 2))
        i = flipped_if(i, 2, lax.rem(r // 8, 2))
        i = flipped_if(i, 1, lax.rem(r // 16, 2))
        return o, i, flipped_if(at_t, 1, lax.rem(r, 2))

    def opening(tok, cot, proj, mixed, gates):
        fill = pltpu.make_async_copy(pack_ref, gathered.at[0], load.at[0])
        take_cot = pltpu.make_async_copy(cot_ref, cot, load.at[1])
        take_tok = pltpu.make_async_copy(tok_ref, tok, load.at[2])
        fill.start()
        take_cot.start()
        take_tok.start()
        fill.wait()
        stage(0).start()
        take_cot.wait()
        shared_c[0, 0] = cot[0:images // 2].reshape(own_rows, width).astype(jnp.bfloat16)
        swap_c(0).start()
        stage(0).wait()
        stage(1).start()
        shared_c[1, 0] = cot[images // 2:].reshape(own_rows, width).astype(jnp.bfloat16)
        swap_c(1).start()
        stage(1).wait()
        stage(2).start()
        stage(2).wait()
        stage(3).start()
        weights.give_all(0, 30, 32)
        swap_c(0).wait()
        cot_plan.send(0, lambda d: weights.give(0, d + 15))
        stage(3).wait()
        stage(4).start()
        swap_c(1).wait()
        cot_plan.send(1, lambda d: weights.give(0, d + 22))
        weights.give_all(0, 1, 16)
        weights.keep_own(0)
        stage(4).wait()

        def place(r, carry):
            o, i, t = relative(r)
            row = pl.multiple_of((o * 8 + i) * depth, depth)
            for c in range(kinds):
                mats_ref[t, c, pl.ds(row, depth)] = gathered[r, c * depth:(c + 1) * depth]
            loose[(o * 8 + i) * 2 + t] = gathered[r, kinds * depth:, 0:LANES].astype(jnp.float32)
            return carry

        lax.fori_loop(0, gathered.shape[0], place, 0)
        turned = loose[...].reshape(width, LANES).T
        norms_ref[...] = turned[96:104] + turned[104:112] + turned[112:120]
        low = turned[0:96].astype(jnp.bfloat16)
        parts_ref[...] = jnp.concatenate([low, jnp.zeros((32, width), jnp.bfloat16)], 0)
        router_ref[0:32] = turned[0:32] + turned[32:64] + turned[64:96]
        router_ref[32:] = jnp.zeros((96, width), jnp.float32)
        take_tok.wait()

        def attend(n, carry):
            m, s = n // steps, lax.rem(n, steps)
            _, routed = forward_rows(n * per_step, per_step, tok, bias_ref, mats_ref, norms_ref, parts_ref,
                                     tok, proj, mixed, gates)
            shared_r[m, 0, pl.ds(pl.multiple_of(s * rows, 16), rows)] = routed
            swap_r(m, s).start()
            return carry

        lax.fori_loop(0, micros * steps, attend, 0)
        outs = [(tok, middle_out), (proj, proj_out), (mixed, mixed_out), (gates, gates_out)]
        stores = [pltpu.make_async_copy(a, b, store.at[n]) for n, (a, b) in enumerate(outs)]
        for copy in stores:
            copy.start()
        for m in range(micros):
            for s in range(steps):
                swap_r(m, s).wait()
            row_plan.send(m, (lambda d: weights.give(1, d + 15)) if m == 0 else None)
        weights.give_all(1, 23, 32)
        weights.give_all(1, 1, 16)
        weights.keep_own(1)
        for copy in stores:
            copy.wait()

    pl.run_scoped(
        opening,
        pltpu.VMEM(tok_ref.shape, jnp.float32),
        pltpu.VMEM(cot_ref.shape, jnp.float32),
        pltpu.VMEM((images, length, 3 * width), jnp.bfloat16),
        pltpu.VMEM((images, length, width), jnp.bfloat16),
        pltpu.VMEM((images, length, LANES), jnp.float32),
    )
    for m in range(micros):
        row_plan.finish(m)
        cot_plan.finish(m)
    back = Answer(staged_back, back_ref, back_send, back_recv, back_keep, 8)
    result = Answer(staged_c, result_ref, result_send, result_recv, result_keep, 8)
    count = slots_ref.shape[1]

    def experts(*scratch):
        def one(k, carry):
            weights.finish(k)
            expert = (at_i * 2 + at_t) * local + k
            expert_phase(k, expert, slots_ref, cots_ref, held, parts_ref, (back, result), gradients, scratch)
            return carry

        lax.fori_loop(0, local, one, 0)

    pl.run_scoped(experts, *expert_scratch(count, width, 512, 480))

    gradients.give_all(0, 26, 32)
    result.send(0, 0, lambda d: gradients.give(1, 15 + d))
    result.send(0, 1, lambda d: gradients.give(1, 22 + d))
    gradients.give_all(1, 30, 32)
    for m in range(micros):
        result.send(1, m)

    def rest(k, carry):
        gradients.give_all(k, 1, 16)
        gradients.keep_own(k)
        return carry

    lax.fori_loop(0, local, rest, 0)

    places = lax.broadcasted_iota(jnp.int32, (1, 8 * CAP), 1)
    block = sum((places >= q * CAP).astype(jnp.int32) for q in range(1, 8))
    places = places + block * (3 * CAP) + at_t * (2 * CAP)

    def taken(table, m, half, here, values):
        first, second = table[m, half, here, 0:1], table[m, half, here, 1:2]
        total = None
        for k in range(local):
            where = places + k * CAP
            hits = jnp.where((first == where) | (second == where), 1.0, 0.0).astype(jnp.bfloat16)
            part = mm(hits, values[k])
            total = part if total is None else total + part
        return total

    across = {"t": 1 - at_t}

    def away(m, s, which):
        here = pl.ds(pl.multiple_of(s * rows, 16), rows)
        buffer = (shared_r, away_g, shared_c)[which]
        return to_peer(buffer.at[m, 0, here], buffer.at[m, 1, here], away_send.at[which, m, s],
                       away_recv.at[which, m, s], across)

    def collect(own):
        def fetched(table, backs):
            take = pltpu.make_async_copy(table_ref, table, fetch.at[2])
            take.start()
            take.wait()
            for m in range(micros):
                for k in range(local):
                    back.finish(k, m)
                    pltpu.make_async_copy(back_ref.at[k, m], backs.at[k], fetch.at[k]).start()
                for k in range(local):
                    pltpu.make_async_copy(back_ref.at[k, m], backs.at[k], fetch.at[k]).wait()

                def leave(s, carry):
                    here = pl.ds(pl.multiple_of(s * rows, 16), rows)
                    total = taken(table, m, 1, here, backs).astype(jnp.bfloat16)
                    shared_r[m, 0, here] = total[:, :width]
                    away_g[m, 0, here] = total[:, width:]
                    away(m, s, 0).start()
                    away(m, s, 1).start()
                    return carry

                lax.fori_loop(0, steps, leave, 0)

                def stay(s, carry):
                    here = pl.ds(pl.multiple_of(s * rows, 16), rows)
                    own[m * steps + s] = taken(table, m, 0, here, backs)
                    return carry

                lax.fori_loop(0, steps, stay, 0)

        pl.run_scoped(
            fetched, pltpu.VMEM(table_ref.shape, jnp.int32), pltpu.VMEM((local, 8 * CAP, width + LANES), jnp.bfloat16))

        def backward(tok, middle, cot, proj, mixed, gates, dproj, dmats, dnorms, drouter):
            dmats[...] = jnp.zeros_like(dmats)
            dnorms[...] = jnp.zeros_like(dnorms)
            drouter[...] = jnp.zeros_like(drouter)
            pairs = [(tok_ref, tok), (middle_out, middle), (cot_ref, cot), (proj_out, proj),
                     (mixed_out, mixed), (gates_out, gates)]

            def micro(m, carry):
                ours = pl.ds(m * (images // micros), images // micros)
                takes = [pltpu.make_async_copy(a.at[ours], b, fetch.at[n]) for n, (a, b) in enumerate(pairs)]
                for copy in takes:
                    copy.start()
                for copy in takes:
                    copy.wait()

                def attend(s, inside):
                    away(m, s, 0).wait()
                    away(m, s, 1).wait()
                    here = pl.ds(pl.multiple_of(s * rows, 16), rows)
                    grad = own[m * steps + s] + jnp.concatenate([
                        shared_r[m, 1, here].astype(jnp.float32), away_g[m, 1, here].astype(jnp.float32)], 1)
                    backward_rows(s * per_step, per_step, grad, tok, middle, cot, gates, proj, mixed,
                                  bias_ref.at[ours], mats_ref, norms_ref, router_ref, cot, dnorms, drouter,
                                  dproj, dmats)
                    return inside

                lax.fori_loop(0, steps, attend, 0)
                keep = pltpu.make_async_copy(cot, input_out.at[ours], store.at[0])
                keep.start()
                keep.wait()
                return carry

            lax.fori_loop(0, micros, micro, 0)
            tail = jnp.concatenate(
                [jnp.zeros((96, width), jnp.float32), dnorms[...], jnp.zeros((24, width), jnp.float32)], 0)
            drouter[...] += tail.T

            def spread(r, carry):
                o, i, t = relative(r)
                row = pl.multiple_of((o * 8 + i) * depth, depth)
                for c in range(kinds):
                    gathered[r, c * depth:(c + 1) * depth] = dmats[t, c, pl.ds(row, depth)].astype(jnp.bfloat16)
                row = pl.multiple_of(((o * 8 + i) * 2 + t) * 16, 16)
                gathered[r, kinds * depth:, 0:LANES] = drouter[pl.ds(row, 16)].astype(jnp.bfloat16)
                gathered[r, kinds * depth:, LANES:] = jnp.zeros((16, columns - LANES), jnp.bfloat16)
                return carry

            lax.fori_loop(0, gathered.shape[0], spread, 0)

        some = images // micros
        pl.run_scoped(
            backward,
            pltpu.VMEM((some, length, width), jnp.float32),
            pltpu.VMEM((some, length, width), jnp.float32),
            pltpu.VMEM((some, length, width), jnp.float32),
            pltpu.VMEM((some, length, 3 * width), jnp.bfloat16),
            pltpu.VMEM((some, length, width), jnp.bfloat16),
            pltpu.VMEM((some, length, LANES), jnp.float32),
            pltpu.VMEM((rows, 3 * width), jnp.float32),
            pltpu.VMEM(mats_ref.shape, jnp.float32),
            pltpu.VMEM((8, width), jnp.float32),
            pltpu.VMEM((width, LANES), jnp.float32),
        )

    pl.run_scoped(collect, pltpu.VMEM((micros * steps, rows, width + LANES), jnp.float32))

    def fold(j):
        size = 2 ** j
        return to_peer(gathered.at[pl.ds(size, size)], partial.at[pl.ds(size, size)],
                       fold_send.at[j], fold_recv.at[j], stages[j])

    def folded(j):
        fold(j).wait()
        size = 2 ** j

        def add(r, carry):
            gathered[r] = (gathered[r].astype(jnp.float32) + partial[size + r].astype(jnp.float32)).astype(
                jnp.bfloat16)
            return carry

        lax.fori_loop(0, size, add, 0)

    def outputs(table, middle, results):
        fold(4).start()
        index_take = pltpu.make_async_copy(table_ref, table, fetch.at[3])
        index_take.start()
        take = pltpu.make_async_copy(middle_out, middle, fetch.at[2])
        take.start()
        def load(m, k):
            return pltpu.make_async_copy(result_ref.at[k, m], results.at[m, k], fetch.at[4 + k])

        folded(4)
        fold(3).start()
        index_take.wait()
        for m in range(micros):
            for k in range(local):
                result.finish(k, m)
                load(m, k).start()
            for k in range(local):
                load(m, k).wait()

            def leave(s, carry):
                here = pl.ds(pl.multiple_of(s * rows, 16), rows)
                shared_c[m, 0, here] = taken(table, m, 1, here, results.at[m]).astype(jnp.bfloat16)
                away(m, s, 2).start()
                return carry

            lax.fori_loop(0, steps, leave, 0)
        folded(3)
        fold(2).start()
        take.wait()
        for m in range(micros):
            def stay(s, carry):
                n = m * steps + s
                here = pl.ds(pl.multiple_of(s * rows, 16), rows)
                away(m, s, 2).wait()
                total = taken(table, m, 0, here, results.at[m]) + shared_c[m, 1, here].astype(jnp.float32)
                images_here = pl.ds(n * per_step, per_step)
                middle[images_here] = middle[images_here] + total.reshape(per_step, length, width)
                return carry

            lax.fori_loop(0, steps, stay, 0)
            if m == 0:
                folded(2)
                fold(1).start()
        keep = pltpu.make_async_copy(middle, block_out, store.at[0])
        keep.start()
        folded(1)
        fold(0).start()
        fold(0).wait()
        small_ref[...] = gathered[0].astype(jnp.float32) + partial[1].astype(jnp.float32)
        keep.wait()

    pl.run_scoped(
        outputs, pltpu.VMEM(table_ref.shape, jnp.int32), pltpu.VMEM(tok_ref.shape, jnp.float32),
        pltpu.VMEM((micros, local, 8 * CAP, width), jnp.bfloat16))

    def close(k, carry):
        gradients.finish(k)
        return carry

    lax.fori_loop(0, local, close, 0)


def opening(pack, cot, index, table, tok, bias, first_in, second_in, local, per_step):
    micros, own_rows = index.shape[0], index.shape[3]
    images, length, width = tok.shape
    columns = pack.shape[1]
    experts, depth, extent = first_in.shape
    steps = own_rows // (per_step * length)
    slots = micros * 8 * CAP
    anywhere = pl.BlockSpec(memory_space=pl.ANY)
    vector = pl.BlockSpec(memory_space=pltpu.VMEM)
    dma = pltpu.SemaphoreType.DMA
    low, wide = jnp.bfloat16, jnp.float32
    weights = (local, 2, 8, 2, 2, depth, extent)
    shape = jax.ShapeDtypeStruct
    return pl.pallas_call(
        functools.partial(opening_kernel, local, per_step),
        in_specs=[anywhere, anywhere, vector, anywhere, anywhere, vector, anywhere, anywhere],
        out_specs=[vector] + [anywhere] * 11,
        out_shape=[
            shape(pack.shape, wide), shape(tok.shape, wide), shape(tok.shape, wide),
            shape((2, experts, 2, depth, extent), low),
            shape((images, length, width), wide), shape((images, length, 3 * width), low),
            shape((images, length, width), low), shape((images, length, LANES), wide),
            shape((local, slots, width), low), shape((local, slots, width), low),
            shape((local, micros, 8 * CAP, width + LANES), low), shape((local, micros, 8 * CAP, width), low),
        ],
        scratch_shapes=[
            pltpu.VMEM((32,) + pack.shape, low),
            pltpu.VMEM((32,) + pack.shape, low),
            pltpu.VMEM((32, width // 32, LANES), wide),
            pltpu.VMEM((2, 4, width, columns), low), pltpu.VMEM((8, width), wide),
            pltpu.VMEM((LANES, width), low), pltpu.VMEM((LANES, width), wide),
            pltpu.VMEM((micros, 2, own_rows, width), low),
            pltpu.VMEM((micros, 2, own_rows, width), low),
            pltpu.VMEM((micros, 2, own_rows, LANES), low),
            pltpu.VMEM((micros, 8, local, CAP, width), low),
            pltpu.VMEM((micros, 8, local, CAP, width), low),
            pltpu.VMEM(weights, low),
            pltpu.VMEM((micros, 8, local, CAP, width + LANES), low),
            dma((3,)), dma((5,)), dma((5,)), dma((micros,)), dma((micros,)),
            dma((micros, steps)), dma((micros, steps)),
            dma((micros, 8, local)), dma((micros, 8, local)), dma((micros, local)),
            dma((micros, 8, local)), dma((micros, 8, local)), dma((micros, local)),
            dma((local, 32, 2)), dma((local, 32, 2)), dma((local, 2)),
            dma((local, 32, 2)), dma((local, 32, 2)), dma((local, 2)),
            dma((local, micros, 8)), dma((local, micros, 8)), dma((local, micros)),
            dma((local, micros, 8)), dma((local, micros, 8)), dma((local, micros)), dma((4,)),
            dma((3, micros, steps)), dma((3, micros, steps)), dma((5,)), dma((5,)), dma((6,)),
        ],
        compiler_params=pltpu.CompilerParams(vmem_limit_bytes=67043328, has_side_effects=True),
        cost_estimate=pl.CostEstimate(flops=1000, bytes_accessed=1000, transcendentals=0),
        name="opening",
    )(pack, cot, index, table, tok, bias, first_in, second_in)


def per_device(planes, inner, parts, tokens, key_mask, expert_ids, slot_ids, norm1_gain, norm1_bias,
               qkv_weight, out_weight, norm2_gain, norm2_bias, router_weight, expert_in, expert_out,
               cotangent):
    micros, own_rows, width = tokens.shape
    length = key_mask.shape[2]
    group_rows = own_rows * parts
    images = own_rows // length
    total = micros * images
    experts = expert_in.shape[0]
    homes = inner * parts
    local = experts // homes
    depth, extent = expert_in.shape[1:]
    small = norm1_gain.shape[0]
    every = ("o", "i", "t")
    plane_at, inner_at, part_at = (lax.axis_index(name) for name in every)
    low = jnp.bfloat16

    loose = jnp.concatenate([
        jnp.stack([norm1_gain, norm1_bias, norm2_gain, norm2_bias], 1), router_weight], 1)
    loose_count = 3 * loose.size
    columns = qkv_weight.shape[2]
    loose_rows = -(-loose_count // (16 * columns)) * 16
    loose_low = jnp.concatenate([p.reshape(-1) for p in three_parts(loose)])
    loose_low = jnp.pad(loose_low, (0, loose_rows * columns - loose_count)).reshape(loose_rows, columns)
    packed = jnp.concatenate([
        qkv_weight.transpose(1, 0, 2).reshape(3 * depth, columns), out_weight.T, loose_low], 0)
    gathered = lax.all_gather(packed, ("o", "i"), axis=0)
    gathered = lax.all_gather(gathered, "t", axis=0)
    mats = gathered[:, :, :4 * depth].reshape(parts, planes * inner, 4, depth, columns)
    mats = mats.transpose(2, 1, 3, 0, 4).reshape(1, 4, width, width)
    loose_all = gathered[:, :, 4 * depth:].reshape(parts, planes * inner, loose_rows * columns)
    loose_all = loose_all[:, :, :loose_count].astype(jnp.float32)
    loose_all = loose_all.reshape(parts, planes * inner, 3, small, 4 + experts)
    loose_all = (loose_all[:, :, 0] + loose_all[:, :, 1]) + loose_all[:, :, 2]
    loose_all = loose_all.transpose(1, 0, 2, 3).reshape(width, 4 + experts)
    norms = loose_all[:, :4].T
    router = jnp.pad(loose_all[:, 4:], ((0, 0), (0, LANES - experts)))
    router_parts = jnp.concatenate(three_parts(router[:, :experts]), 1).T
    router_parts = jnp.pad(router_parts, ((0, LANES - 3 * experts), (0, 0)))

    weights = []
    first_in = expert_in.reshape(homes, local, depth, extent)
    second_in = expert_out.transpose(0, 2, 1).reshape(homes, local, depth, extent)
    for k in range(local):
        both = jnp.stack([first_in[:, k], second_in[:, k]], 1)
        mine = lax.all_to_all(both, ("i", "t"), 0, 0, tiled=True)
        if planes == 2:
            other = lax.ppermute(mine, "o", [(0, 1), (1, 0)])
            full = jnp.where(plane_at == 0, jnp.stack([mine, other]), jnp.stack([other, mine]))
        else:
            full = lax.all_gather(mine, "o", axis=0)
        weights.append(full.reshape(planes, inner, parts, 2, depth, extent))

    own_first = part_at * own_rows
    slot_index = jnp.where(slot_ids >= 0, expert_ids * CAP + slot_ids, -1)
    if parts == 2:
        slot_index = jnp.concatenate([
            lax.dynamic_slice_in_dim(slot_index, own_first, own_rows, 1),
            lax.dynamic_slice_in_dim(slot_index, own_rows - own_first, own_rows, 1)], 1)
    homes_i = lax.broadcasted_iota(jnp.int32, (inner, local, CAP), 0)
    locals_i = lax.broadcasted_iota(jnp.int32, (inner, local, CAP), 1)
    cap_i = lax.broadcasted_iota(jnp.int32, (inner, local, CAP), 2)
    places = ((homes_i * parts + part_at) * local + locals_i) * CAP + cap_i

    def table(m, positions, rows=slice(None)):
        index = slot_index[m, rows]
        flat = positions.reshape(1, -1)
        return ((index[:, 0:1] == flat) | (index[:, 1:2] == flat)).astype(low)

    def share(rows):
        if parts == 2:
            return jnp.concatenate([rows, lax.ppermute(rows, "t", [(0, 1), (1, 0)])], 1)
        return lax.all_gather(rows, "t", axis=1, tiled=True)

    def dispatch(shared):
        sent = []
        for m in range(micros):
            slots = mm(table(m, places), shared[m], TN).astype(low)
            slots = lax.all_to_all(slots.reshape(inner, local * CAP, width), "i", 0, 0, tiled=True)
            sent.append(slots.reshape(inner, local, CAP, width))
        return [
            jnp.concatenate([s[:, k].reshape(inner * CAP, width) for s in sent], 0) for k in range(local)]

    cot_slots = dispatch(share(cotangent.astype(low)))

    flags = lax.dynamic_slice_in_dim(key_mask, part_at * images, images, 1).reshape(total, 1, length)
    bias = jnp.where(flags > 0, 0.0, -1e30).astype(jnp.float32)
    tok = tokens.reshape(total, length, width)
    per_step = 2 if total % 2 == 0 else 1
    middle, routed, proj, mixed, gates = attention_forward(tok, bias, mats, norms, router_parts, per_step)

    row_slots = dispatch(share(routed.reshape(micros, own_rows, width)))

    first_out, second_out, results, backs = [], [], [], []
    for k in range(local):
        expert = ((inner_at * parts + part_at) * local + k).astype(jnp.int32).reshape(1)
        result, back, dweights = run_expert(expert, row_slots[k], cot_slots[k], weights[k], router_parts)
        results.append(result.reshape(micros, inner, CAP, width))
        backs.append(back.reshape(micros, inner, CAP, width + LANES))
        dweights = dweights.reshape(planes, homes, 2, depth, extent)
        if planes == 2:
            theirs = lax.dynamic_index_in_dim(dweights, 1 - plane_at, 0, keepdims=False)
            ours = lax.dynamic_index_in_dim(dweights, plane_at, 0, keepdims=False)
            summed = ours.astype(jnp.float32) + lax.ppermute(
                theirs, "o", [(0, 1), (1, 0)]).astype(jnp.float32)
            summed = summed.astype(low)
        else:
            summed = lax.psum_scatter(dweights, "o", scatter_dimension=0, tiled=True)[0]
        final = lax.all_to_all(summed, ("i", "t"), 0, 0, tiled=True)
        first_out.append(final[:, 0])
        second_out.append(final[:, 1])
    first_grad = jnp.stack(first_out, 1).reshape(experts, depth, extent).astype(jnp.float32)
    second_grad = jnp.stack(second_out, 1).reshape(experts, depth, extent).astype(jnp.float32)
    second_grad = second_grad.transpose(0, 2, 1)

    def collect(values):
        size = values[0].shape[-1]
        answers = []
        for m in range(micros):
            back = jnp.stack([v[m] for v in values], 1).reshape(inner, local * CAP, size)
            back = lax.all_to_all(back, "i", 0, 0, tiled=True).reshape(inner * local * CAP, size)
            if parts == 2:
                away = mm(table(m, places, slice(own_rows, None)), back).astype(low)
                here = mm(table(m, places, slice(0, own_rows)), back)
                answers.append(here + lax.ppermute(away, "t", [(0, 1), (1, 0)]).astype(jnp.float32))
            else:
                whole = mm(table(m, places), back).astype(low)
                answers.append(lax.psum_scatter(
                    whole, "t", scatter_dimension=0, tiled=True).astype(jnp.float32))
        return jnp.stack(answers)

    grad = collect(backs)
    combined = collect(results)
    block_out = middle.reshape(micros, own_rows, width) + combined

    input_grad, dmats, dnorms, drouter = attention_backward(
        tok, middle, cotangent.reshape(total, length, width), grad.reshape(total, length, width + LANES),
        gates, proj, mixed, bias, mats, norms, router.T, per_step)
    input_grad = input_grad.reshape(micros, own_rows, width)

    dmats = dmats.reshape(4, planes, inner, depth, parts, columns).transpose(2, 4, 1, 0, 3, 5)
    dmats = dmats.reshape(homes, planes, 4 * depth, columns)
    dloose = jnp.concatenate([dnorms.T, drouter[:, :experts]], 1)
    dloose = dloose.reshape(planes, inner, parts, small * (4 + experts)).transpose(1, 2, 0, 3)
    dloose = jnp.concatenate(three_parts(dloose), -1)
    dloose = jnp.pad(dloose, ((0, 0),) * 3 + ((0, loose_rows * columns - loose_count),))
    dloose = dloose.reshape(homes, planes, loose_rows, columns)
    payload = jnp.concatenate([dmats, dloose], 2)
    payload = lax.all_to_all(payload, ("i", "t"), 0, 0, tiled=True)
    payload = jnp.sum(payload.astype(jnp.float32), 0)
    if planes == 2:
        theirs = lax.dynamic_index_in_dim(payload, 1 - plane_at, 0, keepdims=False)
        ours = lax.dynamic_index_in_dim(payload, plane_at, 0, keepdims=False)
        reduced = ours + lax.ppermute(theirs, "o", [(0, 1), (1, 0)])
    else:
        reduced = lax.psum_scatter(payload, "o", scatter_dimension=0, tiled=True)[0]
    matrices = reduced[:4 * depth].reshape(4, depth, columns)
    qkv_grad = matrices[:3].transpose(1, 0, 2)
    out_grad = matrices[3].T
    tail = reduced[4 * depth:].reshape(-1)[:loose_count].reshape(3, small, 4 + experts)
    tail = (tail[0] + tail[1]) + tail[2]
    return (
        block_out, input_grad, tail[:, 0], tail[:, 1], qkv_grad, out_grad, tail[:, 2], tail[:, 3],
        tail[:, 4:], first_grad, second_grad,
    )


def per_device_halves(tokens, key_mask, expert_ids, slot_ids, norm1_gain, norm1_bias,
                      qkv_weight, out_weight, norm2_gain, norm2_bias, router_weight, expert_in, expert_out,
                      cotangent):
    micros, own_rows, width = tokens.shape
    length = key_mask.shape[2]
    images = own_rows // length
    total = micros * images
    planes, inner, parts = 2, 8, 2
    experts = expert_in.shape[0]
    homes = inner * parts
    local = experts // homes
    depth, extent = expert_in.shape[1:]
    columns = qkv_weight.shape[2]
    plane_at, inner_at, part_at = (lax.axis_index(name) for name in ("o", "i", "t"))
    low = jnp.bfloat16
    across = [(0, 1), (1, 0)]

    norms_in = jnp.stack([norm1_gain, norm1_bias, norm2_gain, norm2_bias], 1)
    loose = [p for p in three_parts(router_weight)]
    loose += [jnp.pad(p, ((0, 0), (0, 4))) for p in three_parts(norms_in)]
    loose = jnp.concatenate(loose, 1)
    loose = jnp.pad(loose, ((0, 0), (0, columns - loose.shape[1])))
    packed = jnp.concatenate([
        qkv_weight.transpose(1, 0, 2).reshape(3 * depth, columns), out_weight.T, loose], 0)
    slot_index = jnp.where(slot_ids >= 0, expert_ids * CAP + slot_ids, -1).transpose(0, 2, 1)
    own_first = part_at * own_rows
    index = jnp.stack([
        lax.dynamic_slice_in_dim(slot_index, own_first, own_rows, 2),
        lax.dynamic_slice_in_dim(slot_index, own_rows - own_first, own_rows, 2)], 2)

    flags = lax.dynamic_slice_in_dim(key_mask, part_at * images, images, 1).reshape(total, 1, length)
    bias = jnp.where(flags > 0, 0.0, -1e30).astype(jnp.float32)
    tok = tokens.reshape(total, length, width)
    table = jnp.pad(index.transpose(0, 2, 3, 1), ((0, 0), (0, 0), (0, 0), (0, LANES - 2)))
    reduced, block_out, input_grad, dweights = opening(
        packed, cotangent.reshape(tok.shape), index, table, tok, bias, expert_in, expert_out.transpose(0, 2, 1), local, 2)[:4]
    first_grad = dweights[0, :, 0].astype(jnp.float32) + dweights[1, :, 0].astype(jnp.float32)
    second_grad = dweights[0, :, 1].astype(jnp.float32) + dweights[1, :, 1].astype(jnp.float32)
    second_grad = second_grad.transpose(0, 2, 1)
    matrices = reduced[:4 * depth].reshape(4, depth, columns)
    qkv_grad = matrices[:3].transpose(1, 0, 2)
    out_grad = matrices[3].T
    tail = reduced[4 * depth:]
    shape = (micros, own_rows, width)
    return (
        block_out.reshape(shape), input_grad.reshape(shape), tail[:, 96], tail[:, 97], qkv_grad, out_grad,
        tail[:, 98], tail[:, 99], tail[:, :experts], first_grad, second_grad,
    )


def solution(mesh):
    dp, parts = mesh.shape["dp"], mesh.shape["tensor"]
    inner = min(8, 32 // parts, dp)
    planes = dp // inner
    fine = Mesh(mesh.devices.reshape(planes, inner, parts), ("o", "i", "t"))
    dps = ("o", "i")
    every = ("o", "i", "t")
    rows = P(None, every, None)
    step = functools.partial(per_device, planes, inner, parts)
    if (planes, inner, parts) == (2, 8, 2):
        step = per_device_halves
    return jax.shard_map(
        step,
        mesh=fine,
        in_specs=(
            rows, P(None, dps, None), P(None, dps, None), P(None, dps, None), P(every), P(every),
            P(dps, None, "t"), P("t", dps), P(every), P(every), P(every, None),
            P(None, dps, "t"), P(None, "t", dps), rows,
        ),
        out_specs=(
            rows, rows, P(every), P(every), P(dps, None, "t"), P("t", dps), P(every), P(every),
            P(every, None), P(None, dps, "t"), P(None, "t", dps),
        ),
        check_vma=False,
    )
```

```python
import functools

import jax
import jax.numpy as jnp
from jax import lax
from jax.experimental import pallas as pl
from jax.experimental.pallas import tpu as pltpu
from jax.sharding import Mesh, PartitionSpec as P

HEAD = 64
CAP = 120
EPSILON = 1e-06
LANES = 128
VMEM = 60 * 1024 * 1024
NN = (((1,), (0,)), ((), ()))
NT = (((1,), (1,)), ((), ()))
TN = (((0,), (0,)), ((), ()))
HIGH = lax.Precision.HIGHEST
GELU_C = 0.7978845608028654
GELU_A = 0.044715


def mm(a, b, dims=NN, precision=None):
    return lax.dot_general(a, b, dims, precision=precision, preferred_element_type=jnp.float32)


def three_parts(value):
    high = value.astype(jnp.bfloat16)
    rest = value - high.astype(jnp.float32)
    middle = rest.astype(jnp.bfloat16)
    last = (rest - middle.astype(jnp.float32)).astype(jnp.bfloat16)
    return high, middle, last


def standardize(values):
    center = jnp.mean(values, -1, keepdims=True)
    shifted = values - center
    spread = jnp.mean(shifted * shifted, -1, keepdims=True)
    inverse = lax.rsqrt(spread + EPSILON)
    return shifted * inverse, inverse


def norm_back(grad, unit, inverse):
    return inverse * (
        grad
        - jnp.mean(grad, -1, keepdims=True)
        - unit * jnp.mean(grad * unit, -1, keepdims=True)
    )


def even_lanes(shape):
    return lax.broadcasted_iota(jnp.int32, shape, 1) < HEAD


def router_gates(routed, parts):
    logits = mm(routed, parts, NT)
    logits = logits + pltpu.roll(logits, LANES - 32, 1) + pltpu.roll(logits, LANES - 64, 1)
    lane = lax.broadcasted_iota(jnp.int32, logits.shape, 1)
    logits = jnp.where(lane < 32, logits, -1e30)
    lifted = jnp.exp(logits - jnp.max(logits, -1, keepdims=True))
    return lifted / jnp.sum(lifted, -1, keepdims=True)


def forward_rows(first, images, tok_ref, bias_ref, mats_ref, norms_ref, parts_ref,
                 middle_ref, proj_ref, mixed_ref, gates_ref):
    _, length, width = tok_ref.shape
    pieces, _, _, columns = mats_ref.shape
    rows = images * length
    here = pl.ds(first, images)
    tok = tok_ref[here].reshape(rows, width)
    unit, _ = standardize(tok)
    normed = (unit * norms_ref[0:1] + norms_ref[1:2]).astype(jnp.bfloat16)
    for c in range(3):
        for p in range(pieces):
            part = mm(normed, mats_ref[p, c]).reshape(images, length, columns)
            base = c * width + p * columns
            for b in range(images):
                proj_ref[first + b, :, base:base + columns] = part[b].astype(jnp.bfloat16)
    even = even_lanes((length, LANES))
    scale = jnp.bfloat16(HEAD ** -0.5)
    zero = jnp.zeros((), jnp.bfloat16)
    attended = []
    for b in range(images):
        bias = bias_ref[first + b]
        parts = []
        for pair in range(width // LANES):
            lanes = slice(pair * LANES, (pair + 1) * LANES)
            query = proj_ref[first + b, :, lanes] * scale
            keyed = proj_ref[first + b, :, width + pair * LANES:width + (pair + 1) * LANES]
            valued = proj_ref[first + b, :, 2 * width + pair * LANES:2 * width + (pair + 1) * LANES]
            halves = []
            for odd in range(2):
                chosen = jnp.where(even != bool(odd), query, zero)
                scores = mm(chosen, keyed, NT) + bias
                lifted = jnp.exp(scores - jnp.max(scores, -1, keepdims=True))
                probs = lifted * (1.0 / jnp.sum(lifted, -1, keepdims=True))
                halves.append(mm(probs.astype(jnp.bfloat16), valued))
            both = jnp.where(even, halves[0], halves[1])
            mixed_ref[first + b, :, lanes] = both.astype(jnp.bfloat16)
            parts.append(both)
        attended.append(jnp.concatenate(parts, 1))
    joined = jnp.concatenate(attended, 0).astype(jnp.bfloat16)
    middle = tok
    for p in range(pieces):
        middle += mm(joined[:, p * columns:(p + 1) * columns], mats_ref[p, 3], NT)
    middle_ref[here] = middle.reshape(images, length, width)
    unit, _ = standardize(middle)
    routed = unit * norms_ref[2:3] + norms_ref[3:4]
    low = routed.astype(jnp.bfloat16)
    gates_ref[here] = router_gates(low, parts_ref[...]).reshape(images, length, LANES)
    return routed, low


def forward_kernel(
    tok_ref, bias_ref, mats_ref, norms_ref, parts_ref,
    middle_ref, routed_ref, proj_ref, mixed_ref, gates_ref,
):
    images, length, width = tok_ref.shape
    routed, _ = forward_rows(0, images, tok_ref, bias_ref, mats_ref, norms_ref, parts_ref,
                             middle_ref, proj_ref, mixed_ref, gates_ref)
    routed_ref[...] = routed.reshape(images, length, width).astype(jnp.bfloat16)


def attention_forward(tok, bias, mats, norms, router, per_step):
    images, length, width = tok.shape

    def rows(last):
        return pl.BlockSpec((per_step, length, last), lambda s: (s, 0, 0))

    def whole(a):
        return pl.BlockSpec(a.shape, lambda s: (0,) * a.ndim)

    shapes = [
        (width, jnp.float32), (width, jnp.bfloat16), (3 * width, jnp.bfloat16),
        (width, jnp.bfloat16), (LANES, jnp.float32),
    ]
    return pl.pallas_call(
        forward_kernel,
        grid=(images // per_step,),
        in_specs=[
            rows(width), pl.BlockSpec((per_step, 1, length), lambda s: (s, 0, 0)),
            whole(mats), whole(norms), whole(router),
        ],
        out_specs=[rows(n) for n, _ in shapes],
        out_shape=[jax.ShapeDtypeStruct((images, length, n), kind) for n, kind in shapes],
        compiler_params=pltpu.CompilerParams(vmem_limit_bytes=VMEM),
        cost_estimate=pl.CostEstimate(
            flops=images * length * width * width * 10, bytes_accessed=images * length * width * 16,
            transcendentals=images * length * length * 8),
        name="attention_forward",
    )(tok, bias, mats, norms, router)


def backward_rows(first, images, grad, tok_ref, middle_ref, cot_ref, gates_ref, proj_ref, mixed_ref,
                  bias_ref, mats_ref, norms_ref, router_t_ref,
                  input_ref, dnorms_ref, drouter_ref, dproj_ref, dmats_acc):
    _, length, width = tok_ref.shape
    rows = images * length
    here = pl.ds(first, images)

    def flat(ref):
        return ref[here].reshape(rows, ref.shape[2])

    middle = flat(middle_ref)
    unit, inverse = standardize(middle)
    gates = flat(gates_ref)
    gate_cot = grad[:, width:]
    logit_grad = gates * (gate_cot - jnp.sum(gates * gate_cot, -1, keepdims=True))
    routed = (unit * norms_ref[2:3] + norms_ref[3:4]).astype(jnp.bfloat16)
    drouter_ref[...] += mm(routed.astype(jnp.float32), logit_grad, TN, HIGH)
    routed_grad = grad[:, :width] + mm(logit_grad, router_t_ref[...], NN, HIGH)
    dnorms_ref[2:3] += jnp.sum(routed_grad * unit, 0, keepdims=True)
    dnorms_ref[3:4] += jnp.sum(routed_grad, 0, keepdims=True)
    middle_grad = flat(cot_ref) + norm_back(routed_grad * norms_ref[2:3], unit, inverse)
    attn_cot = middle_grad.astype(jnp.bfloat16)
    joined = jnp.concatenate([mixed_ref[first + b].astype(jnp.float32) for b in range(images)], 0)
    joined = joined.astype(jnp.bfloat16)
    pieces, _, _, columns = mats_ref.shape
    spans = [slice(p * columns, (p + 1) * columns) for p in range(pieces)]
    for p in range(pieces):
        dmats_acc[p, 3] += mm(attn_cot, joined[:, spans[p]], TN)
    mixed_grad = jnp.concatenate([mm(attn_cot, mats_ref[p, 3]) for p in range(pieces)], 1)
    mixed_grad = mixed_grad.reshape(images, length, width)
    even = even_lanes((length, LANES))
    zero = jnp.zeros((), jnp.bfloat16)
    scale = jnp.bfloat16(HEAD ** -0.5)
    for b in range(images):
        bias = bias_ref[first + b]
        mixed_low = mixed_grad[b].astype(jnp.bfloat16)
        for pair in range(width // LANES):
            lanes = slice(pair * LANES, (pair + 1) * LANES)
            query = proj_ref[first + b, :, lanes] * scale
            keyed = proj_ref[first + b, :, width + pair * LANES:width + (pair + 1) * LANES]
            valued = proj_ref[first + b, :, 2 * width + pair * LANES:2 * width + (pair + 1) * LANES]
            out_cot = mixed_low[:, lanes]
            query_grad = keyed_grad = value_grad = None
            for odd in range(2):
                mask = even != bool(odd)
                query_half = jnp.where(mask, query, zero)
                keyed_half = jnp.where(mask, keyed, zero)
                cot_half = jnp.where(mask, out_cot, zero)
                scores = mm(query_half, keyed, NT) + bias
                lifted = jnp.exp(scores - jnp.max(scores, -1, keepdims=True))
                probs = lifted * (1.0 / jnp.sum(lifted, -1, keepdims=True))
                prob_grad = mm(cot_half, valued, NT)
                value_part = mm(probs.astype(jnp.bfloat16), cot_half, TN)
                inner = jnp.sum(probs * prob_grad, -1, keepdims=True)
                score_grad = (probs * (prob_grad - inner)).astype(jnp.bfloat16)
                query_part = mm(score_grad, keyed_half)
                keyed_part = mm(score_grad, query_half, TN)
                if odd:
                    query_grad, keyed_grad, value_grad = (
                        query_grad + query_part, keyed_grad + keyed_part, value_grad + value_part)
                else:
                    query_grad, keyed_grad, value_grad = query_part, keyed_part, value_part
            base = pair * LANES
            rows_here = slice(b * length, (b + 1) * length)
            dproj_ref[rows_here, base:base + LANES] = query_grad * (HEAD ** -0.5)
            dproj_ref[rows_here, width + base:width + base + LANES] = keyed_grad
            dproj_ref[rows_here, 2 * width + base:2 * width + base + LANES] = value_grad
    tok = flat(tok_ref)
    unit, inverse = standardize(tok)
    normed = (unit * norms_ref[0:1] + norms_ref[1:2]).astype(jnp.bfloat16)
    normed_grad = jnp.zeros((rows, width), jnp.float32)
    for c in range(3):
        part = dproj_ref[:, c * width:(c + 1) * width].astype(jnp.bfloat16)
        for p in range(pieces):
            dmats_acc[p, c] += mm(normed, part[:, spans[p]], TN)
            normed_grad += mm(part[:, spans[p]], mats_ref[p, c], NT)
    dnorms_ref[0:1] += jnp.sum(normed_grad * unit, 0, keepdims=True)
    dnorms_ref[1:2] += jnp.sum(normed_grad, 0, keepdims=True)
    input_grad = middle_grad + norm_back(normed_grad * norms_ref[0:1], unit, inverse)
    input_ref[here] = input_grad.reshape(images, length, width)


def backward_kernel(
    tok_ref, middle_ref, cot_ref, grad_ref, gates_ref, proj_ref, mixed_ref,
    bias_ref, mats_ref, norms_ref, router_t_ref,
    input_ref, dmats_ref, dnorms_ref, drouter_ref,
    dproj_ref, dmats_acc,
):
    images, length, width = tok_ref.shape
    rows = images * length
    step = pl.program_id(0)

    @pl.when(step == 0)
    def _():
        dmats_acc[...] = jnp.zeros_like(dmats_acc)
        dnorms_ref[...] = jnp.zeros_like(dnorms_ref)
        drouter_ref[...] = jnp.zeros_like(drouter_ref)

    backward_rows(0, images, grad_ref[...].reshape(rows, grad_ref.shape[2]), tok_ref, middle_ref, cot_ref,
                  gates_ref, proj_ref, mixed_ref, bias_ref, mats_ref, norms_ref, router_t_ref,
                  input_ref, dnorms_ref, drouter_ref, dproj_ref, dmats_acc)

    @pl.when(step == pl.num_programs(0) - 1)
    def _():
        dmats_ref[...] = dmats_acc[...].astype(jnp.bfloat16)


def attention_backward(tok, middle, cot, grad, gates, proj, mixed, bias, mats, norms, router_t, per_step):
    images, length, width = tok.shape

    def rows(last):
        return pl.BlockSpec((per_step, length, last), lambda s: (s, 0, 0))

    def whole(shape):
        return pl.BlockSpec(shape, lambda s: (0,) * len(shape))

    return pl.pallas_call(
        backward_kernel,
        grid=(images // per_step,),
        in_specs=[
            rows(width), rows(width), rows(width), rows(width + LANES), rows(LANES),
            rows(3 * width), rows(width), pl.BlockSpec((per_step, 1, length), lambda s: (s, 0, 0)),
            whole(mats.shape), whole(norms.shape), whole(router_t.shape),
        ],
        out_specs=[
            rows(width), whole(mats.shape), whole((4, width)), whole((width, LANES)),
        ],
        out_shape=[
            jax.ShapeDtypeStruct((images, length, width), jnp.float32),
            jax.ShapeDtypeStruct(mats.shape, jnp.bfloat16),
            jax.ShapeDtypeStruct((4, width), jnp.float32),
            jax.ShapeDtypeStruct((width, LANES), jnp.float32),
        ],
        scratch_shapes=[
            pltpu.VMEM((per_step * length, 3 * width), jnp.float32),
            pltpu.VMEM(mats.shape, jnp.float32),
        ],
        compiler_params=pltpu.CompilerParams(vmem_limit_bytes=VMEM),
        cost_estimate=pl.CostEstimate(
            flops=images * length * width * width * 30, bytes_accessed=images * length * width * 30,
            transcendentals=images * length * length * 8),
        name="attention_backward",
    )(tok, middle, cot, grad, gates, proj, mixed, bias, mats, norms, router_t)


def expert_kernel(
    expert_ref, slots_ref, cots_ref, weights_ref, router_ref,
    result_ref, back_ref, dweights_ref,
    rows_t, grads_t, grads, gate_scr, result_acc, back_acc, first_acc, second_acc,
):
    count, width = slots_ref.shape
    tile = weights_ref.shape[-1]
    chunk = rows_t.shape[2]
    step = pl.program_id(0)
    first = weights_ref[:, :, 0, 0].reshape(width, tile)
    second = weights_ref[:, :, 0, 1].reshape(width, tile)

    @pl.when(step == 0)
    def _():
        def prepare(r, carry):
            here = pl.ds(pl.multiple_of(r * chunk, 16), chunk)
            slots = slots_ref[here]
            gates = router_gates(slots, router_ref[...])
            lane = lax.broadcasted_iota(jnp.int32, gates.shape, 1)
            gate = jnp.sum(jnp.where(lane == expert_ref[0], gates, 0.0), -1, keepdims=True)
            gate_scr[here] = jnp.broadcast_to(gate, gates.shape)
            low = (cots_ref[here].astype(jnp.float32) * gate).astype(jnp.bfloat16)
            grads[here] = low
            rows_t[r] = slots.T
            grads_t[r] = low.T
            result_acc[here] = jnp.zeros((chunk, width), jnp.float32)
            back_acc[here] = jnp.zeros((chunk, width), jnp.float32)
            return carry

        lax.fori_loop(0, count // chunk, prepare, 0)

    first_acc[...] = jnp.zeros_like(first_acc)
    second_acc[...] = jnp.zeros_like(second_acc)

    def work(r, carry):
        here = pl.ds(pl.multiple_of(r * chunk, 16), chunk)
        pre = mm(slots_ref[here], first)
        square = pre * pre
        half = 0.5 + 0.5 * jnp.tanh(pre * (GELU_C + (GELU_C * GELU_A) * square))
        hidden = (pre * half).astype(jnp.bfloat16)
        slope = half + 2.0 * half * (1.0 - half) * pre * (GELU_C + (3.0 * GELU_C * GELU_A) * square)
        hidden_grad = mm(grads[here], second)
        pre_grad = (hidden_grad * slope).astype(jnp.bfloat16)
        result_acc[here] += mm(hidden, second, NT)
        back_acc[here] += mm(pre_grad, first, NT)
        first_acc[...] += mm(rows_t[r], pre_grad)
        second_acc[...] += mm(grads_t[r], hidden)
        return carry

    lax.fori_loop(0, count // chunk, work, 0)
    block = weights_ref.shape[:2] + weights_ref.shape[4:]
    dweights_ref[:, :, 0, 0] = first_acc[...].astype(jnp.bfloat16).reshape(block)
    dweights_ref[:, :, 0, 1] = second_acc[...].astype(jnp.bfloat16).reshape(block)

    @pl.when(step == pl.num_programs(0) - 1)
    def _():
        def finish(r, carry):
            here = pl.ds(pl.multiple_of(r * chunk, 16), chunk)
            result = result_acc[here]
            gate = gate_scr[here][:, 0:1]
            result_ref[here] = (result * gate).astype(jnp.bfloat16)
            gate_grad = jnp.sum(cots_ref[here].astype(jnp.float32) * result, -1, keepdims=True)
            lane = lax.broadcasted_iota(jnp.int32, (chunk, LANES), 1)
            back_ref[here, 0:width] = back_acc[here].astype(jnp.bfloat16)
            back_ref[here, width:width + LANES] = jnp.where(
                lane == expert_ref[0], gate_grad, 0.0).astype(jnp.bfloat16)
            return carry

        lax.fori_loop(0, count // chunk, finish, 0)


def run_expert(expert, slots, cots, weights, router):
    count, width = slots.shape
    planes, inner, parts, _, depth, extent = weights.shape
    tile = min(512, extent)
    per_part = extent // tile
    chunk = 480

    def whole(shape):
        return pl.BlockSpec(shape, lambda s, e: (0,) * len(shape))

    weight_spec = pl.BlockSpec(
        (planes, inner, 1, 2, depth, tile), lambda s, e: (0, 0, s // per_part, 0, 0, s % per_part))
    return pl.pallas_call(
        expert_kernel,
        grid_spec=pltpu.PrefetchScalarGridSpec(
            num_scalar_prefetch=1,
            grid=(parts * per_part,),
            in_specs=[whole(slots.shape), whole(cots.shape), weight_spec, whole(router.shape)],
            out_specs=[whole((count, width)), whole((count, width + LANES)), weight_spec],
            scratch_shapes=[
                pltpu.VMEM((count // chunk, width, chunk), jnp.bfloat16),
                pltpu.VMEM((count // chunk, width, chunk), jnp.bfloat16),
                pltpu.VMEM((count, width), jnp.bfloat16),
                pltpu.VMEM((count, LANES), jnp.float32),
                pltpu.VMEM((count, width), jnp.float32),
                pltpu.VMEM((count, width), jnp.float32),
                pltpu.VMEM((width, tile), jnp.float32),
                pltpu.VMEM((width, tile), jnp.float32),
            ],
        ),
        out_shape=[
            jax.ShapeDtypeStruct((count, width), jnp.bfloat16),
            jax.ShapeDtypeStruct((count, width + LANES), jnp.bfloat16),
            jax.ShapeDtypeStruct(weights.shape, jnp.bfloat16),
        ],
        compiler_params=pltpu.CompilerParams(vmem_limit_bytes=VMEM),
        cost_estimate=pl.CostEstimate(
            flops=12 * count * width * extent * parts,
            bytes_accessed=4 * 2 * width * extent * parts + count * width * 8,
            transcendentals=count * extent * parts),
        name="expert",
    )(expert, slots, cots, weights, router)


def flipped(position, bit):
    return position + bit - 2 * bit * lax.rem(position // bit, 2)


def to_peer(source, target, sends, receives, where):
    return pltpu.make_async_remote_copy(
        src_ref=source, dst_ref=target, send_sem=sends, recv_sem=receives, device_id=where,
        device_id_type=pl.DeviceIdType.MESH)


class Dispatch:
    def __init__(self, index_ref, shared, staged, out, sends, receives, keep, inner, parts, local):
        self.index_ref, self.shared, self.staged, self.out = index_ref, shared, staged, out
        self.sends, self.receives, self.keep = sends, receives, keep
        self.inner, self.parts, self.local = inner, parts, local
        self.at_i, self.at_t = lax.axis_index("i"), lax.axis_index("t")

    def copy(self, m, d, k):
        home = lax.rem(self.at_i + d, self.inner)
        target = self.out.at[k, pl.ds(pl.multiple_of((m * self.inner + self.at_i) * CAP, 8), CAP)]
        return to_peer(self.staged.at[m, d, k], target, self.sends.at[m, d, k],
                       self.receives.at[m, d, k], {"i": home})

    def kept(self, m, k):
        target = self.out.at[k, pl.ds(pl.multiple_of((m * self.inner + self.at_i) * CAP, 8), CAP)]
        return pltpu.make_async_copy(self.staged.at[m, 0, k], target, self.keep.at[m, k])

    def fill(self, m, d):
        home = lax.rem(self.at_i + d, self.inner)
        count = self.local * CAP
        base = (home * self.parts + self.at_t) * count
        places = base + lax.broadcasted_iota(jnp.int32, (count, 1), 0)
        total = None
        for half in range(2):
            first = self.index_ref[m, 0, half:half + 1]
            second = self.index_ref[m, 1, half:half + 1]
            hits = jnp.where((first == places) | (second == places), 1.0, 0.0).astype(jnp.bfloat16)
            part = mm(hits, self.shared[m, half])
            total = part if total is None else total + part
        for k in range(self.local):
            self.staged[m, d, k] = total[k * CAP:(k + 1) * CAP].astype(jnp.bfloat16)

    def send(self, m, beside=None):
        def step(d, carry):
            self.fill(m, d)
            for k in range(self.local):
                self.copy(m, d, k).start()
            if beside is not None:
                beside(d)
            return carry

        lax.fori_loop(1, self.inner, step, 0)
        self.fill(m, 0)
        for k in range(self.local):
            self.kept(m, k).start()

    def finish(self, m):
        def step(d, carry):
            for k in range(self.local):
                self.copy(m, d, k).wait()
            return carry

        lax.fori_loop(1, self.inner, step, 0)
        for k in range(self.local):
            self.kept(m, k).wait()


def flipped_if(position, bit, on):
    return position + on * (bit - 2 * bit * lax.rem(position // bit, 2))


class Answer:
    def __init__(self, staged, out, sends, receives, keep, inner):
        self.staged, self.out, self.sends, self.receives, self.keep = staged, out, sends, receives, keep
        self.inner = inner
        self.at_i = lax.axis_index("i")

    def target(self, k, m):
        return self.out.at[k, m, pl.ds(pl.multiple_of(self.at_i * CAP, 8), CAP)]

    def copy(self, k, m, d):
        group = lax.rem(self.at_i + d, self.inner)
        return to_peer(self.staged.at[m, group, k], self.target(k, m), self.sends.at[k, m, d],
                       self.receives.at[k, m, d], {"i": group})

    def kept(self, k, m):
        return pltpu.make_async_copy(self.staged.at[m, self.at_i, k], self.target(k, m), self.keep.at[k, m])

    def send(self, k, m, beside=None):
        def step(d, carry):
            self.copy(k, m, d).start()
            if beside is not None:
                beside(d)
            return carry

        lax.fori_loop(1, self.inner, step, 0)
        self.kept(k, m).start()

    def finish(self, k, m):
        def step(d, carry):
            self.copy(k, m, d).wait()
            return carry

        lax.fori_loop(1, self.inner, step, 0)
        self.kept(k, m).wait()


def device_at(n, origin):
    o, i, t = origin
    return lax.rem(o + n // 16, 2), lax.rem(i + lax.rem(n // 2, 8), 8), lax.rem(t + lax.rem(n, 2), 2)


class Weights:
    def __init__(self, local, sources, target, sends, receives, keep):
        self.local, self.sources, self.target = local, sources, target
        self.sends, self.receives, self.keep = sends, receives, keep
        self.origin = tuple(lax.axis_index(name) for name in ("o", "i", "t"))

    def place(self, k, part):
        o, i, t = self.origin
        return self.target.at[k, o, i, t, part]

    def copy(self, k, n, part):
        o, i, t = device_at(n, self.origin)
        expert = (i * 2 + t) * self.local + k
        return to_peer(self.sources[part].at[expert], self.place(k, part), self.sends.at[k, n, part],
                       self.receives.at[k, n, part], {"o": o, "i": i, "t": t})

    def kept(self, k, part):
        _, i, t = self.origin
        expert = (i * 2 + t) * self.local + k
        return pltpu.make_async_copy(
            self.sources[part].at[expert], self.place(k, part), self.keep.at[k, part])

    def give(self, k, n):
        for part in range(2):
            self.copy(k, n, part).start()

    def give_all(self, k, first, last):
        def step(n, carry):
            self.give(k, n)
            return carry

        lax.fori_loop(first, last, step, 0)

    def keep_own(self, k):
        for part in range(2):
            self.kept(k, part).start()

    def finish(self, k):
        def step(n, carry):
            for part in range(2):
                self.copy(k, n, part).wait()
            return carry

        lax.fori_loop(1, 32, step, 0)
        for part in range(2):
            self.kept(k, part).wait()


class Gradients:
    def __init__(self, local, source, target, sends, receives, keep):
        self.local, self.source, self.target = local, source, target
        self.sends, self.receives, self.keep = sends, receives, keep
        self.origin = tuple(lax.axis_index(name) for name in ("o", "i", "t"))

    def place(self, k, part):
        o, i, t = self.origin
        return self.target.at[o, (i * 2 + t) * self.local + k, part]

    def copy(self, k, n, part):
        o, i, t = device_at(n, self.origin)
        return to_peer(self.source.at[k, o, i, t, part], self.place(k, part), self.sends.at[k, n, part],
                       self.receives.at[k, n, part], {"o": o, "i": i, "t": t})

    def kept(self, k, part):
        o, i, t = self.origin
        return pltpu.make_async_copy(
            self.source.at[k, o, i, t, part], self.place(k, part), self.keep.at[k, part])

    give = Weights.give
    give_all = Weights.give_all
    keep_own = Weights.keep_own
    finish = Weights.finish


def expert_scratch(count, width, tile, chunk):
    steps = count // chunk
    return [
        pltpu.VMEM((count, width), jnp.bfloat16), pltpu.VMEM((count, width), jnp.bfloat16),
        pltpu.VMEM((steps, width, chunk), jnp.bfloat16), pltpu.VMEM((steps, width, chunk), jnp.bfloat16),
        pltpu.VMEM((count, width), jnp.bfloat16), pltpu.VMEM((count, LANES), jnp.float32),
        pltpu.VMEM((count, width), jnp.float32), pltpu.VMEM((count, width), jnp.float32),
        pltpu.VMEM((2, width, tile), jnp.float32), pltpu.VMEM((2, width, tile), jnp.bfloat16),
        pltpu.SemaphoreType.DMA((2,)),
    ]


def expert_phase(k, expert, slots_hbm, cots_hbm, held, parts_ref, answers, gradients, scratch):
    slots, cots, rows_t, grads_t, grads, gate_scr, result_acc, back_acc, sums, tiles, load = scratch
    count, width = slots.shape
    chunk = rows_t.shape[2]
    tile = tiles.shape[2]
    micros, groups = answers[0].staged.shape[:2]
    loads = [pltpu.make_async_copy(slots_hbm.at[k], slots, load.at[0]),
             pltpu.make_async_copy(cots_hbm.at[k], cots, load.at[1])]
    for copy in loads:
        copy.start()
    for copy in loads:
        copy.wait()

    def prepare(r, carry):
        here = pl.ds(pl.multiple_of(r * chunk, 16), chunk)
        rows = slots[here]
        gates = router_gates(rows, parts_ref[...])
        lane = lax.broadcasted_iota(jnp.int32, gates.shape, 1)
        gate = jnp.sum(jnp.where(lane == expert, gates, 0.0), -1, keepdims=True)
        gate_scr[here] = jnp.broadcast_to(gate, gates.shape)
        low = (cots[here].astype(jnp.float32) * gate).astype(jnp.bfloat16)
        grads[here] = low
        rows_t[r] = rows.T
        grads_t[r] = low.T
        result_acc[here] = jnp.zeros((chunk, width), jnp.float32)
        back_acc[here] = jnp.zeros((chunk, width), jnp.float32)
        return carry

    lax.fori_loop(0, count // chunk, prepare, 0)
    per_part = held.shape[6] // tile

    def one_tile(n, carry):
        t = n // per_part
        span = pl.ds(pl.multiple_of(lax.rem(n, per_part) * tile, tile), tile)
        for part in range(2):
            tiles[part] = held[k, :, :, t, part, :, span].reshape(width, tile)
        sums[...] = jnp.zeros_like(sums)

        def work(r, inside):
            here = pl.ds(pl.multiple_of(r * chunk, 16), chunk)
            pre = mm(slots[here], tiles[0])
            square = pre * pre
            half = 0.5 + 0.5 * jnp.tanh(pre * (GELU_C + (GELU_C * GELU_A) * square))
            hidden = (pre * half).astype(jnp.bfloat16)
            slope = half + 2.0 * half * (1.0 - half) * pre * (
                GELU_C + (3.0 * GELU_C * GELU_A) * square)
            pre_grad = (mm(grads[here], tiles[1]) * slope).astype(jnp.bfloat16)
            result_acc[here] += mm(hidden, tiles[1], NT)
            back_acc[here] += mm(pre_grad, tiles[0], NT)
            sums[0] += mm(rows_t[r], pre_grad)
            sums[1] += mm(grads_t[r], hidden)
            return inside

        lax.fori_loop(0, count // chunk, work, 0)
        block = held.shape[1:3] + (held.shape[5], tile)
        for part in range(2):
            held[k, :, :, t, part, :, span] = sums[part].astype(jnp.bfloat16).reshape(block)
        return carry

    lax.fori_loop(0, held.shape[3] * per_part, one_tile, 0)
    per_chunk = chunk // CAP
    back, result = answers

    def finish(n, carry):
        here = pl.ds(pl.multiple_of(n * chunk, 16), chunk)
        m, r = n // (groups // per_chunk), lax.rem(n, groups // per_chunk)
        value = result_acc[here]
        gate_grad = jnp.sum(cots[here].astype(jnp.float32) * value, -1, keepdims=True)
        lane = lax.broadcasted_iota(jnp.int32, (chunk, LANES), 1)
        spread = jnp.where(lane == expert, gate_grad, 0.0)
        value = value * gate_scr[here][:, 0:1]
        grad = back_acc[here]
        for q in range(per_chunk):
            rows = slice(q * CAP, (q + 1) * CAP)
            at = r * per_chunk + q
            result.staged[m, at, k] = value[rows].astype(jnp.bfloat16)
            back.staged[m, at, k, :, 0:width] = grad[rows].astype(jnp.bfloat16)
            back.staged[m, at, k, :, width:width + LANES] = spread[rows].astype(jnp.bfloat16)
        return carry

    lax.fori_loop(0, micros * groups // per_chunk, finish, 0)

    def one_more(d):
        @pl.when(k == 0)
        def _():
            gradients.give(0, 15 + d)

    for m in range(micros):
        back.send(k, m, one_more if m == 0 else None)

    @pl.when(k == 0)
    def _():
        gradients.give_all(0, 23, 26)


def opening_kernel(
    local, per_step, pack_ref, cot_ref, index_ref, table_ref, tok_ref, bias_ref, first_ref, second_ref,
    small_ref, block_out, input_out, dweights_ref, middle_out, proj_out, mixed_out, gates_out,
    slots_ref, cots_ref, back_ref, result_ref,
    gathered, partial, loose, mats_ref, norms_ref, parts_ref, router_ref, shared_c, shared_r, away_g,
    staged_c, staged_r, held, staged_back,
    load, ring_send, ring_recv, pair_send, pair_recv, pair_send_r, pair_recv_r,
    cot_send, cot_recv, cot_keep, row_send, row_recv, row_keep,
    weight_send, weight_recv, weight_keep, grad_send, grad_recv, grad_keep,
    back_send, back_recv, back_keep, result_send, result_recv, result_keep, store,
    away_send, away_recv, fold_send, fold_recv, fetch,
):
    at_o, at_i, at_t = (lax.axis_index(name) for name in ("o", "i", "t"))
    micros, _, own_rows, width = shared_c.shape
    images, length, _ = tok_ref.shape
    kinds, columns = mats_ref.shape[1], mats_ref.shape[3]
    depth = width // 16
    rows = per_step * length
    steps = own_rows // rows
    stages = [
        {"t": 1 - at_t}, {"o": 1 - at_o}, {"i": flipped(at_i, 4)}, {"i": flipped(at_i, 2)},
        {"i": flipped(at_i, 1)},
    ]
    cot_plan = Dispatch(index_ref, shared_c, staged_c, cots_ref, cot_send, cot_recv, cot_keep, 8, 2, local)
    row_plan = Dispatch(index_ref, shared_r, staged_r, slots_ref, row_send, row_recv, row_keep, 8, 2, local)
    weights = Weights(local, (first_ref, second_ref), held, weight_send, weight_recv, weight_keep)
    gradients = Gradients(local, held, dweights_ref, grad_send, grad_recv, grad_keep)

    def stage(j):
        size = 2 ** j
        return to_peer(gathered.at[pl.ds(0, size)], gathered.at[pl.ds(size, size)],
                       ring_send.at[j], ring_recv.at[j], stages[j])

    def swap_c(m):
        return to_peer(shared_c.at[m, 0], shared_c.at[m, 1], pair_send.at[m], pair_recv.at[m],
                       {"t": 1 - at_t})

    def swap_r(m, s):
        here = pl.ds(pl.multiple_of(s * rows, 16), rows)
        return to_peer(shared_r.at[m, 0, here], shared_r.at[m, 1, here], pair_send_r.at[m, s],
                       pair_recv_r.at[m, s], {"t": 1 - at_t})

    def relative(r):
        o = flipped_if(at_o, 1, lax.rem(r // 2, 2))
        i = flipped_if(at_i, 4, lax.rem(r // 4, 2))
        i = flipped_if(i, 2, lax.rem(r // 8, 2))
        i = flipped_if(i, 1, lax.rem(r // 16, 2))
        return o, i, flipped_if(at_t, 1, lax.rem(r, 2))

    def opening(tok, cot, proj, mixed, gates):
        fill = pltpu.make_async_copy(pack_ref, gathered.at[0], load.at[0])
        take_cot = pltpu.make_async_copy(cot_ref, cot, load.at[1])
        take_tok = pltpu.make_async_copy(tok_ref, tok, load.at[2])
        fill.start()
        take_cot.start()
        take_tok.start()
        fill.wait()
        stage(0).start()
        take_cot.wait()
        shared_c[0, 0] = cot[0:images // 2].reshape(own_rows, width).astype(jnp.bfloat16)
        swap_c(0).start()
        stage(0).wait()
        stage(1).start()
        shared_c[1, 0] = cot[images // 2:].reshape(own_rows, width).astype(jnp.bfloat16)
        swap_c(1).start()
        stage(1).wait()
        stage(2).start()
        stage(2).wait()
        stage(3).start()
        weights.give_all(0, 30, 32)
        swap_c(0).wait()
        cot_plan.send(0, lambda d: weights.give(0, d + 15))
        stage(3).wait()
        stage(4).start()
        swap_c(1).wait()
        cot_plan.send(1, lambda d: weights.give(0, d + 22))
        weights.give_all(0, 1, 16)
        weights.keep_own(0)
        stage(4).wait()

        def place(r, carry):
            o, i, t = relative(r)
            row = pl.multiple_of((o * 8 + i) * depth, depth)
            for c in range(kinds):
                mats_ref[t, c, pl.ds(row, depth)] = gathered[r, c * depth:(c + 1) * depth]
            loose[(o * 8 + i) * 2 + t] = gathered[r, kinds * depth:, 0:LANES].astype(jnp.float32)
            return carry

        lax.fori_loop(0, gathered.shape[0], place, 0)
        turned = loose[...].reshape(width, LANES).T
        norms_ref[...] = turned[96:104] + turned[104:112] + turned[112:120]
        low = turned[0:96].astype(jnp.bfloat16)
        parts_ref[...] = jnp.concatenate([low, jnp.zeros((32, width), jnp.bfloat16)], 0)
        router_ref[0:32] = turned[0:32] + turned[32:64] + turned[64:96]
        router_ref[32:] = jnp.zeros((96, width), jnp.float32)
        take_tok.wait()

        def attend(n, carry):
            m, s = n // steps, lax.rem(n, steps)
            _, routed = forward_rows(n * per_step, per_step, tok, bias_ref, mats_ref, norms_ref, parts_ref,
                                     tok, proj, mixed, gates)
            shared_r[m, 0, pl.ds(pl.multiple_of(s * rows, 16), rows)] = routed
            swap_r(m, s).start()
            return carry

        lax.fori_loop(0, micros * steps, attend, 0)
        outs = [(tok, middle_out), (proj, proj_out), (mixed, mixed_out), (gates, gates_out)]
        stores = [pltpu.make_async_copy(a, b, store.at[n]) for n, (a, b) in enumerate(outs)]
        for copy in stores:
            copy.start()
        for m in range(micros):
            for s in range(steps):
                swap_r(m, s).wait()
            row_plan.send(m, (lambda d: weights.give(1, d + 15)) if m == 0 else None)
        weights.give_all(1, 23, 32)
        weights.give_all(1, 1, 16)
        weights.keep_own(1)
        for copy in stores:
            copy.wait()

    pl.run_scoped(
        opening,
        pltpu.VMEM(tok_ref.shape, jnp.float32),
        pltpu.VMEM(cot_ref.shape, jnp.float32),
        pltpu.VMEM((images, length, 3 * width), jnp.bfloat16),
        pltpu.VMEM((images, length, width), jnp.bfloat16),
        pltpu.VMEM((images, length, LANES), jnp.float32),
    )
    for m in range(micros):
        row_plan.finish(m)
        cot_plan.finish(m)
    back = Answer(staged_back, back_ref, back_send, back_recv, back_keep, 8)
    result = Answer(staged_c, result_ref, result_send, result_recv, result_keep, 8)
    count = slots_ref.shape[1]

    def experts(*scratch):
        def one(k, carry):
            weights.finish(k)
            expert = (at_i * 2 + at_t) * local + k
            expert_phase(k, expert, slots_ref, cots_ref, held, parts_ref, (back, result), gradients, scratch)
            return carry

        lax.fori_loop(0, local, one, 0)

    pl.run_scoped(experts, *expert_scratch(count, width, 512, 480))

    gradients.give_all(0, 26, 32)
    result.send(0, 0, lambda d: gradients.give(1, 15 + d))
    result.send(0, 1, lambda d: gradients.give(1, 22 + d))
    gradients.give_all(1, 30, 32)
    for m in range(micros):
        result.send(1, m)

    def rest(k, carry):
        gradients.give_all(k, 1, 16)
        gradients.keep_own(k)
        return carry

    lax.fori_loop(0, local, rest, 0)

    places = lax.broadcasted_iota(jnp.int32, (1, 8 * CAP), 1)
    block = sum((places >= q * CAP).astype(jnp.int32) for q in range(1, 8))
    places = places + block * (3 * CAP) + at_t * (2 * CAP)

    def taken(table, m, half, here, values):
        first, second = table[m, half, here, 0:1], table[m, half, here, 1:2]
        total = None
        for k in range(local):
            where = places + k * CAP
            hits = jnp.where((first == where) | (second == where), 1.0, 0.0).astype(jnp.bfloat16)
            part = mm(hits, values[k])
            total = part if total is None else total + part
        return total

    across = {"t": 1 - at_t}

    def away(m, s, which):
        here = pl.ds(pl.multiple_of(s * rows, 16), rows)
        buffer = (shared_r, away_g, shared_c)[which]
        return to_peer(buffer.at[m, 0, here], buffer.at[m, 1, here], away_send.at[which, m, s],
                       away_recv.at[which, m, s], across)

    def collect(own):
        def fetched(table, backs):
            take = pltpu.make_async_copy(table_ref, table, fetch.at[2])
            take.start()
            take.wait()
            for m in range(micros):
                for k in range(local):
                    back.finish(k, m)
                    pltpu.make_async_copy(back_ref.at[k, m], backs.at[k], fetch.at[k]).start()
                for k in range(local):
                    pltpu.make_async_copy(back_ref.at[k, m], backs.at[k], fetch.at[k]).wait()

                def leave(s, carry):
                    here = pl.ds(pl.multiple_of(s * rows, 16), rows)
                    total = taken(table, m, 1, here, backs).astype(jnp.bfloat16)
                    shared_r[m, 0, here] = total[:, :width]
                    away_g[m, 0, here] = total[:, width:]
                    away(m, s, 0).start()
                    away(m, s, 1).start()
                    return carry

                lax.fori_loop(0, steps, leave, 0)

                def stay(s, carry):
                    here = pl.ds(pl.multiple_of(s * rows, 16), rows)
                    own[m * steps + s] = taken(table, m, 0, here, backs)
                    return carry

                lax.fori_loop(0, steps, stay, 0)

        pl.run_scoped(
            fetched, pltpu.VMEM(table_ref.shape, jnp.int32), pltpu.VMEM((local, 8 * CAP, width + LANES), jnp.bfloat16))

        def backward(tok, middle, cot, proj, mixed, gates, dproj, dmats, dnorms, drouter):
            dmats[...] = jnp.zeros_like(dmats)
            dnorms[...] = jnp.zeros_like(dnorms)
            drouter[...] = jnp.zeros_like(drouter)
            pairs = [(tok_ref, tok), (middle_out, middle), (cot_ref, cot), (proj_out, proj),
                     (mixed_out, mixed), (gates_out, gates)]

            def micro(m, carry):
                ours = pl.ds(m * (images // micros), images // micros)
                takes = [pltpu.make_async_copy(a.at[ours], b, fetch.at[n]) for n, (a, b) in enumerate(pairs)]
                for copy in takes:
                    copy.start()
                for copy in takes:
                    copy.wait()

                def attend(s, inside):
                    away(m, s, 0).wait()
                    away(m, s, 1).wait()
                    here = pl.ds(pl.multiple_of(s * rows, 16), rows)
                    grad = own[m * steps + s] + jnp.concatenate([
                        shared_r[m, 1, here].astype(jnp.float32), away_g[m, 1, here].astype(jnp.float32)], 1)
                    backward_rows(s * per_step, per_step, grad, tok, middle, cot, gates, proj, mixed,
                                  bias_ref.at[ours], mats_ref, norms_ref, router_ref, cot, dnorms, drouter,
                                  dproj, dmats)
                    return inside

                lax.fori_loop(0, steps, attend, 0)
                keep = pltpu.make_async_copy(cot, input_out.at[ours], store.at[0])
                keep.start()
                keep.wait()
                return carry

            lax.fori_loop(0, micros, micro, 0)
            tail = jnp.concatenate(
                [jnp.zeros((96, width), jnp.float32), dnorms[...], jnp.zeros((24, width), jnp.float32)], 0)
            drouter[...] += tail.T

            def spread(r, carry):
                o, i, t = relative(r)
                row = pl.multiple_of((o * 8 + i) * depth, depth)
                for c in range(kinds):
                    gathered[r, c * depth:(c + 1) * depth] = dmats[t, c, pl.ds(row, depth)].astype(jnp.bfloat16)
                row = pl.multiple_of(((o * 8 + i) * 2 + t) * 16, 16)
                gathered[r, kinds * depth:, 0:LANES] = drouter[pl.ds(row, 16)].astype(jnp.bfloat16)
                gathered[r, kinds * depth:, LANES:] = jnp.zeros((16, columns - LANES), jnp.bfloat16)
                return carry

            lax.fori_loop(0, gathered.shape[0], spread, 0)

        some = images // micros
        pl.run_scoped(
            backward,
            pltpu.VMEM((some, length, width), jnp.float32),
            pltpu.VMEM((some, length, width), jnp.float32),
            pltpu.VMEM((some, length, width), jnp.float32),
            pltpu.VMEM((some, length, 3 * width), jnp.bfloat16),
            pltpu.VMEM((some, length, width), jnp.bfloat16),
            pltpu.VMEM((some, length, LANES), jnp.float32),
            pltpu.VMEM((rows, 3 * width), jnp.float32),
            pltpu.VMEM(mats_ref.shape, jnp.float32),
            pltpu.VMEM((8, width), jnp.float32),
            pltpu.VMEM((width, LANES), jnp.float32),
        )

    pl.run_scoped(collect, pltpu.VMEM((micros * steps, rows, width + LANES), jnp.float32))

    def fold(j):
        size = 2 ** j
        return to_peer(gathered.at[pl.ds(size, size)], partial.at[pl.ds(size, size)],
                       fold_send.at[j], fold_recv.at[j], stages[j])

    def folded(j):
        fold(j).wait()
        size = 2 ** j

        def add(r, carry):
            gathered[r] = (gathered[r].astype(jnp.float32) + partial[size + r].astype(jnp.float32)).astype(
                jnp.bfloat16)
            return carry

        lax.fori_loop(0, size, add, 0)

    def outputs(table, middle, results):
        fold(4).start()
        index_take = pltpu.make_async_copy(table_ref, table, fetch.at[3])
        index_take.start()
        take = pltpu.make_async_copy(middle_out, middle, fetch.at[2])
        take.start()
        def load(m, k):
            return pltpu.make_async_copy(result_ref.at[k, m], results.at[m, k], fetch.at[4 + k])

        folded(4)
        fold(3).start()
        index_take.wait()
        for m in range(micros):
            for k in range(local):
                result.finish(k, m)
                load(m, k).start()
            for k in range(local):
                load(m, k).wait()

            def leave(s, carry):
                here = pl.ds(pl.multiple_of(s * rows, 16), rows)
                shared_c[m, 0, here] = taken(table, m, 1, here, results.at[m]).astype(jnp.bfloat16)
                away(m, s, 2).start()
                return carry

            lax.fori_loop(0, steps, leave, 0)
        folded(3)
        fold(2).start()
        take.wait()
        for m in range(micros):
            def stay(s, carry):
                n = m * steps + s
                here = pl.ds(pl.multiple_of(s * rows, 16), rows)
                away(m, s, 2).wait()
                total = taken(table, m, 0, here, results.at[m]) + shared_c[m, 1, here].astype(jnp.float32)
                images_here = pl.ds(n * per_step, per_step)
                middle[images_here] = middle[images_here] + total.reshape(per_step, length, width)
                return carry

            lax.fori_loop(0, steps, stay, 0)
            if m == 0:
                folded(2)
                fold(1).start()
        keep = pltpu.make_async_copy(middle, block_out, store.at[0])
        keep.start()
        folded(1)
        fold(0).start()
        fold(0).wait()
        small_ref[...] = gathered[0].astype(jnp.float32) + partial[1].astype(jnp.float32)
        keep.wait()

    pl.run_scoped(
        outputs, pltpu.VMEM(table_ref.shape, jnp.int32), pltpu.VMEM(tok_ref.shape, jnp.float32),
        pltpu.VMEM((micros, local, 8 * CAP, width), jnp.bfloat16))

    def close(k, carry):
        gradients.finish(k)
        return carry

    lax.fori_loop(0, local, close, 0)


def opening(pack, cot, index, table, tok, bias, first_in, second_in, local, per_step):
    micros, own_rows = index.shape[0], index.shape[3]
    images, length, width = tok.shape
    columns = pack.shape[1]
    experts, depth, extent = first_in.shape
    steps = own_rows // (per_step * length)
    slots = micros * 8 * CAP
    anywhere = pl.BlockSpec(memory_space=pl.ANY)
    vector = pl.BlockSpec(memory_space=pltpu.VMEM)
    dma = pltpu.SemaphoreType.DMA
    low, wide = jnp.bfloat16, jnp.float32
    weights = (local, 2, 8, 2, 2, depth, extent)
    shape = jax.ShapeDtypeStruct
    return pl.pallas_call(
        functools.partial(opening_kernel, local, per_step),
        in_specs=[anywhere, anywhere, vector, anywhere, anywhere, vector, anywhere, anywhere],
        out_specs=[vector] + [anywhere] * 11,
        out_shape=[
            shape(pack.shape, wide), shape(tok.shape, wide), shape(tok.shape, wide),
            shape((2, experts, 2, depth, extent), low),
            shape((images, length, width), wide), shape((images, length, 3 * width), low),
            shape((images, length, width), low), shape((images, length, LANES), wide),
            shape((local, slots, width), low), shape((local, slots, width), low),
            shape((local, micros, 8 * CAP, width + LANES), low), shape((local, micros, 8 * CAP, width), low),
        ],
        scratch_shapes=[
            pltpu.VMEM((32,) + pack.shape, low),
            pltpu.VMEM((32,) + pack.shape, low),
            pltpu.VMEM((32, width // 32, LANES), wide),
            pltpu.VMEM((2, 4, width, columns), low), pltpu.VMEM((8, width), wide),
            pltpu.VMEM((LANES, width), low), pltpu.VMEM((LANES, width), wide),
            pltpu.VMEM((micros, 2, own_rows, width), low),
            pltpu.VMEM((micros, 2, own_rows, width), low),
            pltpu.VMEM((micros, 2, own_rows, LANES), low),
            pltpu.VMEM((micros, 8, local, CAP, width), low),
            pltpu.VMEM((micros, 8, local, CAP, width), low),
            pltpu.VMEM(weights, low),
            pltpu.VMEM((micros, 8, local, CAP, width + LANES), low),
            dma((3,)), dma((5,)), dma((5,)), dma((micros,)), dma((micros,)),
            dma((micros, steps)), dma((micros, steps)),
            dma((micros, 8, local)), dma((micros, 8, local)), dma((micros, local)),
            dma((micros, 8, local)), dma((micros, 8, local)), dma((micros, local)),
            dma((local, 32, 2)), dma((local, 32, 2)), dma((local, 2)),
            dma((local, 32, 2)), dma((local, 32, 2)), dma((local, 2)),
            dma((local, micros, 8)), dma((local, micros, 8)), dma((local, micros)),
            dma((local, micros, 8)), dma((local, micros, 8)), dma((local, micros)), dma((4,)),
            dma((3, micros, steps)), dma((3, micros, steps)), dma((5,)), dma((5,)), dma((6,)),
        ],
        compiler_params=pltpu.CompilerParams(vmem_limit_bytes=67043328, has_side_effects=True),
        cost_estimate=pl.CostEstimate(flops=1000, bytes_accessed=1000, transcendentals=0),
        name="opening",
    )(pack, cot, index, table, tok, bias, first_in, second_in)


def per_device(planes, inner, parts, tokens, key_mask, expert_ids, slot_ids, norm1_gain, norm1_bias,
               qkv_weight, out_weight, norm2_gain, norm2_bias, router_weight, expert_in, expert_out,
               cotangent):
    micros, own_rows, width = tokens.shape
    length = key_mask.shape[2]
    group_rows = own_rows * parts
    images = own_rows // length
    total = micros * images
    experts = expert_in.shape[0]
    homes = inner * parts
    local = experts // homes
    depth, extent = expert_in.shape[1:]
    small = norm1_gain.shape[0]
    every = ("o", "i", "t")
    plane_at, inner_at, part_at = (lax.axis_index(name) for name in every)
    low = jnp.bfloat16

    loose = jnp.concatenate([
        jnp.stack([norm1_gain, norm1_bias, norm2_gain, norm2_bias], 1), router_weight], 1)
    loose_count = 3 * loose.size
    columns = qkv_weight.shape[2]
    loose_rows = -(-loose_count // (16 * columns)) * 16
    loose_low = jnp.concatenate([p.reshape(-1) for p in three_parts(loose)])
    loose_low = jnp.pad(loose_low, (0, loose_rows * columns - loose_count)).reshape(loose_rows, columns)
    packed = jnp.concatenate([
        qkv_weight.transpose(1, 0, 2).reshape(3 * depth, columns), out_weight.T, loose_low], 0)
    gathered = lax.all_gather(packed, ("o", "i"), axis=0)
    gathered = lax.all_gather(gathered, "t", axis=0)
    mats = gathered[:, :, :4 * depth].reshape(parts, planes * inner, 4, depth, columns)
    mats = mats.transpose(2, 1, 3, 0, 4).reshape(1, 4, width, width)
    loose_all = gathered[:, :, 4 * depth:].reshape(parts, planes * inner, loose_rows * columns)
    loose_all = loose_all[:, :, :loose_count].astype(jnp.float32)
    loose_all = loose_all.reshape(parts, planes * inner, 3, small, 4 + experts)
    loose_all = (loose_all[:, :, 0] + loose_all[:, :, 1]) + loose_all[:, :, 2]
    loose_all = loose_all.transpose(1, 0, 2, 3).reshape(width, 4 + experts)
    norms = loose_all[:, :4].T
    router = jnp.pad(loose_all[:, 4:], ((0, 0), (0, LANES - experts)))
    router_parts = jnp.concatenate(three_parts(router[:, :experts]), 1).T
    router_parts = jnp.pad(router_parts, ((0, LANES - 3 * experts), (0, 0)))

    weights = []
    first_in = expert_in.reshape(homes, local, depth, extent)
    second_in = expert_out.transpose(0, 2, 1).reshape(homes, local, depth, extent)
    for k in range(local):
        both = jnp.stack([first_in[:, k], second_in[:, k]], 1)
        mine = lax.all_to_all(both, ("i", "t"), 0, 0, tiled=True)
        if planes == 2:
            other = lax.ppermute(mine, "o", [(0, 1), (1, 0)])
            full = jnp.where(plane_at == 0, jnp.stack([mine, other]), jnp.stack([other, mine]))
        else:
            full = lax.all_gather(mine, "o", axis=0)
        weights.append(full.reshape(planes, inner, parts, 2, depth, extent))

    own_first = part_at * own_rows
    slot_index = jnp.where(slot_ids >= 0, expert_ids * CAP + slot_ids, -1)
    if parts == 2:
        slot_index = jnp.concatenate([
            lax.dynamic_slice_in_dim(slot_index, own_first, own_rows, 1),
            lax.dynamic_slice_in_dim(slot_index, own_rows - own_first, own_rows, 1)], 1)
    homes_i = lax.broadcasted_iota(jnp.int32, (inner, local, CAP), 0)
    locals_i = lax.broadcasted_iota(jnp.int32, (inner, local, CAP), 1)
    cap_i = lax.broadcasted_iota(jnp.int32, (inner, local, CAP), 2)
    places = ((homes_i * parts + part_at) * local + locals_i) * CAP + cap_i

    def table(m, positions, rows=slice(None)):
        index = slot_index[m, rows]
        flat = positions.reshape(1, -1)
        return ((index[:, 0:1] == flat) | (index[:, 1:2] == flat)).astype(low)

    def share(rows):
        if parts == 2:
            return jnp.concatenate([rows, lax.ppermute(rows, "t", [(0, 1), (1, 0)])], 1)
        return lax.all_gather(rows, "t", axis=1, tiled=True)

    def dispatch(shared):
        sent = []
        for m in range(micros):
            slots = mm(table(m, places), shared[m], TN).astype(low)
            slots = lax.all_to_all(slots.reshape(inner, local * CAP, width), "i", 0, 0, tiled=True)
            sent.append(slots.reshape(inner, local, CAP, width))
        return [
            jnp.concatenate([s[:, k].reshape(inner * CAP, width) for s in sent], 0) for k in range(local)]

    cot_slots = dispatch(share(cotangent.astype(low)))

    flags = lax.dynamic_slice_in_dim(key_mask, part_at * images, images, 1).reshape(total, 1, length)
    bias = jnp.where(flags > 0, 0.0, -1e30).astype(jnp.float32)
    tok = tokens.reshape(total, length, width)
    per_step = 2 if total % 2 == 0 else 1
    middle, routed, proj, mixed, gates = attention_forward(tok, bias, mats, norms, router_parts, per_step)

    row_slots = dispatch(share(routed.reshape(micros, own_rows, width)))

    first_out, second_out, results, backs = [], [], [], []
    for k in range(local):
        expert = ((inner_at * parts + part_at) * local + k).astype(jnp.int32).reshape(1)
        result, back, dweights = run_expert(expert, row_slots[k], cot_slots[k], weights[k], router_parts)
        results.append(result.reshape(micros, inner, CAP, width))
        backs.append(back.reshape(micros, inner, CAP, width + LANES))
        dweights = dweights.reshape(planes, homes, 2, depth, extent)
        if planes == 2:
            theirs = lax.dynamic_index_in_dim(dweights, 1 - plane_at, 0, keepdims=False)
            ours = lax.dynamic_index_in_dim(dweights, plane_at, 0, keepdims=False)
            summed = ours.astype(jnp.float32) + lax.ppermute(
                theirs, "o", [(0, 1), (1, 0)]).astype(jnp.float32)
            summed = summed.astype(low)
        else:
            summed = lax.psum_scatter(dweights, "o", scatter_dimension=0, tiled=True)[0]
        final = lax.all_to_all(summed, ("i", "t"), 0, 0, tiled=True)
        first_out.append(final[:, 0])
        second_out.append(final[:, 1])
    first_grad = jnp.stack(first_out, 1).reshape(experts, depth, extent).astype(jnp.float32)
    second_grad = jnp.stack(second_out, 1).reshape(experts, depth, extent).astype(jnp.float32)
    second_grad = second_grad.transpose(0, 2, 1)

    def collect(values):
        size = values[0].shape[-1]
        answers = []
        for m in range(micros):
            back = jnp.stack([v[m] for v in values], 1).reshape(inner, local * CAP, size)
            back = lax.all_to_all(back, "i", 0, 0, tiled=True).reshape(inner * local * CAP, size)
            if parts == 2:
                away = mm(table(m, places, slice(own_rows, None)), back).astype(low)
                here = mm(table(m, places, slice(0, own_rows)), back)
                answers.append(here + lax.ppermute(away, "t", [(0, 1), (1, 0)]).astype(jnp.float32))
            else:
                whole = mm(table(m, places), back).astype(low)
                answers.append(lax.psum_scatter(
                    whole, "t", scatter_dimension=0, tiled=True).astype(jnp.float32))
        return jnp.stack(answers)

    grad = collect(backs)
    combined = collect(results)
    block_out = middle.reshape(micros, own_rows, width) + combined

    input_grad, dmats, dnorms, drouter = attention_backward(
        tok, middle, cotangent.reshape(total, length, width), grad.reshape(total, length, width + LANES),
        gates, proj, mixed, bias, mats, norms, router.T, per_step)
    input_grad = input_grad.reshape(micros, own_rows, width)

    dmats = dmats.reshape(4, planes, inner, depth, parts, columns).transpose(2, 4, 1, 0, 3, 5)
    dmats = dmats.reshape(homes, planes, 4 * depth, columns)
    dloose = jnp.concatenate([dnorms.T, drouter[:, :experts]], 1)
    dloose = dloose.reshape(planes, inner, parts, small * (4 + experts)).transpose(1, 2, 0, 3)
    dloose = jnp.concatenate(three_parts(dloose), -1)
    dloose = jnp.pad(dloose, ((0, 0),) * 3 + ((0, loose_rows * columns - loose_count),))
    dloose = dloose.reshape(homes, planes, loose_rows, columns)
    payload = jnp.concatenate([dmats, dloose], 2)
    payload = lax.all_to_all(payload, ("i", "t"), 0, 0, tiled=True)
    payload = jnp.sum(payload.astype(jnp.float32), 0)
    if planes == 2:
        theirs = lax.dynamic_index_in_dim(payload, 1 - plane_at, 0, keepdims=False)
        ours = lax.dynamic_index_in_dim(payload, plane_at, 0, keepdims=False)
        reduced = ours + lax.ppermute(theirs, "o", [(0, 1), (1, 0)])
    else:
        reduced = lax.psum_scatter(payload, "o", scatter_dimension=0, tiled=True)[0]
    matrices = reduced[:4 * depth].reshape(4, depth, columns)
    qkv_grad = matrices[:3].transpose(1, 0, 2)
    out_grad = matrices[3].T
    tail = reduced[4 * depth:].reshape(-1)[:loose_count].reshape(3, small, 4 + experts)
    tail = (tail[0] + tail[1]) + tail[2]
    return (
        block_out, input_grad, tail[:, 0], tail[:, 1], qkv_grad, out_grad, tail[:, 2], tail[:, 3],
        tail[:, 4:], first_grad, second_grad,
    )


def per_device_halves(tokens, key_mask, expert_ids, slot_ids, norm1_gain, norm1_bias,
                      qkv_weight, out_weight, norm2_gain, norm2_bias, router_weight, expert_in, expert_out,
                      cotangent):
    micros, own_rows, width = tokens.shape
    length = key_mask.shape[2]
    images = own_rows // length
    total = micros * images
    planes, inner, parts = 2, 8, 2
    experts = expert_in.shape[0]
    homes = inner * parts
    local = experts // homes
    depth, extent = expert_in.shape[1:]
    columns = qkv_weight.shape[2]
    plane_at, inner_at, part_at = (lax.axis_index(name) for name in ("o", "i", "t"))
    low = jnp.bfloat16
    across = [(0, 1), (1, 0)]

    norms_in = jnp.stack([norm1_gain, norm1_bias, norm2_gain, norm2_bias], 1)
    loose = [p for p in three_parts(router_weight)]
    loose += [jnp.pad(p, ((0, 0), (0, 4))) for p in three_parts(norms_in)]
    loose = jnp.concatenate(loose, 1)
    loose = jnp.pad(loose, ((0, 0), (0, columns - loose.shape[1])))
    packed = jnp.concatenate([
        qkv_weight.transpose(1, 0, 2).reshape(3 * depth, columns), out_weight.T, loose], 0)
    slot_index = jnp.where(slot_ids >= 0, expert_ids * CAP + slot_ids, -1)
    own_first = part_at * own_rows
    halves = jnp.stack([
        lax.dynamic_slice_in_dim(slot_index, own_first, own_rows, 1),
        lax.dynamic_slice_in_dim(slot_index, own_rows - own_first, own_rows, 1)], 1)
    index = halves.transpose(0, 3, 1, 2)

    flags = lax.dynamic_slice_in_dim(key_mask, part_at * images, images, 1).reshape(total, 1, length)
    bias = jnp.where(flags > 0, 0.0, -1e30).astype(jnp.float32)
    tok = tokens.reshape(total, length, width)
    table = jnp.pad(halves, ((0, 0), (0, 0), (0, 0), (0, LANES - 2)))
    reduced, block_out, input_grad, dweights = opening(
        packed, cotangent.reshape(tok.shape), index, table, tok, bias, expert_in, expert_out.transpose(0, 2, 1), local, 2)[:4]
    first_grad = dweights[0, :, 0].astype(jnp.float32) + dweights[1, :, 0].astype(jnp.float32)
    second_grad = dweights[0, :, 1].astype(jnp.float32) + dweights[1, :, 1].astype(jnp.float32)
    second_grad = second_grad.transpose(0, 2, 1)
    matrices = reduced[:4 * depth].reshape(4, depth, columns)
    qkv_grad = matrices[:3].transpose(1, 0, 2)
    out_grad = matrices[3].T
    tail = reduced[4 * depth:]
    shape = (micros, own_rows, width)
    return (
        block_out.reshape(shape), input_grad.reshape(shape), tail[:, 96], tail[:, 97], qkv_grad, out_grad,
        tail[:, 98], tail[:, 99], tail[:, :experts], first_grad, second_grad,
    )


def solution(mesh):
    dp, parts = mesh.shape["dp"], mesh.shape["tensor"]
    inner = min(8, 32 // parts, dp)
    planes = dp // inner
    fine = Mesh(mesh.devices.reshape(planes, inner, parts), ("o", "i", "t"))
    dps = ("o", "i")
    every = ("o", "i", "t")
    rows = P(None, every, None)
    step = functools.partial(per_device, planes, inner, parts)
    if (planes, inner, parts) == (2, 8, 2):
        step = per_device_halves
    return jax.shard_map(
        step,
        mesh=fine,
        in_specs=(
            rows, P(None, dps, None), P(None, dps, None), P(None, dps, None), P(every), P(every),
            P(dps, None, "t"), P("t", dps), P(every), P(every), P(every, None),
            P(None, dps, "t"), P(None, "t", dps), rows,
        ),
        out_specs=(
            rows, rows, P(every), P(every), P(dps, None, "t"), P("t", dps), P(every), P(every),
            P(every, None), P(None, dps, "t"), P(None, "t", dps),
        ),
        check_vma=False,
    )
```
